32 devices in a mesh: gx: 2 (over y), gy: 4 (over x, core), gz: 4 (over z).
Axes of the slice: x: 2, y: 2, z: 4, core: 2. Of those that a mesh axis runs over, the one named last changes fastest.
Arguments:
- loads: float32 [16, 4, 16, 1024], P(None, 'gx', 'gy', 'gz'), may hold values from -60 to 60
- moduli: float32 [8], replicated, may hold values from 0.5 to 4
- material: int32 [4, 16, 1024], P('gx', 'gy', 'gz'), may hold values from 0 to 7
Outputs:
- solution: float32 [16, 4, 16, 1024], P(None, 'gx', 'gy', 'gz')
- residual: float32 [16, 4, 16, 1024], P(None, 'gx', 'gy', 'gz')
The draws below stay inside these ranges and needn't reach their ends.
All inputs are finite; a program needn't handle non-finite values.
Results may differ from the reference program's by a relative error of at most 0.005.
The reference program's roundings to bfloat16 on the way (of `kernel`) count: a program that leaves them out, or rounds other values in their place, can miss the bound.
Values may be sent and summed in bfloat16 or wider, within the bound.
A program may use at most 64 MiB of HBM per device.

```python
import math
import jax
import jax.numpy as jnp
import numpy as np
from jax import lax

COLS = 16
MATS = 8
ITERS = 2
NX = 4
NY = 16
NZ = 1024


def draw_loads(key, part):
    key_base = jax.random.fold_in(jax.random.fold_in(key, 11), 0)
    key_scale = jax.random.fold_in(jax.random.fold_in(key, 11), 1)
    key_modes = jax.random.fold_in(jax.random.fold_in(key, 11), 3)
    shape = (COLS, NX, NY, NZ)
    pos_x = jnp.arange(NX, dtype=jnp.float32).reshape(1, NX, 1, 1)
    pos_y = jnp.arange(NY, dtype=jnp.float32).reshape(1, 1, NY, 1)
    pos_z = jnp.arange(NZ, dtype=jnp.float32).reshape(1, 1, 1, NZ)
    depth = pos_z / max(NZ - 1, 1)
    across = pos_x / max(NX - 1, 1)
    upper = (pos_y >= NY // 2).astype(jnp.float32)
    ramp = (1.0 + 2.0 * depth) * 0.5
    roughness = jnp.exp(-math.log(10.0) * (1.2 * upper + 0.4 * across + 0.6 * depth))
    scales = jnp.exp(jax.random.uniform(key_scale, (COLS, 1, 1, 1), jnp.float32, 0.0, math.log(10.0))) / 3.0
    key_my, key_mz, key_coef = jax.random.split(key_modes, 3)
    wave_y = jax.random.randint(key_my, (COLS, 3), 1, 3).astype(jnp.float32)
    wave_z = jax.random.randint(key_mz, (COLS, 3), 1, 5).astype(jnp.float32)
    coefs = jax.random.normal(key_coef, (COLS, 3), jnp.float32)
    shape_x = jnp.sin(math.pi * (pos_x + 1.0) / (NX + 1.0))
    smooth = jnp.zeros(shape, jnp.float32)
    for mode in range(3):
        my = wave_y[:, mode].reshape(COLS, 1, 1, 1)
        mz = wave_z[:, mode].reshape(COLS, 1, 1, 1)
        amp = coefs[:, mode].reshape(COLS, 1, 1, 1)
        term = shape_x * jnp.sin(math.pi * my * (pos_y + 1.0) / (NY + 1.0)) * jnp.sin(math.pi * mz * (pos_z + 1.0) / (NZ + 1.0))
        smooth = smooth + amp * term
    smooth = smooth * math.sqrt(8.0 / 3.0)
    rough = jax.random.normal(key_base, shape, jnp.float32)
    field = roughness * rough + 0.7 * smooth
    return jnp.clip(field * scales * ramp, -60.0, 60.0)


def touch_ends(result, stream_key, least, top_value):
    spot = [jax.random.randint(jax.random.fold_in(stream_key, axis), (), 0, length) for axis, length in enumerate(result.shape)]
    widest = result.shape.index(max(result.shape))
    beside = spot[:widest] + [(spot[widest] + 1) % result.shape[widest]] + spot[widest + 1:]
    return result.at[tuple(spot)].set(least).at[tuple(beside)].set(top_value)


def setup_inputs(seed: int = 0) -> dict:
    arg_keys = jax.random.split(jax.random.key(seed), 4)
    loads = draw_loads(jax.random.fold_in(arg_keys[3], 71), 0)
    moduli = jnp.clip(jnp.exp(jax.random.uniform(arg_keys[1], (MATS,), jnp.float32, math.log(0.5), math.log(4.0))), 0.5, 4.0)
    material = touch_ends(jax.random.randint(arg_keys[2], (NX, NY, NZ), 0, MATS), jax.random.fold_in(arg_keys[2], 1), 0, MATS - 1).astype(jnp.int32)
    return dict(loads=loads, moduli=moduli, material=material)


SIGMA = 0.25

def stiffness_table():
    line_mass = np.array([[1.0 / 3.0, 1.0 / 6.0], [1.0 / 6.0, 1.0 / 3.0]])
    line_stiff = np.array([[1.0, -1.0], [-1.0, 1.0]])
    table = np.zeros((8, 8))
    for target in range(8):
        for source in range(8):
            target_bits = [target >> 2 & 1, target >> 1 & 1, target & 1]
            source_bits = [source >> 2 & 1, source >> 1 & 1, source & 1]
            total = 0.0
            for stiff_dim in range(3):
                factor = 1.0
                for other in range(3):
                    if other == stiff_dim:
                        factor = factor * line_stiff[target_bits[other], source_bits[other]]
                    else:
                        factor = factor * line_mass[target_bits[other], source_bits[other]]
                total = total + factor
            table[target, source] = total
    return table

def corner_bits(corner):
    return (corner >> 2 & 1, corner >> 1 & 1, corner & 1)

def apply_column(column, weights, kernel):
    size_x, size_y, size_z = column.shape
    padded = jnp.pad(column.astype(jnp.bfloat16), 1)
    pieces = []
    for corner in range(8):
        bit_x, bit_y, bit_z = corner_bits(corner)
        pieces.append(padded[bit_x:bit_x + size_x + 1, bit_y:bit_y + size_y + 1, bit_z:bit_z + size_z + 1])
    stacked = jnp.stack(pieces).astype(jnp.float32)
    total = SIGMA * column
    for corner in range(8):
        bit_x, bit_y, bit_z = corner_bits(corner)
        part = jnp.einsum('b,bxyz->xyz', kernel[corner], stacked, precision=lax.Precision.HIGHEST) * weights
        total = total + part[1 - bit_x:1 - bit_x + size_x, 1 - bit_y:1 - bit_y + size_y, 1 - bit_z:1 - bit_z + size_z]
    return total

def gram(left, right):
    return jnp.einsum('cxyz,dxyz->cd', left, right, precision=lax.Precision.HIGHEST)

def combine(block, coeffs):
    return jnp.einsum('cxyz,cd->dxyz', block, coeffs, precision=lax.Precision.HIGHEST)

def solve_small(matrix, rhs_small):
    factor = jnp.linalg.cholesky(matrix)
    return jax.scipy.linalg.cho_solve((factor, True), rhs_small)

def reference(loads, moduli, material):
    kernel = jnp.asarray(stiffness_table(), jnp.float32).astype(jnp.bfloat16).astype(jnp.float32)
    node_modulus = jnp.take(moduli, material, axis=0)
    padded_mod = jnp.pad(node_modulus, 1)
    size_x, size_y, size_z = material.shape
    weights = jnp.zeros((size_x + 1, size_y + 1, size_z + 1), jnp.float32)
    for corner in range(8):
        bit_x, bit_y, bit_z = corner_bits(corner)
        weights = weights + padded_mod[bit_x:bit_x + size_x + 1, bit_y:bit_y + size_y + 1, bit_z:bit_z + size_z + 1]
    weights = weights * 0.125

    def operator(block):
        return lax.map(lambda column: apply_column(column, weights, kernel), block)
    solution = jnp.zeros_like(loads)
    residual = loads
    direction = loads
    current = gram(residual, residual)
    for iteration in range(ITERS):
        image = operator(direction)
        alpha = solve_small(gram(direction, image), current)
        solution = solution + combine(direction, alpha)
        residual = residual - combine(image, alpha)
        if iteration + 1 < ITERS:
            updated = gram(residual, residual)
            beta = solve_small(current, updated)
            direction = residual + combine(direction, beta)
            current = updated
    return (solution, residual)
```

```python
import functools
import itertools

import jax
import jax.numpy as jnp
import numpy as np
from jax import lax
from jax.experimental import pallas as pl
from jax.experimental.pallas import tpu as pltpu
from jax.sharding import PartitionSpec as P

SIGMA = 0.25
AXES = ("gx", "gy", "gz")
HIGH = lax.Precision.HIGHEST
F32 = jnp.float32
BF16 = jnp.bfloat16
LANES = 128
DIRECT_LIMIT = 32
IDS = 64


def stiffness_values():
    mass = (1.0 / 3.0, 1.0 / 6.0)
    stiff = (1.0, -1.0)
    values = []
    for differing in range(4):
        bits = [1 if dim < differing else 0 for dim in range(3)]
        total = 0.0
        for dim in range(3):
            factor = 1.0
            for other in range(3):
                factor *= stiff[bits[other]] if other == dim else mass[bits[other]]
            total += factor
        values.append(float(np.asarray(total, np.float32).astype(jnp.bfloat16).astype(np.float32)))
    return values


def dot(left, right, left_dim, right_dim, precision=HIGH):
    return lax.dot_general(
        left, right, (((left_dim,), (right_dim,)), ((), ())), precision=precision, preferred_element_type=F32
    )


def pack(matrix):
    rows, cols = matrix.shape
    wide = jnp.concatenate([matrix, jnp.zeros((rows, LANES - cols), F32)], axis=1)
    pieces = [
        jnp.sum(pltpu.roll(wide[start : start + 8], 0, 1, stride=cols, stride_axis=0), axis=0, keepdims=True)
        for start in range(0, rows, 8)
    ]
    return jnp.concatenate(pieces, axis=0)


def unpack(tile, cols):
    rows = tile.shape[0]
    tall = jnp.concatenate([tile, jnp.zeros((8 - rows, LANES), F32)], axis=0)
    turned = [tall] + [pltpu.roll(tall, LANES - cols * group, 1) for group in range(1, 8)]
    return jnp.concatenate(
        [turned[group][row : row + 1] for row in range(rows) for group in range(8)], axis=0
    )[:, 0:cols]


def solve(matrix, rhs):
    size = matrix.shape[0]
    wide = jnp.concatenate([rhs, jnp.zeros((size, LANES - rhs.shape[1]), F32)], axis=1)
    left = [jnp.broadcast_to(matrix[:, i : i + 1], (size, LANES)) for i in range(size)]
    right = [wide[i : i + 1, :] for i in range(size)]
    start = 0
    for step in range(size):
        if step == size // 2 and step % 8 == 0:
            left = [row[step:, :] for row in left]
            start = step
        at = step - start
        scale = 1.0 / left[step][at : at + 1, :]
        pivot, pivot_right = left[step] * scale, right[step] * scale
        for i in range(size):
            if i != step:
                factor = left[i][at : at + 1, :]
                left[i] = left[i] - factor * pivot
                right[i] = right[i] - factor * pivot_right
        left[step], right[step] = pivot, pivot_right
    return jnp.concatenate(right, axis=0)[:, 0 : rhs.shape[1]]


def tree_sum(terms):
    while len(terms) > 1:
        terms = [a + b for a, b in zip(terms[0::2], terms[1::2])] + terms[len(terms) & ~1 :]
    return terms[0]


def main_body(sizes, plans, stiff, moduli_hbm, loads_ref, mat_hbm, base_ref, pair_ref, coef_ref,
              stack, padded, padded_im, mats_rx, ends, ends_rx, ends_im, ends_im_rx, field, wt, wtr,
              shares_table, shares_last, moduli_ref, mat_ref, credit,
              halo_send, halo_recv, sum_send, sum_recv, local_sems, vouch_sem):
    cols, nx, ny, nz = loads_ref.shape
    mats = moduli_ref.shape[0]
    me = [lax.axis_index(axis) for axis in AXES]
    k_self, k_edge, k_far = stiff[0], stiff[1], stiff[2]
    assert k_edge == 0.0 and stiff[2] == stiff[3]
    assert 2 * nx * ny <= IDS and (nx * ny * nz) % (cols * LANES) == 0 and nz % LANES == 0
    xs, ys = range(nx + 2), range(ny + 2)
    shares_of = (shares_table, shares_last)
    own = list(itertools.product(range(nx), range(ny)))

    directions = [
        d for d in itertools.product((-1, 0, 1), repeat=3)
        if any(d) and all(step == 0 or sizes[i] > 1 for i, step in enumerate(d))
    ]
    directions.sort(key=lambda d: -sum(abs(step) for step in d))

    def exists(direction):
        good = None
        for i, step in enumerate(direction):
            if step:
                here = (me[i] > 0) if step < 0 else (me[i] < sizes[i] - 1)
                good = here if good is None else jnp.logical_and(good, here)
        return good

    def target(direction):
        return {axis: me[i] + direction[i] for i, axis in enumerate(AXES)}

    def place(direction):
        return 1 - direction[0], 1 - direction[1]

    def halo_start(round_):
        core, source, edge = ((padded, ends, ends_rx), (padded_im, ends_im, ends_im_rx))[round_]
        for direction in directions:
            dx, dy, dz = direction
            pairs = []
            if dz == 0:
                src_x = {0: pl.ds(1, nx), 1: pl.ds(nx, 1), -1: pl.ds(1, 1)}[dx]
                dst_x = {0: pl.ds(1, nx), 1: pl.ds(0, 1), -1: pl.ds(nx + 1, 1)}[dx]
                src_y = {0: pl.ds(1, ny), 1: pl.ds(ny, 1), -1: pl.ds(1, 1)}[dy]
                dst_y = {0: pl.ds(1, ny), 1: pl.ds(0, 1), -1: pl.ds(ny + 1, 1)}[dy]
                pairs.append((core.at[src_x, src_y], core.at[dst_x, dst_y]))
                if round_ == 0:
                    pairs.append((mats_rx.at[1, 1], mats_rx.at[place(direction)]))
            else:
                pairs.append((source.at[1 if dz > 0 else 0], edge.at[(*place(direction), 0 if dz > 0 else 1)]))

            @pl.when(exists(direction))
            def _():
                for src, dst in pairs:
                    pltpu.make_async_remote_copy(
                        src_ref=src, dst_ref=dst, send_sem=halo_send.at[round_], recv_sem=halo_recv.at[round_],
                        device_id=target(direction), device_id_type=pl.DeviceIdType.MESH,
                    ).start()

    def halo_wait(round_, sem):
        numbers = [
            ((me[i] > 0).astype(jnp.int32) + (me[i] < sizes[i] - 1).astype(jnp.int32)) for i in range(3)
        ]
        choices = [(0,) if size == 1 else (1,) if size == 2 else (1, 2) for size in sizes]
        per = nz // LANES
        for cx, cy, cz in itertools.product(*choices):
            total = per * (cx * ny + cy * nx + cx * cy) + cz * (1 + cx) * (1 + cy)
            if round_ == 0:
                total += (cx + cy + cx * cy) * (nx * ny * nz // (cols * LANES))
            if total:
                tests = [numbers[i] == c for i, c in enumerate((cx, cy, cz)) if len(choices[i]) > 1]

                def take():
                    part = credit.at[pl.ds(0, total)]
                    pltpu.make_async_copy(part, part, sem).wait()

                if tests:
                    pl.when(functools.reduce(jnp.logical_and, tests))(take)
                else:
                    take()

    def each(count, body):
        if count <= 8:
            for k in range(1, count):
                body(k, 0)
        else:
            lax.fori_loop(1, count, body, 0)

    def group_of(axes):
        count, index = 1, 0
        for axis in axes:
            i = AXES.index(axis)
            count *= sizes[i]
            index = index * sizes[i] + me[i]
        return count, index

    def peer_id(axes, peer):
        coords = {axis: me[i] for i, axis in enumerate(AXES)}
        for axis in reversed(axes):
            size = sizes[AXES.index(axis)]
            coords[axis] = lax.rem(peer, size)
            peer = lax.div(peer, size)
        return coords

    def offset_of(round_, number):
        return sum(group_of(axes)[0] for axes in plans[round_][:number])

    direct = (AXES,) in plans

    for bx, by in itertools.product(range(3), repeat=2):
        for side in range(2):
            ends_rx[bx, by, side] = jnp.zeros(ends_rx.shape[3:], BF16)
            ends_im_rx[bx, by, side] = jnp.zeros(ends_im_rx.shape[3:], BF16)
        if (bx, by) != (1, 1):
            mats_rx[bx, by] = jnp.zeros(mats_rx.shape[2:], BF16)
    for x in xs:
        for y in ys:
            if not (1 <= x <= nx and 1 <= y <= ny):
                padded[x, y] = jnp.zeros(padded.shape[2:], BF16)
                padded_im[x, y] = jnp.zeros(padded_im.shape[2:], BF16)

    barrier = pltpu.get_barrier_semaphore()
    expected = 0
    if direct:
        flat = sizes[0] * sizes[1]
        spot = me[0] * sizes[1] + me[1]
        for dz in (-1, 0, 1):
            good = True if dz == 0 else exists((0, 0, dz))

            def greet(k, carry, dz=dz):
                there = lax.rem(spot + k, flat)
                pl.semaphore_signal(
                    barrier, inc=1, device_id_type=pl.DeviceIdType.MESH,
                    device_id={"gx": lax.div(there, sizes[1]), "gy": lax.rem(there, sizes[1]), "gz": me[2] + dz},
                )
                return carry

            if dz == 0:
                each(flat, greet)
                expected = expected + flat - 1
            elif sizes[2] > 1:
                @pl.when(good)
                def _():
                    greet(0, 0)
                    each(flat, greet)
                expected = expected + jnp.where(good, flat, 0)
    else:
        for axes in plans[0]:
            count, index = group_of(axes)

            def greet(k, carry, axes=axes, count=count, index=index):
                pl.semaphore_signal(barrier, inc=1, device_id=peer_id(axes, lax.rem(index + k, count)),
                                    device_id_type=pl.DeviceIdType.MESH)
                return carry

            each(count, greet)
            expected = expected + count - 1
        for direction in directions:
            good = exists(direction)

            @pl.when(good)
            def _():
                pl.semaphore_signal(barrier, inc=1, device_id=target(direction),
                                    device_id_type=pl.DeviceIdType.MESH)
            expected = expected + jnp.where(good, 1, 0)

    for x, y in own:
        pltpu.make_async_copy(loads_ref.at[:, x, y, :], stack.at[x, y, pl.ds(0, cols), :], local_sems.at[0]).start()
    mat_copy = pltpu.make_async_copy(mat_hbm, mat_ref, local_sems.at[1])
    mat_copy.start()
    moduli_copy = pltpu.make_async_copy(moduli_hbm, moduli_ref, local_sems.at[2])
    moduli_copy.start()

    vouches = max(sizes[2] - 2, 0) if direct else 0

    def vouch(round_):
        for dz in (-1, 1):
            @pl.when(exists((0, 0, dz)))
            def _():
                pl.semaphore_signal(vouch_sem.at[round_, 0 if dz > 0 else 1], inc=1, device_id=target((0, 0, dz)),
                                    device_id_type=pl.DeviceIdType.MESH)

    def vouched(round_):
        for dz in (-1, 1):
            @pl.when(exists((0, 0, dz)))
            def _():
                pl.semaphore_wait(vouch_sem.at[round_, 1 if dz > 0 else 0], 1)

    lane = lax.broadcasted_iota(jnp.int32, (1, LANES), 1)

    def spread(firsts, lasts, row, first, last, at):
        where_first, where_last = at + 2 * row, (at + 2 * row - 1) % LANES
        return (jnp.where(lane == where_first, pltpu.roll(first, where_first, 1), firsts),
                jnp.where(lane == where_last, pltpu.roll(last, (where_last + 1) % LANES, 1), lasts))

    mat_copy.wait()
    ids = jnp.concatenate([mat_ref[x] for x in range(nx)], axis=0)
    ids = (ids + 1).astype(F32)
    mats_rx[1, 1] = ids.astype(BF16)
    firsts = lasts = jnp.zeros((cols, LANES), F32)
    for x, y in own:
        row = x * ny + y
        first = jnp.broadcast_to(ids[row : row + 1, 0:LANES], (cols, LANES))
        last = jnp.broadcast_to(ids[row : row + 1, nz - LANES : nz], (cols, LANES))
        firsts, lasts = spread(firsts, lasts, row, first, last, IDS)
    whole = stack.at[:, :, pl.ds(0, cols), :]
    pltpu.make_async_copy(whole, whole, local_sems.at[0]).wait()
    for x, y in own:
        values = stack[x, y, 0:cols, :]
        padded[x + 1, y + 1] = values.astype(BF16)
        firsts, lasts = spread(firsts, lasts, x * ny + y, values[:, 0:LANES], values[:, nz - LANES : nz], 0)
    ends[0] = firsts.astype(BF16)
    ends[1] = lasts.astype(BF16)
    pl.semaphore_wait(barrier, expected)
    halo_start(0)
    if vouches:
        vouch(0)

    def gram(left, right):
        return tree_sum([dot(left(x, y), right(x, y), 1, 1) for x, y in own])

    def sum_copy(round_, number, peer):
        axes = plans[round_][number]
        count, index = group_of(axes)
        slot = offset_of(round_, number) + index
        return pltpu.make_async_remote_copy(
            src_ref=shares_of[round_].at[slot], dst_ref=shares_of[round_].at[slot],
            send_sem=sum_send.at[round_, number], recv_sem=sum_recv.at[round_, number],
            device_id=peer, device_id_type=pl.DeviceIdType.MESH,
        )

    def sum_start(round_, number, tile):
        axes = plans[round_][number]
        count, index = group_of(axes)
        shares_of[round_][offset_of(round_, number) + index] = tile
        if axes == AXES:
            plane = []
            for k in range(flat):
                there = lax.rem(spot + k, flat)
                plane.append((lax.div(there, sizes[1]), lax.rem(there, sizes[1])))
            low = 2 * me[2] < sizes[2]
            far, turn = jnp.where(low, sizes[2] - 1, 0), jnp.where(low, -1, 1)
            away = jnp.where(low, sizes[2] - 1 - me[2], me[2])
            for i in range(sizes[2] - 1):
                level = far + turn * (i + jnp.where(i < away, 0, 1))
                for gx, gy in plane[::-1]:
                    sum_copy(round_, number, {"gx": gx, "gy": gy, "gz": level}).start()
            for gx, gy in plane[:0:-1]:
                sum_copy(round_, number, {"gx": gx, "gy": gy, "gz": me[2]}).start()
        else:
            def send(k, carry):
                sum_copy(round_, number, peer_id(axes, lax.rem(index + k, count))).start()
                return carry

            each(count, send)

    def sum_wait(round_, number, sem):
        count, _ = group_of(plans[round_][number])
        if count > 1:
            part = shares_of[round_].at[pl.ds(0, count - 1)]
            pltpu.make_async_copy(part, part, sem.at[round_, number]).wait()

    def sum_finish(round_, number):
        sum_wait(round_, number, sum_recv)
        start = offset_of(round_, number)
        return tree_sum([shares_of[round_][start + peer] for peer in range(group_of(plans[round_][number])[0])])

    def sum_turn(round_):
        for number in range(1, len(plans[round_])):
            sum_start(round_, number, sum_finish(round_, number - 1))

    def sum_rest(round_):
        return sum_finish(round_, len(plans[round_]) - 1)

    def sum_left(round_):
        for number in range(len(plans[round_])):
            sum_wait(round_, number, sum_send)

    def loads_at(x, y):
        return stack[x, y, 0:cols, :]

    def image_at(x, y):
        return stack[x, y, cols:, :]

    square_part = gram(loads_at, loads_at)
    for round_ in range(1, vouches):
        vouched(round_ - 1)
        vouch(round_)
    if vouches:
        vouched(vouches - 1)
    moduli_copy.wait()

    def block_of(x, y):
        bx, lx = (0, nx - 1) if x == 0 else (2, 0) if x == nx + 1 else (1, x - 1)
        by, ly = (0, ny - 1) if y == 0 else (2, 0) if y == ny + 1 else (1, y - 1)
        return bx, by, lx * ny + ly

    odd = lax.rem(lane, 2) == 1

    def merged(edge):
        return {
            (bx, by): jnp.where(odd, edge[bx, by, 0].astype(F32), edge[bx, by, 1].astype(F32))
            for bx, by in itertools.product(range(3), repeat=2)
        }

    def tail_of(tiles, x, y, at=0):
        bx, by, row = block_of(x, y)
        return pltpu.roll(tiles[bx, by], (2 * LANES - at - 2 * row) % LANES, 1)

    def modulus_of(ids):
        return tree_sum([jnp.where(ids == float(number + 1), moduli_ref[number], 0.0) for number in range(mats)])

    halo_wait(0, halo_recv.at[0])
    full = nz + LANES
    tails = merged(ends_rx)
    flats = {key: modulus_of(mats_rx[key].astype(F32)) for key in tails}
    sides = {key: modulus_of(tile[0:8]) for key, tile in tails.items()}
    moduli = {}
    for x in xs:
        for y in ys:
            field[x, y] = jnp.concatenate([padded[x, y].astype(F32), tail_of(tails, x, y)], axis=1)
            bx, by, row = block_of(x, y)
            moduli[x, y] = jnp.concatenate([
                jnp.broadcast_to(flats[bx, by][row : row + 1, :], (8, nz)), tail_of(sides, x, y, IDS)
            ], axis=1)
    for x in range(nx + 1):
        for y in range(ny + 1):
            total = (moduli[x, y] + moduli[x, y + 1]) + (moduli[x + 1, y] + moduli[x + 1, y + 1])
            weight = 0.125 * (total + pltpu.roll(total, full - 1, 1))
            wt[x, y] = weight
            wtr[x, y] = pltpu.roll(weight, 1, 1)

    def double(tile):
        return jnp.concatenate([tile, tile], axis=0)

    def operate(direction_of, write):
        for x in range(nx):
            for y in range(ny):
                here = field[x + 1, y + 1]
                ahead = behind = flat = None
                w_ahead = w_behind = None
                for ex in (x, x + 1):
                    for ey in (y, y + 1):
                        corner_sum = (field[ex, ey] + field[ex, ey + 1]) + (field[ex + 1, ey] + field[ex + 1, ey + 1])
                        after, before = wt[ex, ey], wtr[ex, ey]
                        opposite = field[2 * ex - x, 2 * ey - y][:, 0:nz]
                        one = double(before) * corner_sum
                        two = double(after) * corner_sum
                        three = double((before + after)[:, 0:nz]) * opposite
                        ahead = one if ahead is None else ahead + one
                        behind = two if behind is None else behind + two
                        flat = three if flat is None else flat + three
                        w_ahead = before if w_ahead is None else w_ahead + before
                        w_behind = after if w_behind is None else w_behind + after
                ahead = ahead - double(w_ahead) * here
                behind = behind - double(w_behind) * here
                around = pltpu.roll(ahead, full - 1, 1)[:, 0:nz] + pltpu.roll(behind, 1, 1)[:, 0:nz] + flat
                centre = double((w_ahead + w_behind)[:, 0:nz]) * here[:, 0:nz]
                write(x, y, SIGMA * direction_of(x, y) + (k_far * around + k_self * centre))

    image_ends = [jnp.zeros((cols, LANES), F32)] * 2

    def write_first(x, y, image):
        stack[x, y, cols:, :] = image
        padded_im[x + 1, y + 1] = image.astype(BF16)
        image_ends[:] = spread(*image_ends, x * ny + y, image[:, 0:LANES], image[:, nz - LANES : nz], 0)

    operate(loads_at, write_first)
    ends_im[0] = image_ends[0].astype(BF16)
    ends_im[1] = image_ends[1].astype(BF16)
    halo_start(1)
    half = cols // 2
    both_part = gram(image_at, lambda x, y: stack[x, y])
    near_part = gram(image_at, lambda x, y: padded[x + 1, y + 1].astype(F32))
    parts = jnp.concatenate(
        [square_part, both_part, near_part, jnp.zeros((cols, LANES - 4 * cols), F32)], axis=1
    )
    sum_start(0, 0, jnp.where(lane < LANES // 2, parts[0:half], pltpu.roll(parts[half:], LANES // 2, 1)))
    sum_turn(0)

    halo_wait(1, halo_recv.at[1])
    tails_im = merged(ends_im_rx)
    for x in xs:
        for y in ys:
            inner = 1 <= x <= nx and 1 <= y <= ny
            value = image_at(x - 1, y - 1) if inner else padded_im[x, y].astype(F32)
            field[x, y] = jnp.concatenate([value, tail_of(tails_im, x, y)], axis=1)
    last_parts = []

    def write_last(x, y, image):
        last_parts.append(dot(image_at(x, y), image, 1, 1))

    operate(image_at, write_last)
    sum_start(1, 0, pack(tree_sum(last_parts)))

    tile = sum_rest(0)
    table = jnp.concatenate([tile, pltpu.roll(tile, LANES // 2, 1)], axis=0)
    square, cross, quad, near = (table[:, cols * k : cols * (k + 1)] for k in range(4))
    cross = 0.5 * (cross + cross.T)
    near = 0.5 * (near + near.T)
    row_id = lax.broadcasted_iota(jnp.int32, (cols, cols), 0)
    col_id = lax.broadcasted_iota(jnp.int32, (cols, cols), 1)
    eye = jnp.where(row_id == col_id, 1.0, 0.0)
    inverse = solve(square, eye)
    alpha = solve(cross, square)
    updated = square + dot(alpha, dot(quad, alpha, 1, 0) - cross, 0, 0) - dot(cross, alpha, 0, 0)
    grown = eye + dot(inverse, updated, 1, 0)
    alpha_t = alpha.T
    mix = jnp.concatenate([grown.T, -alpha_t], axis=1)
    mix_hi = mix.astype(BF16)
    mix_lo = (mix - mix_hi.astype(F32)).astype(BF16)
    mix_both = jnp.concatenate([mix_hi, mix_lo], axis=0)
    known = dot(grown, dot(near, grown, 1, 0) - dot(quad, alpha, 1, 0), 0, 0) - dot(alpha, dot(quad, grown, 1, 0), 0, 0)

    for x in xs:
        for y in ys:
            inner = 1 <= x <= nx and 1 <= y <= ny
            near_tail = jnp.concatenate([
                tail_of(tails, x, y).astype(BF16), tail_of(tails_im, x, y).astype(BF16)
            ], axis=0)
            if not inner:
                near_tail = jnp.concatenate([
                    jnp.concatenate([padded[x, y], padded_im[x, y]], axis=0), near_tail
                ], axis=1)
            twice = dot(mix_both, near_tail, 1, 0, None)
            mixed = twice[0:cols] + twice[cols:]
            if inner:
                direction = dot(mix, stack[x - 1, y - 1], 1, 0)
                pair_ref[x - 1, y - 1, 0:cols, :] = direction
                mixed = jnp.concatenate([direction, mixed], axis=1)
            field[x, y] = mixed.astype(BF16).astype(F32)

    def write_second(x, y, image):
        pair_ref[x, y, cols:, :] = image

    operate(lambda x, y: pair_ref[x, y, 0:cols, :], write_second)
    for x, y in own:
        base_ref[x, y, 0:cols, :] = dot(alpha_t, stack[x, y, 0:cols, :], 1, 0)
        base_ref[x, y, cols:, :] = stack[x, y, 0:cols, :] - dot(alpha_t, stack[x, y, cols:, :], 1, 0)
    halo_wait(0, halo_send.at[0])
    halo_wait(1, halo_send.at[1])
    sum_left(0)
    sum_turn(1)
    last = unpack(sum_rest(1), cols)
    total = known + dot(alpha, dot(last, alpha, 1, 0), 0, 0)
    coef_ref[...] = solve(0.5 * (total + total.T), updated).T
    sum_left(1)


def last_body(coef_ref, base_ref, pair_ref, sol_ref, res_ref, stage, sems):
    cols, nx, ny, nz = sol_ref.shape
    coef = coef_ref[...]
    for x, y in itertools.product(range(nx), range(ny)):
        for which, ref, sign in ((0, sol_ref, 1.0), (1, res_ref, -1.0)):
            rows = slice(which * cols, (which + 1) * cols)
            stage[which, x, y] = base_ref[x, y, rows, :] + sign * dot(coef, pair_ref[x, y, rows, :], 1, 0)
            pltpu.make_async_copy(stage.at[which, x, y], ref.at[:, x, y, :], sems.at[which]).start()
    for which in range(2):
        pltpu.make_async_copy(stage.at[which], stage.at[which], sems.at[which]).wait()


def on_device(sizes, loads, moduli, material):
    cols, nx, ny, nz = loads.shape
    count = int(np.prod(sizes))
    split = (("gx", "gy"), ("gz",))
    plans = (split, (AXES,) if count <= DIRECT_LIMIT else split)

    def slots(phases):
        return sum(int(np.prod([sizes[AXES.index(a)] for a in axes])) for axes in phases)

    vmem = pl.BlockSpec(memory_space=pltpu.VMEM)
    anywhere = pl.BlockSpec(memory_space=pl.ANY)
    full = nz + LANES
    credits = (nz // LANES) * 2 * (nx + ny + 2) + 18 + 8 * (nx * ny * nz // (cols * LANES))
    base, pair, coef = pl.pallas_call(
        functools.partial(main_body, sizes, plans, stiffness_values()),
        out_shape=(
            pltpu.VMEM((nx, ny, 2 * cols, nz), F32),
            pltpu.VMEM((nx, ny, 2 * cols, nz), F32),
            pltpu.VMEM((cols, cols), F32),
        ),
        in_specs=[anywhere, anywhere, anywhere],
        out_specs=(vmem, vmem, vmem),
        scratch_shapes=[
            pltpu.VMEM((nx, ny, 2 * cols, nz), F32),
            pltpu.VMEM((nx + 2, ny + 2, cols, nz), BF16),
            pltpu.VMEM((nx + 2, ny + 2, cols, nz), BF16),
            pltpu.VMEM((3, 3, nx * ny, nz), BF16),
            pltpu.VMEM((2, cols, LANES), BF16),
            pltpu.VMEM((3, 3, 2, cols, LANES), BF16),
            pltpu.VMEM((2, cols, LANES), BF16),
            pltpu.VMEM((3, 3, 2, cols, LANES), BF16),
            pltpu.VMEM((nx + 2, ny + 2, cols, full), F32),
            pltpu.VMEM((nx + 1, ny + 1, 8, full), F32),
            pltpu.VMEM((nx + 1, ny + 1, 8, full), F32),
            pltpu.VMEM((slots(plans[0]), cols // 2, LANES), F32),
            pltpu.VMEM((slots(plans[1]), cols * cols // LANES, LANES), F32),
            pltpu.SMEM(moduli.shape, F32),
            pltpu.VMEM(material.shape, jnp.int32),
            pltpu.VMEM((credits, cols, LANES), BF16),
            pltpu.SemaphoreType.DMA((2,)),
            pltpu.SemaphoreType.DMA((2,)),
            pltpu.SemaphoreType.DMA((2, 2)),
            pltpu.SemaphoreType.DMA((2, 2)),
            pltpu.SemaphoreType.DMA((3,)),
            pltpu.SemaphoreType.REGULAR((max(sizes[2] - 2, 1) if count <= DIRECT_LIMIT else 1, 2)),
        ],
        compiler_params=pltpu.CompilerParams(collective_id=0, has_side_effects=True),
    )(moduli, loads, material)
    out = jax.ShapeDtypeStruct(loads.shape, F32)
    return pl.pallas_call(
        last_body,
        out_shape=(out, out),
        in_specs=[vmem, vmem, vmem],
        out_specs=(anywhere, anywhere),
        scratch_shapes=[pltpu.VMEM((2, nx, ny, cols, nz), F32), pltpu.SemaphoreType.DMA((2,))],
        compiler_params=pltpu.CompilerParams(vmem_limit_bytes=4 * 2**20),
    )(coef, base, pair)


def solution(mesh):
    sizes = tuple(mesh.shape[axis] for axis in AXES)
    in_specs = (P(None, "gx", "gy", "gz"), P(), P("gx", "gy", "gz"))
    out_specs = (P(None, "gx", "gy", "gz"), P(None, "gx", "gy", "gz"))
    return jax.shard_map(
        functools.partial(on_device, sizes), mesh=mesh, in_specs=in_specs, out_specs=out_specs, check_vma=False
    )
```

```python
import functools
import itertools

import jax
import jax.numpy as jnp
import numpy as np
from jax import lax
from jax.experimental import pallas as pl
from jax.experimental.pallas import tpu as pltpu
from jax.sharding import PartitionSpec as P

SIGMA = 0.25
AXES = ("gx", "gy", "gz")
HIGH = lax.Precision.HIGHEST
F32 = jnp.float32
BF16 = jnp.bfloat16
LANES = 128
DIRECT_LIMIT = 32
IDS = 64


def stiffness_values():
    mass = (1.0 / 3.0, 1.0 / 6.0)
    stiff = (1.0, -1.0)
    values = []
    for differing in range(4):
        bits = [1 if dim < differing else 0 for dim in range(3)]
        total = 0.0
        for dim in range(3):
            factor = 1.0
            for other in range(3):
                factor *= stiff[bits[other]] if other == dim else mass[bits[other]]
            total += factor
        values.append(float(np.asarray(total, np.float32).astype(jnp.bfloat16).astype(np.float32)))
    return values


def dot(left, right, left_dim, right_dim, precision=HIGH):
    return lax.dot_general(
        left, right, (((left_dim,), (right_dim,)), ((), ())), precision=precision, preferred_element_type=F32
    )


def pack(matrix):
    rows, cols = matrix.shape
    wide = jnp.concatenate([matrix, jnp.zeros((rows, LANES - cols), F32)], axis=1)
    pieces = [
        jnp.sum(pltpu.roll(wide[start : start + 8], 0, 1, stride=cols, stride_axis=0), axis=0, keepdims=True)
        for start in range(0, rows, 8)
    ]
    return jnp.concatenate(pieces, axis=0)


def unpack(tile, cols):
    rows = tile.shape[0]
    tall = jnp.concatenate([tile, jnp.zeros((8 - rows, LANES), F32)], axis=0)
    turned = [tall] + [pltpu.roll(tall, LANES - cols * group, 1) for group in range(1, 8)]
    return jnp.concatenate(
        [turned[group][row : row + 1] for row in range(rows) for group in range(8)], axis=0
    )[:, 0:cols]


def solve(matrix, rhs):
    size = matrix.shape[0]
    wide = jnp.concatenate([rhs, jnp.zeros((size, LANES - rhs.shape[1]), F32)], axis=1)
    left = [jnp.broadcast_to(matrix[:, i : i + 1], (size, LANES)) for i in range(size)]
    right = [wide[i : i + 1, :] for i in range(size)]
    start = 0
    for step in range(size):
        if step == size // 2 and step % 8 == 0:
            left = [row[step:, :] for row in left]
            start = step
        at = step - start
        scale = 1.0 / left[step][at : at + 1, :]
        pivot, pivot_right = left[step] * scale, right[step] * scale
        for i in range(size):
            if i != step:
                factor = left[i][at : at + 1, :]
                left[i] = left[i] - factor * pivot
                right[i] = right[i] - factor * pivot_right
        left[step], right[step] = pivot, pivot_right
    return jnp.concatenate(right, axis=0)[:, 0 : rhs.shape[1]]


def tree_sum(terms):
    while len(terms) > 1:
        terms = [a + b for a, b in zip(terms[0::2], terms[1::2])] + terms[len(terms) & ~1 :]
    return terms[0]


def main_body(sizes, plans, stiff, moduli_hbm, loads_ref, mat_hbm, base_ref, pair_ref, coef_ref,
              stack, padded, padded_im, mats_rx, ends, ends_rx, ends_im, ends_im_rx, field, wt, wtr,
              shares_square, shares_table, shares_last, tail_im, moduli_ref, mat_ref, credit,
              halo_send, halo_recv, sum_send, sum_recv, local_sems, vouch_sem):
    cols, nx, ny, nz = loads_ref.shape
    mats = moduli_ref.shape[0]
    me = [lax.axis_index(axis) for axis in AXES]
    k_self, k_edge, k_far = stiff[0], stiff[1], stiff[2]
    assert k_edge == 0.0 and stiff[2] == stiff[3]
    assert 4 * nx * ny <= IDS and (nx * ny * nz) % (cols * LANES) == 0 and nz % LANES == 0
    xs, ys = range(nx + 2), range(ny + 2)
    shares_of = (shares_square, shares_table, shares_last)
    own = list(itertools.product(range(nx), range(ny)))

    directions = [
        d for d in itertools.product((-1, 0, 1), repeat=3)
        if any(d) and all(step == 0 or sizes[i] > 1 for i, step in enumerate(d))
    ]
    directions.sort(key=lambda d: -sum(abs(step) for step in d))

    def exists(direction):
        good = None
        for i, step in enumerate(direction):
            if step:
                here = (me[i] > 0) if step < 0 else (me[i] < sizes[i] - 1)
                good = here if good is None else jnp.logical_and(good, here)
        return good

    def target(direction):
        return {axis: me[i] + direction[i] for i, axis in enumerate(AXES)}

    def place(direction):
        return 1 - direction[0], 1 - direction[1]

    def halo_start(round_):
        core = (padded, padded_im)[round_]
        for direction in directions:
            dx, dy, dz = direction
            pairs = []
            if dz == 0:
                src_x = {0: pl.ds(1, nx), 1: pl.ds(nx, 1), -1: pl.ds(1, 1)}[dx]
                dst_x = {0: pl.ds(1, nx), 1: pl.ds(0, 1), -1: pl.ds(nx + 1, 1)}[dx]
                src_y = {0: pl.ds(1, ny), 1: pl.ds(ny, 1), -1: pl.ds(1, 1)}[dy]
                dst_y = {0: pl.ds(1, ny), 1: pl.ds(0, 1), -1: pl.ds(ny + 1, 1)}[dy]
                pairs.append((core.at[src_x, src_y], core.at[dst_x, dst_y]))
                if round_ == 0:
                    pairs.append((mats_rx.at[1, 1], mats_rx.at[place(direction)]))
                else:
                    pairs.insert(0, (ends_im, ends_im_rx.at[place(direction)]))
            elif round_ == 0:
                pairs.append((ends.at[1 if dz > 0 else 0], ends_rx.at[(*place(direction), 0 if dz > 0 else 1)]))
            else:
                continue

            @pl.when(exists(direction))
            def _():
                for src, dst in pairs:
                    pltpu.make_async_remote_copy(
                        src_ref=src, dst_ref=dst, send_sem=halo_send.at[round_], recv_sem=halo_recv.at[round_],
                        device_id=target(direction), device_id_type=pl.DeviceIdType.MESH,
                    ).start()

    def halo_wait(round_, sem):
        numbers = [
            ((me[i] > 0).astype(jnp.int32) + (me[i] < sizes[i] - 1).astype(jnp.int32)) for i in range(3)
        ]
        choices = [(0,) if size == 1 else (1,) if size == 2 else (1, 2) for size in sizes]
        per = nz // LANES
        for cx, cy, cz in itertools.product(*choices):
            total = per * (cx * ny + cy * nx + cx * cy)
            if round_ == 0:
                total += (cx + cy + cx * cy) * (nx * ny * nz // (cols * LANES)) + cz * (1 + cx) * (1 + cy)
            else:
                total += cx + cy + cx * cy
            if total:
                tests = [numbers[i] == c for i, c in enumerate((cx, cy, cz)) if len(choices[i]) > 1]

                def take():
                    part = credit.at[pl.ds(0, total)]
                    pltpu.make_async_copy(part, part, sem).wait()

                if tests:
                    pl.when(functools.reduce(jnp.logical_and, tests))(take)
                else:
                    take()

    def each(count, body):
        if count <= 8:
            for k in range(1, count):
                body(k, 0)
        else:
            lax.fori_loop(1, count, body, 0)

    def group_of(axes):
        count, index = 1, 0
        for axis in axes:
            i = AXES.index(axis)
            count *= sizes[i]
            index = index * sizes[i] + me[i]
        return count, index

    def peer_id(axes, peer):
        coords = {axis: me[i] for i, axis in enumerate(AXES)}
        for axis in reversed(axes):
            size = sizes[AXES.index(axis)]
            coords[axis] = lax.rem(peer, size)
            peer = lax.div(peer, size)
        return coords

    def offset_of(round_, number):
        return sum(group_of(axes)[0] for axes in plans[round_][:number])

    direct = (AXES,) in plans

    for bx, by in itertools.product(range(3), repeat=2):
        for side in range(2):
            ends_rx[bx, by, side] = jnp.zeros(ends_rx.shape[3:], BF16)
        if (bx, by) != (1, 1):
            ends_im_rx[bx, by] = jnp.zeros(ends_im_rx.shape[2:], BF16)
            mats_rx[bx, by] = jnp.zeros(mats_rx.shape[2:], BF16)
    for x in xs:
        for y in ys:
            if not (1 <= x <= nx and 1 <= y <= ny):
                padded[x, y] = jnp.zeros(padded.shape[2:], BF16)
                padded_im[x, y] = jnp.zeros(padded_im.shape[2:], BF16)

    barrier = pltpu.get_barrier_semaphore()
    expected = 0
    if direct:
        flat = sizes[0] * sizes[1]
        spot = me[0] * sizes[1] + me[1]
        for dz in (-1, 0, 1):
            good = True if dz == 0 else exists((0, 0, dz))

            def greet(k, carry, dz=dz):
                there = lax.rem(spot + k, flat)
                pl.semaphore_signal(
                    barrier, inc=1, device_id_type=pl.DeviceIdType.MESH,
                    device_id={"gx": lax.div(there, sizes[1]), "gy": lax.rem(there, sizes[1]), "gz": me[2] + dz},
                )
                return carry

            if dz == 0:
                each(flat, greet)
                expected = expected + flat - 1
            elif sizes[2] > 1:
                @pl.when(good)
                def _():
                    greet(0, 0)
                    each(flat, greet)
                expected = expected + jnp.where(good, flat, 0)
    else:
        for axes in plans[0]:
            count, index = group_of(axes)

            def greet(k, carry, axes=axes, count=count, index=index):
                pl.semaphore_signal(barrier, inc=1, device_id=peer_id(axes, lax.rem(index + k, count)),
                                    device_id_type=pl.DeviceIdType.MESH)
                return carry

            each(count, greet)
            expected = expected + count - 1
        for direction in directions:
            good = exists(direction)

            @pl.when(good)
            def _():
                pl.semaphore_signal(barrier, inc=1, device_id=target(direction),
                                    device_id_type=pl.DeviceIdType.MESH)
            expected = expected + jnp.where(good, 1, 0)

    for x, y in own:
        pltpu.make_async_copy(loads_ref.at[:, x, y, :], stack.at[x, y, pl.ds(0, cols), :], local_sems.at[0]).start()
    mat_copy = pltpu.make_async_copy(mat_hbm, mat_ref, local_sems.at[1])
    mat_copy.start()
    moduli_copy = pltpu.make_async_copy(moduli_hbm, moduli_ref, local_sems.at[2])
    moduli_copy.start()

    vouches = max(sizes[2] - 2, 0) if direct else 0

    def vouch(round_):
        for dz in (-1, 1):
            @pl.when(exists((0, 0, dz)))
            def _():
                pl.semaphore_signal(vouch_sem.at[round_, 0 if dz > 0 else 1], inc=1, device_id=target((0, 0, dz)),
                                    device_id_type=pl.DeviceIdType.MESH)

    def vouched(round_):
        for dz in (-1, 1):
            @pl.when(exists((0, 0, dz)))
            def _():
                pl.semaphore_wait(vouch_sem.at[round_, 1 if dz > 0 else 0], 1)

    lane = lax.broadcasted_iota(jnp.int32, (1, LANES), 1)

    def spread(firsts, lasts, row, first, last, at):
        spot = at + 4 * row
        ahead = jnp.logical_and(lane >= spot, lane < spot + 2)
        start = (spot - 2) % LANES
        behind = jnp.logical_and(lane >= start, lane < start + 2)
        return (jnp.where(ahead, pltpu.roll(first, spot, 1), firsts),
                jnp.where(behind, pltpu.roll(last, spot, 1), lasts))

    mat_copy.wait()
    ids = jnp.concatenate([mat_ref[x] for x in range(nx)], axis=0)
    ids = (ids + 1).astype(F32)
    mats_rx[1, 1] = ids.astype(BF16)
    firsts = lasts = jnp.zeros((cols, LANES), F32)
    for x, y in own:
        row = x * ny + y
        first = jnp.broadcast_to(ids[row : row + 1, 0:LANES], (cols, LANES))
        last = jnp.broadcast_to(ids[row : row + 1, nz - LANES : nz], (cols, LANES))
        firsts, lasts = spread(firsts, lasts, row, first, last, IDS)
    whole = stack.at[:, :, pl.ds(0, cols), :]
    pltpu.make_async_copy(whole, whole, local_sems.at[0]).wait()
    for x, y in own:
        values = stack[x, y, 0:cols, :]
        padded[x + 1, y + 1] = values.astype(BF16)
        firsts, lasts = spread(firsts, lasts, x * ny + y, values[:, 0:LANES], values[:, nz - LANES : nz], 0)
    ends[0] = firsts.astype(BF16)
    ends[1] = lasts.astype(BF16)
    pl.semaphore_wait(barrier, expected)
    halo_start(0)
    if vouches:
        vouch(0)

    def gram(left, right):
        return tree_sum([dot(left(x, y), right(x, y), 1, 1) for x, y in own])

    def sum_copy(round_, number, peer):
        axes = plans[round_][number]
        count, index = group_of(axes)
        slot = offset_of(round_, number) + index
        return pltpu.make_async_remote_copy(
            src_ref=shares_of[round_].at[slot], dst_ref=shares_of[round_].at[slot],
            send_sem=sum_send.at[round_, number], recv_sem=sum_recv.at[round_, number],
            device_id=peer, device_id_type=pl.DeviceIdType.MESH,
        )

    def sum_start(round_, number, tile):
        axes = plans[round_][number]
        count, index = group_of(axes)
        shares_of[round_][offset_of(round_, number) + index] = tile
        if axes == AXES:
            plane = []
            for k in range(flat):
                there = lax.rem(spot + k, flat)
                plane.append((lax.div(there, sizes[1]), lax.rem(there, sizes[1])))
            low = 2 * me[2] < sizes[2]
            far, turn = jnp.where(low, sizes[2] - 1, 0), jnp.where(low, -1, 1)
            away = jnp.where(low, sizes[2] - 1 - me[2], me[2])
            for i in range(sizes[2] - 1):
                level = far + turn * (i + jnp.where(i < away, 0, 1))
                for gx, gy in plane[::-1]:
                    sum_copy(round_, number, {"gx": gx, "gy": gy, "gz": level}).start()
            for gx, gy in plane[:0:-1]:
                sum_copy(round_, number, {"gx": gx, "gy": gy, "gz": me[2]}).start()
        else:
            def send(k, carry):
                sum_copy(round_, number, peer_id(axes, lax.rem(index + k, count))).start()
                return carry

            each(count, send)

    def sum_wait(round_, number, sem):
        count, _ = group_of(plans[round_][number])
        if count > 1:
            part = shares_of[round_].at[pl.ds(0, count - 1)]
            pltpu.make_async_copy(part, part, sem.at[round_, number]).wait()

    def sum_finish(round_, number):
        sum_wait(round_, number, sum_recv)
        start = offset_of(round_, number)
        return tree_sum([shares_of[round_][start + peer] for peer in range(group_of(plans[round_][number])[0])])

    def sum_turn(round_):
        for number in range(1, len(plans[round_])):
            sum_start(round_, number, sum_finish(round_, number - 1))

    def sum_rest(round_):
        return sum_finish(round_, len(plans[round_]) - 1)

    def sum_left(round_):
        for number in range(len(plans[round_])):
            sum_wait(round_, number, sum_send)

    def loads_at(x, y):
        return stack[x, y, 0:cols, :]

    def image_at(x, y):
        return stack[x, y, cols:, :]

    square_part = gram(loads_at, loads_at)
    sum_start(0, 0, pack(square_part))
    for round_ in range(1, vouches):
        vouched(round_ - 1)
        vouch(round_)
    moduli_copy.wait()

    def block_of(x, y):
        bx, lx = (0, nx - 1) if x == 0 else (2, 0) if x == nx + 1 else (1, x - 1)
        by, ly = (0, ny - 1) if y == 0 else (2, 0) if y == ny + 1 else (1, y - 1)
        return bx, by, lx * ny + ly

    odd = lax.rem(lane, 4) >= 2

    def merged(edge):
        return {
            (bx, by): jnp.where(odd, edge[bx, by, 0].astype(F32), edge[bx, by, 1].astype(F32))
            for bx, by in itertools.product(range(3), repeat=2)
        }

    def tail_of(tiles, x, y, at=0):
        bx, by, row = block_of(x, y)
        return pltpu.roll(tiles[bx, by], (2 * LANES - at - 4 * row) % LANES, 1)

    def modulus_of(ids):
        return tree_sum([jnp.where(ids == float(number + 1), moduli_ref[number], 0.0) for number in range(mats)])

    halo_wait(0, halo_recv.at[0])
    full = nz + LANES
    tails = merged(ends_rx)
    flats = {key: modulus_of(mats_rx[key].astype(F32)) for key in tails}
    sides = {key: modulus_of(tile[0:8]) for key, tile in tails.items()}
    moduli = {}
    for x in xs:
        for y in ys:
            field[x, y] = jnp.concatenate([padded[x, y].astype(F32), tail_of(tails, x, y)], axis=1)
            bx, by, row = block_of(x, y)
            moduli[x, y] = jnp.concatenate([
                jnp.broadcast_to(flats[bx, by][row : row + 1, :], (8, nz)), tail_of(sides, x, y, IDS)
            ], axis=1)
    for x in range(nx + 1):
        for y in range(ny + 1):
            total = (moduli[x, y] + moduli[x, y + 1]) + (moduli[x + 1, y] + moduli[x + 1, y + 1])
            weight = 0.125 * (total + pltpu.roll(total, full - 1, 1))
            wt[x, y] = weight
            wtr[x, y] = pltpu.roll(weight, 1, 1)

    def double(tile):
        return jnp.concatenate([tile, tile], axis=0)

    def operate(direction_of, write, width=None):
        width = width or nz
        for x in range(nx):
            for y in range(ny):
                here = field[x + 1, y + 1]
                ahead = behind = flat = None
                w_ahead = w_behind = None
                for ex in (x, x + 1):
                    for ey in (y, y + 1):
                        corner_sum = (field[ex, ey] + field[ex, ey + 1]) + (field[ex + 1, ey] + field[ex + 1, ey + 1])
                        after, before = wt[ex, ey], wtr[ex, ey]
                        opposite = field[2 * ex - x, 2 * ey - y][:, 0:width]
                        one = double(before) * corner_sum
                        two = double(after) * corner_sum
                        three = double((before + after)[:, 0:width]) * opposite
                        ahead = one if ahead is None else ahead + one
                        behind = two if behind is None else behind + two
                        flat = three if flat is None else flat + three
                        w_ahead = before if w_ahead is None else w_ahead + before
                        w_behind = after if w_behind is None else w_behind + after
                ahead = ahead - double(w_ahead) * here
                behind = behind - double(w_behind) * here
                around = pltpu.roll(ahead, full - 1, 1)[:, 0:width] + pltpu.roll(behind, 1, 1)[:, 0:width] + flat
                centre = double((w_ahead + w_behind)[:, 0:width]) * here[:, 0:width]
                write(x, y, SIGMA * direction_of(x, y) + (k_far * around + k_self * centre))

    has_right = (me[2] < sizes[2] - 1).astype(jnp.int32)
    has_left = (me[2] > 0).astype(jnp.int32)
    beyond = jnp.logical_or(lane < has_right, lane >= LANES - has_left)
    image_ends = [jnp.zeros((cols, LANES), F32)]

    def write_first(x, y, image):
        row = x * ny + y
        stack[x, y, cols:, :] = image[:, 0:nz]
        padded_im[x + 1, y + 1] = image[:, 0:nz].astype(BF16)
        tail = jnp.where(beyond, image[:, nz:], 0.0)
        tail_im[x, y] = tail
        turned = pltpu.roll(tail, 4 * row, 1)
        image_ends[0] = image_ends[0] + turned

    operate(lambda x, y: jnp.concatenate([loads_at(x, y), field[x + 1, y + 1][:, nz:]], axis=1), write_first, full)
    ends_im[...] = image_ends[0].astype(BF16)
    halo_start(1)
    both_part = gram(image_at, lambda x, y: stack[x, y])
    if vouches:
        vouched(vouches - 1)
    sum_start(1, 0, jnp.concatenate([pack(both_part[:, 0:cols]), pack(both_part[:, cols:])], axis=0))
    sum_turn(0)

    halo_wait(1, halo_recv.at[1])
    turned_im = {}
    for x in xs:
        for y in ys:
            if 1 <= x <= nx and 1 <= y <= ny:
                turned_im[x, y] = tail_im[x - 1, y - 1]
            else:
                bx, by, row = block_of(x, y)
                turned_im[x, y] = pltpu.roll(ends_im_rx[bx, by].astype(F32), (LANES - 4 * row) % LANES, 1)
    for x in xs:
        for y in ys:
            inner = 1 <= x <= nx and 1 <= y <= ny
            value = image_at(x - 1, y - 1) if inner else padded_im[x, y].astype(F32)
            field[x, y] = jnp.concatenate([value, turned_im[x, y]], axis=1)
    last_parts = []

    def write_last(x, y, image):
        last_parts.append(dot(image_at(x, y), image, 1, 1))

    operate(image_at, write_last)
    sum_start(2, 0, pack(tree_sum(last_parts)))

    square = unpack(sum_rest(0), cols)
    sum_turn(1)
    row_id = lax.broadcasted_iota(jnp.int32, (cols, cols), 0)
    col_id = lax.broadcasted_iota(jnp.int32, (cols, cols), 1)
    eye = jnp.where(row_id == col_id, 1.0, 0.0)
    inverse = solve(square, eye)
    table = sum_rest(1)
    half = table.shape[0] // 2
    cross, quad = unpack(table[0:half], cols), unpack(table[half:], cols)
    cross = 0.5 * (cross + cross.T)
    alpha = solve(cross, square)
    updated = square + dot(alpha, dot(quad, alpha, 1, 0) - cross, 0, 0) - dot(cross, alpha, 0, 0)
    grown = eye + dot(inverse, updated, 1, 0)
    alpha_t = alpha.T
    mix = jnp.concatenate([grown.T, -alpha_t], axis=1)
    mix_hi = mix.astype(BF16)
    mix_lo = (mix - mix_hi.astype(F32)).astype(BF16)
    mix_both = jnp.concatenate([mix_hi, mix_lo], axis=0)
    known = dot(grown, dot(cross, grown, 1, 0) - dot(quad, alpha, 1, 0), 0, 0) - dot(alpha, dot(quad, grown, 1, 0), 0, 0)

    known = 0.5 * (known + known.T)

    for x in xs:
        for y in ys:
            inner = 1 <= x <= nx and 1 <= y <= ny
            near_tail = jnp.concatenate([
                tail_of(tails, x, y).astype(BF16), turned_im[x, y].astype(BF16)
            ], axis=0)
            if not inner:
                near_tail = jnp.concatenate([
                    jnp.concatenate([padded[x, y], padded_im[x, y]], axis=0), near_tail
                ], axis=1)
            twice = dot(mix_both, near_tail, 1, 0, None)
            mixed = twice[0:cols] + twice[cols:]
            if inner:
                direction = dot(mix, stack[x - 1, y - 1], 1, 0)
                pair_ref[x - 1, y - 1, 0:cols, :] = direction
                mixed = jnp.concatenate([direction, mixed], axis=1)
            field[x, y] = mixed.astype(BF16).astype(F32)

    def write_second(x, y, image):
        pair_ref[x, y, cols:, :] = image

    operate(lambda x, y: pair_ref[x, y, 0:cols, :], write_second)
    for x, y in own:
        base_ref[x, y, 0:cols, :] = dot(alpha_t, stack[x, y, 0:cols, :], 1, 0)
        base_ref[x, y, cols:, :] = stack[x, y, 0:cols, :] - dot(alpha_t, stack[x, y, cols:, :], 1, 0)
    halo_wait(0, halo_send.at[0])
    halo_wait(1, halo_send.at[1])
    sum_left(0)
    sum_left(1)
    sum_turn(2)
    last = unpack(sum_rest(2), cols)
    turned = dot(alpha_t, last, 1, 0) + dot(alpha_t, last, 1, 1)
    coef_ref[...] = solve(known + 0.5 * dot(turned, alpha, 1, 0), updated).T
    sum_left(2)


def last_body(coef_ref, base_ref, pair_ref, sol_ref, res_ref, stage, sems):
    cols, nx, ny, nz = sol_ref.shape
    coef = coef_ref[...]
    for x in range(nx):
        for which, ref, sign in ((0, sol_ref, 1.0), (1, res_ref, -1.0)):
            rows = slice(which * cols, (which + 1) * cols)
            for y in range(ny):
                stage[which, :, x, y, :] = (
                    base_ref[x, y, rows, :] + sign * dot(coef, pair_ref[x, y, rows, :], 1, 0)
                )
            pltpu.make_async_copy(stage.at[which, :, x], ref.at[:, x], sems.at[which]).start()
    for which in range(2):
        pltpu.make_async_copy(stage.at[which], stage.at[which], sems.at[which]).wait()


def on_device(sizes, loads, moduli, material):
    cols, nx, ny, nz = loads.shape
    count = int(np.prod(sizes))
    split = (("gx", "gy"), ("gz",))
    quick = (AXES,) if count <= DIRECT_LIMIT else split
    plans = (split, quick, quick)

    def slots(phases):
        return sum(int(np.prod([sizes[AXES.index(a)] for a in axes])) for axes in phases)

    vmem = pl.BlockSpec(memory_space=pltpu.VMEM)
    anywhere = pl.BlockSpec(memory_space=pl.ANY)
    full = nz + LANES
    credits = (nz // LANES) * 2 * (nx + ny + 2) + 18 + 8 * (nx * ny * nz // (cols * LANES))
    base, pair, coef = pl.pallas_call(
        functools.partial(main_body, sizes, plans, stiffness_values()),
        out_shape=(
            pltpu.VMEM((nx, ny, 2 * cols, nz), F32),
            pltpu.VMEM((nx, ny, 2 * cols, nz), F32),
            pltpu.VMEM((cols, cols), F32),
        ),
        in_specs=[anywhere, anywhere, anywhere],
        out_specs=(vmem, vmem, vmem),
        scratch_shapes=[
            pltpu.VMEM((nx, ny, 2 * cols, nz), F32),
            pltpu.VMEM((nx + 2, ny + 2, cols, nz), BF16),
            pltpu.VMEM((nx + 2, ny + 2, cols, nz), BF16),
            pltpu.VMEM((3, 3, nx * ny, nz), BF16),
            pltpu.VMEM((2, cols, LANES), BF16),
            pltpu.VMEM((3, 3, 2, cols, LANES), BF16),
            pltpu.VMEM((cols, LANES), BF16),
            pltpu.VMEM((3, 3, cols, LANES), BF16),
            pltpu.VMEM((nx + 2, ny + 2, cols, full), F32),
            pltpu.VMEM((nx + 1, ny + 1, 8, full), F32),
            pltpu.VMEM((nx + 1, ny + 1, 8, full), F32),
            pltpu.VMEM((slots(plans[0]), cols * cols // LANES, LANES), F32),
            pltpu.VMEM((slots(plans[1]), 2 * cols * cols // LANES, LANES), F32),
            pltpu.VMEM((slots(plans[2]), cols * cols // LANES, LANES), F32),
            pltpu.VMEM((nx, ny, cols, LANES), F32),
            pltpu.SMEM(moduli.shape, F32),
            pltpu.VMEM(material.shape, jnp.int32),
            pltpu.VMEM((credits, cols, LANES), BF16),
            pltpu.SemaphoreType.DMA((2,)),
            pltpu.SemaphoreType.DMA((2,)),
            pltpu.SemaphoreType.DMA((3, 2)),
            pltpu.SemaphoreType.DMA((3, 2)),
            pltpu.SemaphoreType.DMA((3,)),
            pltpu.SemaphoreType.REGULAR((max(sizes[2] - 2, 1) if count <= DIRECT_LIMIT else 1, 2)),
        ],
        compiler_params=pltpu.CompilerParams(collective_id=0, has_side_effects=True),
    )(moduli, loads, material)
    out = jax.ShapeDtypeStruct(loads.shape, F32)
    return pl.pallas_call(
        last_body,
        out_shape=(out, out),
        in_specs=[vmem, vmem, vmem],
        out_specs=(anywhere, anywhere),
        scratch_shapes=[pltpu.VMEM((2, cols, nx, ny, nz), F32), pltpu.SemaphoreType.DMA((2,))],
        compiler_params=pltpu.CompilerParams(vmem_limit_bytes=4 * 2**20),
    )(coef, base, pair)


def solution(mesh):
    sizes = tuple(mesh.shape[axis] for axis in AXES)
    in_specs = (P(None, "gx", "gy", "gz"), P(), P("gx", "gy", "gz"))
    out_specs = (P(None, "gx", "gy", "gz"), P(None, "gx", "gy", "gz"))
    return jax.shard_map(
        functools.partial(on_device, sizes), mesh=mesh, in_specs=in_specs, out_specs=out_specs, check_vma=False
    )
```

```python
import functools
import itertools

import jax
import jax.numpy as jnp
import numpy as np
from jax import lax
from jax.experimental import pallas as pl
from jax.experimental.pallas import tpu as pltpu
from jax.sharding import PartitionSpec as P

SIGMA = 0.25
AXES = ("gx", "gy", "gz")
HIGH = lax.Precision.HIGHEST
F32 = jnp.float32
BF16 = jnp.bfloat16
LANES = 128
DIRECT_LIMIT = 32
IDS = 64
TILE_UNITS = 64


def stiffness_values():
    mass = (1.0 / 3.0, 1.0 / 6.0)
    stiff = (1.0, -1.0)
    values = []
    for differing in range(4):
        bits = [1 if dim < differing else 0 for dim in range(3)]
        total = 0.0
        for dim in range(3):
            factor = 1.0
            for other in range(3):
                factor *= stiff[bits[other]] if other == dim else mass[bits[other]]
            total += factor
        values.append(float(np.asarray(total, np.float32).astype(jnp.bfloat16).astype(np.float32)))
    return values


def dot(left, right, left_dim, right_dim, precision=HIGH):
    return lax.dot_general(
        left, right, (((left_dim,), (right_dim,)), ((), ())), precision=precision, preferred_element_type=F32
    )


def pack(matrix):
    rows, cols = matrix.shape
    wide = jnp.concatenate([matrix, jnp.zeros((rows, LANES - cols), F32)], axis=1)
    pieces = [
        jnp.sum(pltpu.roll(wide[start : start + 8], 0, 1, stride=cols, stride_axis=0), axis=0, keepdims=True)
        for start in range(0, rows, 8)
    ]
    return jnp.concatenate(pieces, axis=0)


def unpack(tile, cols):
    rows = tile.shape[0]
    tall = jnp.concatenate([tile, jnp.zeros((8 - rows, LANES), F32)], axis=0)
    turned = [tall] + [pltpu.roll(tall, LANES - cols * group, 1) for group in range(1, 8)]
    return jnp.concatenate(
        [turned[group][row : row + 1] for row in range(rows) for group in range(8)], axis=0
    )[:, 0:cols]


def solve(matrix, rhs):
    size = matrix.shape[0]
    wide = jnp.concatenate([rhs, jnp.zeros((size, LANES - rhs.shape[1]), F32)], axis=1)
    left = [jnp.broadcast_to(matrix[:, i : i + 1], (size, LANES)) for i in range(size)]
    right = [wide[i : i + 1, :] for i in range(size)]
    start = 0
    for step in range(size):
        if step == size // 2 and step % 8 == 0:
            left = [row[step:, :] for row in left]
            start = step
        at = step - start
        scale = 1.0 / left[step][at : at + 1, :]
        pivot, pivot_right = left[step] * scale, right[step] * scale
        for i in range(size):
            if i != step:
                factor = left[i][at : at + 1, :]
                left[i] = left[i] - factor * pivot
                right[i] = right[i] - factor * pivot_right
        left[step], right[step] = pivot, pivot_right
    return jnp.concatenate(right, axis=0)[:, 0 : rhs.shape[1]]


def halves(value):
    high = value.astype(BF16)
    return high, (value - high.astype(F32)).astype(BF16)


def split_dot(left_high, left_low, right_high, right_low, left_dim, right_dim):
    rows = left_high.shape[0]
    both = dot(jnp.concatenate([left_high, left_low], axis=0), right_high, left_dim, right_dim, None)
    return both[0:rows] + both[rows:] + dot(left_high, right_low, left_dim, right_dim, None)


def tree_sum(terms):
    while len(terms) > 1:
        terms = [a + b for a, b in zip(terms[0::2], terms[1::2])] + terms[len(terms) & ~1 :]
    return terms[0]


def main_body(sizes, plans, stiff, moduli_hbm, loads_ref, mat_hbm, base_ref, pair_ref, coef_ref,
              stack, low, padded, padded_im, mats_rx, ends, ends_rx, ends_im, ends_im_rx, field, wt, wtr, level, node,
              shares_square, shares_table, shares_last, tail_im, moduli_ref, mat_ref, credit,
              sent, halo_recv, sum_recv, local_sems, vouch_sem):
    cols, nx, ny, nz = loads_ref.shape
    mats = moduli_ref.shape[0]
    me = [lax.axis_index(axis) for axis in AXES]
    k_self, k_edge, k_far = stiff[0], stiff[1], stiff[2]
    assert k_edge == 0.0 and stiff[2] == stiff[3]
    assert 4 * nx * ny <= IDS and (nx * ny * nz) % (cols * LANES) == 0 and nz % LANES == 0 and TILE_UNITS % cols == 0
    xs, ys = range(nx + 2), range(ny + 2)
    shares_of = (shares_square, shares_table, shares_last)
    own = list(itertools.product(range(nx), range(ny)))

    directions = [
        d for d in itertools.product((-1, 0, 1), repeat=3)
        if any(d) and all(step == 0 or sizes[i] > 1 for i, step in enumerate(d))
    ]
    directions.sort(key=lambda d: -sum(abs(step) for step in d))

    def exists(direction):
        good = None
        for i, step in enumerate(direction):
            if step:
                here = (me[i] > 0) if step < 0 else (me[i] < sizes[i] - 1)
                good = here if good is None else jnp.logical_and(good, here)
        return good

    def target(direction):
        return {axis: me[i] + direction[i] for i, axis in enumerate(AXES)}

    def place(direction):
        return 1 - direction[0], 1 - direction[1]

    def halo_start(round_):
        core = (padded, padded_im)[round_]
        for direction in directions:
            dx, dy, dz = direction
            pairs = []
            if dz == 0:
                src_x = {0: pl.ds(1, nx), 1: pl.ds(nx, 1), -1: pl.ds(1, 1)}[dx]
                dst_x = {0: pl.ds(1, nx), 1: pl.ds(0, 1), -1: pl.ds(nx + 1, 1)}[dx]
                src_y = {0: pl.ds(1, ny), 1: pl.ds(ny, 1), -1: pl.ds(1, 1)}[dy]
                dst_y = {0: pl.ds(1, ny), 1: pl.ds(0, 1), -1: pl.ds(ny + 1, 1)}[dy]
                pairs.append((core.at[src_x, src_y], core.at[dst_x, dst_y]))
                if round_ == 0:
                    pairs.append((mats_rx.at[1, 1], mats_rx.at[place(direction)]))
                else:
                    pairs.insert(0, (ends_im, ends_im_rx.at[place(direction)]))
            elif round_ == 0:
                pairs.append((ends.at[1 if dz > 0 else 0], ends_rx.at[(*place(direction), 0 if dz > 0 else 1)]))
            else:
                continue

            @pl.when(exists(direction))
            def _():
                for src, dst in pairs:
                    pltpu.make_async_remote_copy(
                        src_ref=src, dst_ref=dst, send_sem=sent, recv_sem=halo_recv.at[round_],
                        device_id=target(direction), device_id_type=pl.DeviceIdType.MESH,
                    ).start()

    def wait_units(total, sem):
        part = credit.at[pl.ds(0, total)]
        pltpu.make_async_copy(part, part, sem).wait()

    def halo_wait(rounds, sem, more=0):
        numbers = [
            ((me[i] > 0).astype(jnp.int32) + (me[i] < sizes[i] - 1).astype(jnp.int32)) for i in range(3)
        ]
        choices = [(0,) if size == 1 else (1,) if size == 2 else (1, 2) for size in sizes]
        per = nz // LANES
        for cx, cy, cz in itertools.product(*choices):
            total = 0
            for round_ in rounds:
                total += per * (cx * ny + cy * nx + cx * cy)
                if round_ == 0:
                    total += (cx + cy + cx * cy) * (nx * ny * nz // (cols * LANES)) + cz * (1 + cx) * (1 + cy)
                else:
                    total += cx + cy + cx * cy
            total = total * TILE_UNITS // cols + more
            if total:
                tests = [numbers[i] == c for i, c in enumerate((cx, cy, cz)) if len(choices[i]) > 1]
                take = functools.partial(wait_units, total, sem)
                if tests:
                    pl.when(functools.reduce(jnp.logical_and, tests))(take)
                else:
                    take()

    def each(count, body):
        if count <= 8:
            for k in range(1, count):
                body(k, 0)
        else:
            lax.fori_loop(1, count, body, 0)

    def group_of(axes):
        count, index = 1, 0
        for axis in axes:
            i = AXES.index(axis)
            count *= sizes[i]
            index = index * sizes[i] + me[i]
        return count, index

    def peer_id(axes, peer):
        coords = {axis: me[i] for i, axis in enumerate(AXES)}
        for axis in reversed(axes):
            size = sizes[AXES.index(axis)]
            coords[axis] = lax.rem(peer, size)
            peer = lax.div(peer, size)
        return coords

    def offset_of(round_, number):
        return sum(group_of(axes)[0] for axes in plans[round_][:number])

    direct = (AXES,) in plans

    barrier = pltpu.get_barrier_semaphore()
    expected = 0
    if direct:
        flat = sizes[0] * sizes[1]
        spot = me[0] * sizes[1] + me[1]
        for dz in (-1, 0, 1):
            good = True if dz == 0 else exists((0, 0, dz))

            def greet(k, carry, dz=dz):
                there = lax.rem(spot + k, flat)
                pl.semaphore_signal(
                    barrier, inc=1, device_id_type=pl.DeviceIdType.MESH,
                    device_id={"gx": lax.div(there, sizes[1]), "gy": lax.rem(there, sizes[1]), "gz": me[2] + dz},
                )
                return carry

            if dz == 0:
                each(flat, greet)
                expected = expected + flat - 1
            elif sizes[2] > 1:
                @pl.when(good)
                def _():
                    greet(0, 0)
                    each(flat, greet)
                expected = expected + jnp.where(good, flat, 0)
    else:
        for axes in plans[0]:
            count, index = group_of(axes)

            def greet(k, carry, axes=axes, count=count, index=index):
                pl.semaphore_signal(barrier, inc=1, device_id=peer_id(axes, lax.rem(index + k, count)),
                                    device_id_type=pl.DeviceIdType.MESH)
                return carry

            each(count, greet)
            expected = expected + count - 1
        for direction in directions:
            good = exists(direction)

            @pl.when(good)
            def _():
                pl.semaphore_signal(barrier, inc=1, device_id=target(direction),
                                    device_id_type=pl.DeviceIdType.MESH)
            expected = expected + jnp.where(good, 1, 0)

    for x, y in own:
        pltpu.make_async_copy(loads_ref.at[:, x, y, :], stack.at[x, y, pl.ds(0, cols), :], local_sems.at[0]).start()
    mat_copy = pltpu.make_async_copy(mat_hbm, mat_ref, local_sems.at[1])
    mat_copy.start()
    moduli_copy = pltpu.make_async_copy(moduli_hbm, moduli_ref, local_sems.at[2])
    moduli_copy.start()

    for direction in itertools.product((-1, 0, 1), repeat=3):
        dx, dy, dz = direction
        if any(direction):
            bx, by = 1 + dx, 1 + dy
            clear = []
            if dz:
                clear.append(ends_rx.at[bx, by, 0 if dz < 0 else 1])
            else:
                x_part = {0: range(1, nx + 1), 1: (nx + 1,), -1: (0,)}[dx]
                y_part = {0: range(1, ny + 1), 1: (ny + 1,), -1: (0,)}[dy]
                for x, y in itertools.product(x_part, y_part):
                    clear += [padded.at[x, y], padded_im.at[x, y]]
                clear += [mats_rx.at[bx, by], ends_im_rx.at[bx, by]]

            def wipe():
                for ref in clear:
                    ref[...] = jnp.zeros(ref.shape, ref.dtype)

            if all(step == 0 or sizes[i] > 1 for i, step in enumerate(direction)):
                pl.when(jnp.logical_not(exists(direction)))(wipe)
            else:
                wipe()

    vouches = max(sizes[2] - 2, 0) if direct else 0

    def vouch(round_):
        for dz in (-1, 1):
            @pl.when(exists((0, 0, dz)))
            def _():
                pl.semaphore_signal(vouch_sem.at[round_, 0 if dz > 0 else 1], inc=1, device_id=target((0, 0, dz)),
                                    device_id_type=pl.DeviceIdType.MESH)

    def vouched(round_):
        for dz in (-1, 1):
            @pl.when(exists((0, 0, dz)))
            def _():
                pl.semaphore_wait(vouch_sem.at[round_, 1 if dz > 0 else 0], 1)

    lane = lax.broadcasted_iota(jnp.int32, (1, LANES), 1)

    def spread(firsts, lasts, row, first, last, at):
        spot = at + 4 * row
        ahead = jnp.logical_and(lane >= spot, lane < spot + 2)
        start = (spot - 2) % LANES
        behind = jnp.logical_and(lane >= start, lane < start + 2)
        return (jnp.where(ahead, pltpu.roll(first, spot, 1), firsts),
                jnp.where(behind, pltpu.roll(last, spot, 1), lasts))

    mat_copy.wait()
    ids = jnp.concatenate([mat_ref[x] for x in range(nx)], axis=0)
    ids = (ids + 1).astype(F32)
    mats_rx[1, 1] = ids.astype(BF16)
    firsts = lasts = jnp.zeros((cols, LANES), F32)
    for x, y in own:
        row = x * ny + y
        first = jnp.broadcast_to(ids[row : row + 1, 0:LANES], (cols, LANES))
        last = jnp.broadcast_to(ids[row : row + 1, nz - LANES : nz], (cols, LANES))
        firsts, lasts = spread(firsts, lasts, row, first, last, IDS)
    whole = stack.at[:, :, pl.ds(0, cols), :]
    pltpu.make_async_copy(whole, whole, local_sems.at[0]).wait()
    for x, y in own:
        values = stack[x, y, 0:cols, :]
        padded[x + 1, y + 1] = values.astype(BF16)
        firsts, lasts = spread(firsts, lasts, x * ny + y, values[:, 0:LANES], values[:, nz - LANES : nz], 0)
    ends[0] = firsts.astype(BF16)
    ends[1] = lasts.astype(BF16)
    pl.semaphore_wait(barrier, expected)
    halo_start(0)
    if vouches:
        vouch(0)

    def gram(left, right):
        return tree_sum([split_dot(*left(x, y), *right(x, y), 1, 1) for x, y in own])

    def sum_copy(round_, number, peer):
        axes = plans[round_][number]
        count, index = group_of(axes)
        slot = offset_of(round_, number) + index
        return pltpu.make_async_remote_copy(
            src_ref=shares_of[round_].at[slot], dst_ref=shares_of[round_].at[slot],
            send_sem=sent, recv_sem=sum_recv.at[arrival(round_, number)],
            device_id=peer, device_id_type=pl.DeviceIdType.MESH,
        )

    def sum_start(round_, number, tile):
        axes = plans[round_][number]
        count, index = group_of(axes)
        shares_of[round_][offset_of(round_, number) + index] = tile
        if axes == AXES:
            plane = []
            for k in range(flat):
                there = lax.rem(spot + k, flat)
                plane.append((lax.div(there, sizes[1]), lax.rem(there, sizes[1])))
            low = 2 * me[2] < sizes[2]
            far, turn = jnp.where(low, sizes[2] - 1, 0), jnp.where(low, -1, 1)
            away = jnp.where(low, sizes[2] - 1 - me[2], me[2])
            for i in range(sizes[2] - 1):
                level = far + turn * (i + jnp.where(i < away, 0, 1))
                for gx, gy in plane[::-1]:
                    sum_copy(round_, number, {"gx": gx, "gy": gy, "gz": level}).start()
            for gx, gy in plane[:0:-1]:
                sum_copy(round_, number, {"gx": gx, "gy": gy, "gz": me[2]}).start()
        else:
            def send(k, carry):
                sum_copy(round_, number, peer_id(axes, lax.rem(index + k, count))).start()
                return carry

            each(count, send)

    def arrival(round_, number):
        return sum(len(phases) for phases in plans[:round_]) + number

    def sum_units(round_, number):
        return (group_of(plans[round_][number])[0] - 1) * (2 if round_ == 1 else 1)

    def sum_finish(round_, number):
        total = sum_units(round_, number)
        if total:
            wait_units(total, sum_recv.at[arrival(round_, number)])
        start = offset_of(round_, number)
        return tree_sum([shares_of[round_][start + peer] for peer in range(group_of(plans[round_][number])[0])])

    def sum_turn(round_):
        for number in range(1, len(plans[round_])):
            sum_start(round_, number, sum_finish(round_, number - 1))

    def sum_rest(round_):
        return sum_finish(round_, len(plans[round_]) - 1)

    def loads_at(x, y):
        return stack[x, y, 0:cols, :]

    def image_at(x, y):
        return stack[x, y, cols:, :]

    for x, y in own:
        low[x, y, 0:cols, :] = (loads_at(x, y) - padded[x + 1, y + 1].astype(F32)).astype(BF16)

    def loads_split(x, y):
        return padded[x + 1, y + 1], low[x, y, 0:cols, :]

    def image_split(x, y):
        return padded_im[x + 1, y + 1], low[x, y, cols:, :]

    square_part = gram(loads_split, loads_split)
    sum_start(0, 0, pack(square_part))
    for round_ in range(1, vouches):
        vouched(round_ - 1)
        vouch(round_)
    moduli_copy.wait()

    def block_of(x, y):
        bx, lx = (0, nx - 1) if x == 0 else (2, 0) if x == nx + 1 else (1, x - 1)
        by, ly = (0, ny - 1) if y == 0 else (2, 0) if y == ny + 1 else (1, y - 1)
        return bx, by, lx * ny + ly

    odd = lax.rem(lane, 4) >= 2

    def merged(edge):
        return {
            (bx, by): jnp.where(odd, edge[bx, by, 0].astype(F32), edge[bx, by, 1].astype(F32))
            for bx, by in itertools.product(range(3), repeat=2)
        }

    def tail_of(tiles, x, y, at=0):
        bx, by, row = block_of(x, y)
        return pltpu.roll(tiles[bx, by], (2 * LANES - at - 4 * row) % LANES, 1)

    def modulus_of(ids):
        found = jnp.zeros(ids.shape, F32)
        for number in range(mats):
            found = jnp.where(ids == float(number + 1), moduli_ref[number], found)
        return found

    own_modulus = modulus_of(mats_rx[1, 1].astype(F32))
    halo_wait((0,), halo_recv.at[0])
    full = nz + LANES
    tails = merged(ends_rx)
    flats = {
        key: own_modulus if key == (1, 1) else modulus_of(mats_rx[key].astype(F32)) for key in tails
    }
    sides = {key: modulus_of(tile[0:8]) for key, tile in tails.items()}
    moduli = {}
    for x in xs:
        for y in ys:
            field[x, y] = jnp.concatenate([padded[x, y].astype(F32), tail_of(tails, x, y)], axis=1)
            bx, by, row = block_of(x, y)
            moduli[x, y] = jnp.concatenate([
                jnp.broadcast_to(flats[bx, by][row : row + 1, :], (8, nz)), tail_of(sides, x, y, IDS)
            ], axis=1)
    for x in range(nx + 1):
        for y in range(ny + 1):
            total = (moduli[x, y] + moduli[x, y + 1]) + (moduli[x + 1, y] + moduli[x + 1, y + 1])
            after = (0.125 * k_far) * (total + pltpu.roll(total, full - 1, 1))
            before = pltpu.roll(after, 1, 1)
            wt[x, y], wtr[x, y], level[x, y] = after, before, before + after

    def around_of(weights, x, y):
        return (weights[x, y] + weights[x, y + 1]) + (weights[x + 1, y] + weights[x + 1, y + 1])

    for x, y in own:
        above, below = around_of(wtr, x, y), around_of(wt, x, y)
        node[0, x, y], node[1, x, y], node[2, x, y] = above, below, (k_self / k_far) * (above + below)

    def double(tile):
        return jnp.concatenate([tile, tile], axis=0)

    def operate(direction_of, write, width=None):
        width = width or nz
        lines, ahead_of, behind_of = {}, {}, {}

        def line(x, y):
            if (x, y) not in lines:
                lines[x, y] = field[x, y] + field[x, y + 1]
            return lines[x, y]

        for x in range(nx):
            for y in range(ny):
                here = field[x + 1, y + 1]
                corners = list(itertools.product((x, x + 1), (y, y + 1)))
                flats = []
                for ex, ey in corners:
                    if (ex, ey) not in ahead_of:
                        corner_sum = line(ex, ey) + line(ex + 1, ey)
                        ahead_of[ex, ey] = double(wtr[ex, ey]) * corner_sum
                        behind_of[ex, ey] = double(wt[ex, ey]) * corner_sum
                    opposite = field[2 * ex - x, 2 * ey - y][:, 0:width]
                    flats.append(double(level[ex, ey, :, 0:width]) * opposite)
                ahead = tree_sum([ahead_of[key] for key in corners]) - double(node[0, x, y]) * here
                behind = tree_sum([behind_of[key] for key in corners]) - double(node[1, x, y]) * here
                around = pltpu.roll(ahead, full - 1, 1)[:, 0:width] + pltpu.roll(behind, 1, 1)[:, 0:width]
                centre = double(node[2, x, y, :, 0:width]) * here[:, 0:width]
                write(x, y, SIGMA * direction_of(x, y) + (around + tree_sum(flats) + centre))

    has_right = (me[2] < sizes[2] - 1).astype(jnp.int32)
    has_left = (me[2] > 0).astype(jnp.int32)
    beyond = jnp.logical_or(lane < has_right, lane >= LANES - has_left)
    image_ends = [jnp.zeros((cols, LANES), F32)]

    def write_first(x, y, image):
        row = x * ny + y
        stack[x, y, cols:, :] = image[:, 0:nz]
        padded_im[x + 1, y + 1], low[x, y, cols:, :] = halves(image[:, 0:nz])
        tail = jnp.where(beyond, image[:, nz:], 0.0)
        tail_im[x, y] = tail
        turned = pltpu.roll(tail, 4 * row, 1)
        image_ends[0] = image_ends[0] + turned

    operate(lambda x, y: jnp.concatenate([loads_at(x, y), field[x + 1, y + 1][:, nz:]], axis=1), write_first, full)
    ends_im[...] = image_ends[0].astype(BF16)
    halo_start(1)
    def pair_split(x, y):
        return jnp.concatenate([padded[x + 1, y + 1], padded_im[x + 1, y + 1]], axis=0), low[x, y]

    both_part = gram(image_split, pair_split)
    if vouches:
        vouched(vouches - 1)
    sum_start(1, 0, jnp.concatenate([pack(both_part[:, 0:cols]), pack(both_part[:, cols:])], axis=0))
    sum_turn(0)

    halo_wait((1,), halo_recv.at[1])
    turned_im = {}
    for x in xs:
        for y in ys:
            if 1 <= x <= nx and 1 <= y <= ny:
                turned_im[x, y] = tail_im[x - 1, y - 1]
            else:
                bx, by, row = block_of(x, y)
                turned_im[x, y] = pltpu.roll(ends_im_rx[bx, by].astype(F32), (LANES - 4 * row) % LANES, 1)
    for x in xs:
        for y in ys:
            inner = 1 <= x <= nx and 1 <= y <= ny
            value = image_at(x - 1, y - 1) if inner else padded_im[x, y].astype(F32)
            field[x, y] = jnp.concatenate([value, turned_im[x, y]], axis=1)
    last_parts = []

    def write_last(x, y, image):
        last_parts.append(split_dot(*image_split(x, y), *halves(image), 1, 1))

    operate(image_at, write_last)
    sum_start(2, 0, pack(tree_sum(last_parts)))

    square = unpack(sum_rest(0), cols)
    sum_turn(1)
    row_id = lax.broadcasted_iota(jnp.int32, (cols, cols), 0)
    col_id = lax.broadcasted_iota(jnp.int32, (cols, cols), 1)
    eye = jnp.where(row_id == col_id, 1.0, 0.0)
    inverse = solve(square, eye)
    table = sum_rest(1)
    half = table.shape[0] // 2
    cross, quad = unpack(table[0:half], cols), unpack(table[half:], cols)
    cross = 0.5 * (cross + cross.T)
    alpha = solve(cross, square)
    moved = dot(jnp.concatenate([quad, cross], axis=0), alpha, 1, 0)
    alpha_t = alpha.T
    updated = square + dot(alpha_t, moved[0:cols], 1, 0) - (moved[cols:] + moved[cols:].T)
    grown_t = eye + dot(updated, inverse, 1, 0)
    mix = jnp.concatenate([grown_t, -alpha_t], axis=1)
    mix_hi, mix_lo = halves(mix)
    mix_both = jnp.concatenate([mix_hi, mix_lo], axis=0)
    known = dot(grown_t, dot(cross, grown_t, 1, 1), 1, 0)
    joint = dot(grown_t, moved[0:cols], 1, 0)
    known = 0.5 * (known + known.T) - (joint + joint.T)

    for x in xs:
        for y in ys:
            inner = 1 <= x <= nx and 1 <= y <= ny
            near_tail = jnp.concatenate([
                tail_of(tails, x, y).astype(BF16), turned_im[x, y].astype(BF16)
            ], axis=0)
            if not inner:
                near_tail = jnp.concatenate([
                    jnp.concatenate([padded[x, y], padded_im[x, y]], axis=0), near_tail
                ], axis=1)
            twice = dot(mix_both, near_tail, 1, 0, None)
            mixed = twice[0:cols] + twice[cols:]
            if inner:
                direction = dot(mix, stack[x - 1, y - 1], 1, 0)
                mixed = jnp.concatenate([direction, mixed], axis=1)
            rounded = mixed.astype(BF16)
            field[x, y] = rounded.astype(F32)
            if inner:
                stack[x - 1, y - 1, cols:, :] = direction
                pair_ref[x - 1, y - 1, 0, 0:cols, :] = rounded[:, 0:nz]
                pair_ref[x - 1, y - 1, 0, cols:, :] = (direction - rounded[:, 0:nz].astype(F32)).astype(BF16)

    def write_second(x, y, image):
        pair_ref[x, y, 1, 0:cols, :], pair_ref[x, y, 1, cols:, :] = halves(image)

    operate(image_at, write_second)
    alpha_split = halves(alpha_t)
    for x, y in own:
        base_ref[x, y, 0:cols, :] = split_dot(*alpha_split, *loads_split(x, y), 1, 0)
        base_ref[x, y, cols:, :] = loads_at(x, y) - split_dot(*alpha_split, *image_split(x, y), 1, 0)
    halo_wait((0, 1), sent, sum(
        sum_units(round_, number) for round_ in range(3) for number in range(len(plans[round_]))
        if (round_, number) != (2, 1)
    ))
    sum_turn(2)
    last = unpack(sum_rest(2), cols)
    turned = dot(alpha_t, last, 1, 0) + dot(alpha_t, last, 1, 1)
    coef_ref[0:cols, :], coef_ref[cols:, :] = halves(solve(known + 0.5 * dot(turned, alpha, 1, 0), updated).T)
    if len(plans[2]) > 1:
        wait_units(sum_units(2, 1), sent)


def last_body(coef_ref, base_ref, pair_ref, sol_ref, res_ref, stage, sems):
    cols, nx, ny, nz = sol_ref.shape
    high, low = coef_ref[0:cols, :], coef_ref[cols:, :]
    for x in range(nx):
        for which, ref, sign in ((0, sol_ref, 1.0), (1, res_ref, -1.0)):
            rows = slice(which * cols, (which + 1) * cols)
            for y in range(ny):
                added = split_dot(high, low, pair_ref[x, y, which, 0:cols, :], pair_ref[x, y, which, cols:, :], 1, 0)
                stage[which, :, x, y, :] = base_ref[x, y, rows, :] + sign * added
            pltpu.make_async_copy(stage.at[which, :, x], ref.at[:, x], sems.at[which]).start()
    for which in range(2):
        pltpu.make_async_copy(stage.at[which], stage.at[which], sems.at[which]).wait()


def on_device(sizes, loads, moduli, material):
    cols, nx, ny, nz = loads.shape
    count = int(np.prod(sizes))
    split = (("gx", "gy"), ("gz",))
    quick = (AXES,) if count <= DIRECT_LIMIT else split
    plans = (split, quick, quick)

    def slots(phases):
        return sum(int(np.prod([sizes[AXES.index(a)] for a in axes])) for axes in phases)

    vmem = pl.BlockSpec(memory_space=pltpu.VMEM)
    anywhere = pl.BlockSpec(memory_space=pl.ANY)
    full = nz + LANES
    tiles = 2 * ((nz // LANES) * 2 * (nx + ny + 2) + 26) + 8 * (nx * ny * nz // (cols * LANES))
    credits = tiles * TILE_UNITS // cols + 2 * sum(slots(phases) for phases in plans)
    base, pair, coef = pl.pallas_call(
        functools.partial(main_body, sizes, plans, stiffness_values()),
        out_shape=(
            pltpu.VMEM((nx, ny, 2 * cols, nz), F32),
            pltpu.VMEM((nx, ny, 2, 2 * cols, nz), BF16),
            pltpu.VMEM((2 * cols, cols), BF16),
        ),
        in_specs=[anywhere, anywhere, anywhere],
        out_specs=(vmem, vmem, vmem),
        scratch_shapes=[
            pltpu.VMEM((nx, ny, 2 * cols, nz), F32),
            pltpu.VMEM((nx, ny, 2 * cols, nz), BF16),
            pltpu.VMEM((nx + 2, ny + 2, cols, nz), BF16),
            pltpu.VMEM((nx + 2, ny + 2, cols, nz), BF16),
            pltpu.VMEM((3, 3, nx * ny, nz), BF16),
            pltpu.VMEM((2, cols, LANES), BF16),
            pltpu.VMEM((3, 3, 2, cols, LANES), BF16),
            pltpu.VMEM((cols, LANES), BF16),
            pltpu.VMEM((3, 3, cols, LANES), BF16),
            pltpu.VMEM((nx + 2, ny + 2, cols, full), F32),
            pltpu.VMEM((nx + 1, ny + 1, 8, full), F32),
            pltpu.VMEM((nx + 1, ny + 1, 8, full), F32),
            pltpu.VMEM((nx + 1, ny + 1, 8, full), F32),
            pltpu.VMEM((3, nx, ny, 8, full), F32),
            pltpu.VMEM((slots(plans[0]), cols * cols // LANES, LANES), F32),
            pltpu.VMEM((slots(plans[1]), 2 * cols * cols // LANES, LANES), F32),
            pltpu.VMEM((slots(plans[2]), cols * cols // LANES, LANES), F32),
            pltpu.VMEM((nx, ny, cols, LANES), F32),
            pltpu.SMEM(moduli.shape, F32),
            pltpu.VMEM(material.shape, jnp.int32),
            pltpu.VMEM((credits, cols * cols // LANES, LANES), F32),
            pltpu.SemaphoreType.DMA,
            pltpu.SemaphoreType.DMA((2,)),
            pltpu.SemaphoreType.DMA((sum(len(phases) for phases in plans),)),
            pltpu.SemaphoreType.DMA((3,)),
            pltpu.SemaphoreType.REGULAR((max(sizes[2] - 2, 1) if count <= DIRECT_LIMIT else 1, 2)),
        ],
        compiler_params=pltpu.CompilerParams(collective_id=0, has_side_effects=True),
    )(moduli, loads, material)
    out = jax.ShapeDtypeStruct(loads.shape, F32)
    return pl.pallas_call(
        last_body,
        out_shape=(out, out),
        in_specs=[vmem, vmem, vmem],
        out_specs=(anywhere, anywhere),
        scratch_shapes=[pltpu.VMEM((2, cols, nx, ny, nz), F32), pltpu.SemaphoreType.DMA((2,))],
        compiler_params=pltpu.CompilerParams(vmem_limit_bytes=4 * 2**20),
    )(coef, base, pair)


def solution(mesh):
    sizes = tuple(mesh.shape[axis] for axis in AXES)
    in_specs = (P(None, "gx", "gy", "gz"), P(), P("gx", "gy", "gz"))
    out_specs = (P(None, "gx", "gy", "gz"), P(None, "gx", "gy", "gz"))
    return jax.shard_map(
        functools.partial(on_device, sizes), mesh=mesh, in_specs=in_specs, out_specs=out_specs, check_vma=False
    )
```

```python
import functools
import itertools

import jax
import jax.numpy as jnp
import numpy as np
from jax import lax
from jax.experimental import pallas as pl
from jax.experimental.pallas import tpu as pltpu
from jax.sharding import PartitionSpec as P

SIGMA = 0.25
AXES = ("gx", "gy", "gz")
HIGH = lax.Precision.HIGHEST
F32 = jnp.float32
BF16 = jnp.bfloat16
LANES = 128
DIRECT_LIMIT = 32
IDS = 32
TILE_UNITS = 64


def stiffness_values():
    mass = (1.0 / 3.0, 1.0 / 6.0)
    stiff = (1.0, -1.0)
    values = []
    for differing in range(4):
        bits = [1 if dim < differing else 0 for dim in range(3)]
        total = 0.0
        for dim in range(3):
            factor = 1.0
            for other in range(3):
                factor *= stiff[bits[other]] if other == dim else mass[bits[other]]
            total += factor
        values.append(float(np.asarray(total, np.float32).astype(jnp.bfloat16).astype(np.float32)))
    return values


def dot(left, right, left_dim, right_dim, precision=HIGH):
    return lax.dot_general(
        left, right, (((left_dim,), (right_dim,)), ((), ())), precision=precision, preferred_element_type=F32
    )


def pack(matrix):
    rows, cols = matrix.shape
    wide = jnp.concatenate([matrix, jnp.zeros((rows, LANES - cols), F32)], axis=1)
    pieces = [
        jnp.sum(pltpu.roll(wide[start : start + 8], 0, 1, stride=cols, stride_axis=0), axis=0, keepdims=True)
        for start in range(0, rows, 8)
    ]
    return jnp.concatenate(pieces, axis=0)


def unpack(tile, cols):
    rows = tile.shape[0]
    tall = jnp.concatenate([tile, jnp.zeros((8 - rows, LANES), F32)], axis=0)
    turned = [tall] + [pltpu.roll(tall, LANES - cols * group, 1) for group in range(1, 8)]
    return jnp.concatenate(
        [turned[group][row : row + 1] for row in range(rows) for group in range(8)], axis=0
    )


def solve(columns, right):
    size = len(right)
    scales = [1.0 / columns[i][i : i + 1, :] for i in range(size)]
    left = [columns[i] * scales[i] for i in range(size)]
    right = [right[i] * scales[i] for i in range(size)]
    start = 0
    for step in range(0, size, 2):
        if step == size // 2 and step % 8 == 0:
            left = [row[step:, :] for row in left]
            start = step
        at = step - start
        top, low, top_right, low_right = left[step], left[step + 1], right[step], right[step + 1]
        first, mixed = top[at : at + 1, :], top[at + 1 : at + 2, :]
        cross, second = low[at : at + 1, :], low[at + 1 : at + 2, :]
        scale = 1.0 / (first * second - mixed * cross)
        aa, ab, ba, bb = second * scale, mixed * scale, cross * scale, first * scale
        one, two = aa * top - ab * low, bb * low - ba * top
        one_right, two_right = aa * top_right - ab * low_right, bb * low_right - ba * top_right
        for i in range(size):
            if i not in (step, step + 1):
                factor, other = left[i][at : at + 1, :], left[i][at + 1 : at + 2, :]
                left[i] = left[i] - (factor * one + other * two)
                right[i] = right[i] - (factor * one_right + other * two_right)
        left[step], left[step + 1], right[step], right[step + 1] = one, two, one_right, two_right
    return right


def columns_of(matrix):
    size = matrix.shape[0]
    return [jnp.broadcast_to(matrix[:, k : k + 1], (size, LANES)) for k in range(size)]


def rows_of(matrix):
    return [matrix[k : k + 1, :] for k in range(matrix.shape[0])]


def weave(columns, rows):
    return tree_sum([column * row for column, row in zip(columns, rows)])


def turn(matrix):
    size = matrix.shape[0]
    return jnp.concatenate([matrix[:, 0:size].T, jnp.zeros((size, LANES - size), F32)], axis=1)


def halves(value):
    high = value.astype(BF16)
    return high, (value - high.astype(F32)).astype(BF16)


def split_dot(left_high, left_low, right_high, right_low, left_dim, right_dim):
    rows = left_high.shape[0]
    both = dot(jnp.concatenate([left_high, left_low], axis=0), right_high, left_dim, right_dim, None)
    return both[0:rows] + both[rows:] + dot(left_high, right_low, left_dim, right_dim, None)


def tree_sum(terms):
    while len(terms) > 1:
        terms = [a + b for a, b in zip(terms[0::2], terms[1::2])] + terms[len(terms) & ~1 :]
    return terms[0]


def main_body(sizes, plans, stiff, moduli_hbm, loads_ref, mat_hbm, base_ref, pair_ref, coef_ref,
              stack, low, padded, padded_im, mats_rx, ends, ends_rx, field, field_im, wt, wtr, level, node,
              shares_square, shares_table, shares_last, moduli_ref, mat_ref, credit,
              sent, sent_first, halo_recv, sum_recv, local_sems, vouch_sem):
    cols, nx, ny, nz = loads_ref.shape
    mats = moduli_ref.shape[0]
    me = [lax.axis_index(axis) for axis in AXES]
    k_self, k_edge, k_far = stiff[0], stiff[1], stiff[2]
    assert k_edge == 0.0 and stiff[2] == stiff[3]
    assert 4 * nx * ny <= IDS and (nx * ny * nz) % (cols * LANES) == 0 and nz % LANES == 0 and TILE_UNITS % cols == 0
    assert nx >= 2 and ny >= 2
    shares_of = (shares_square, shares_table, shares_last)
    own = list(itertools.product(range(nx), range(ny)))

    directions = [
        d for d in itertools.product((-1, 0, 1), repeat=3)
        if any(d) and all(step == 0 or sizes[i] > 1 for i, step in enumerate(d))
    ]
    directions.sort(key=lambda d: -sum(abs(step) for step in d))

    def exists(direction):
        good = None
        for i, step in enumerate(direction):
            if step:
                here = (me[i] > 0) if step < 0 else (me[i] < sizes[i] - 1)
                good = here if good is None else jnp.logical_and(good, here)
        return good

    def target(direction):
        return {axis: me[i] + direction[i] for i, axis in enumerate(AXES)}

    def place(direction):
        return 1 - direction[0], 1 - direction[1]

    def spans(step, size, ring):
        if step == 0:
            return pl.ds(2, size), pl.ds(2, size)
        if ring == 0:
            return (pl.ds(size, 2), pl.ds(0, 2)) if step > 0 else (pl.ds(2, 2), pl.ds(size + 2, 2))
        if step > 0:
            return pl.ds(size + 2 - ring, 1), pl.ds(2 - ring, 1)
        return pl.ds(1 + ring, 1), pl.ds(size + 1 + ring, 1)

    def slab(direction, ring_x, ring_y):
        src_x, dst_x = spans(direction[0], nx, ring_x)
        src_y, dst_y = spans(direction[1], ny, ring_y)
        return padded.at[src_x, src_y], padded.at[dst_x, dst_y]

    def halo_start(round_):
        for direction in directions:
            dx, dy, dz = direction
            pairs = []
            if dz == 0:
                if round_ == 0:
                    pairs.append(slab(direction, 1, 1))
                    pairs.append((mats_rx.at[1, 1], mats_rx.at[place(direction)]))
                elif dx and dy:
                    pairs.append(slab(direction, 2, 0))
                    pairs.append(slab(direction, 1, 2))
                else:
                    pairs.append(slab(direction, 2, 2))
            elif round_ == 0:
                pairs.append((ends.at[1 if dz > 0 else 0], ends_rx.at[(*place(direction), 0 if dz > 0 else 1)]))
            else:
                continue

            @pl.when(exists(direction))
            def _():
                for src, dst in pairs:
                    pltpu.make_async_remote_copy(
                        src_ref=src, dst_ref=dst, send_sem=sent if round_ else sent_first, recv_sem=halo_recv.at[round_],
                        device_id=target(direction), device_id_type=pl.DeviceIdType.MESH,
                    ).start()

    def wait_units(total, sem):
        part = credit.at[pl.ds(0, total)]
        pltpu.make_async_copy(part, part, sem).wait()

    def halo_wait(rounds, sem, more=0):
        numbers = [
            ((me[i] > 0).astype(jnp.int32) + (me[i] < sizes[i] - 1).astype(jnp.int32)) for i in range(3)
        ]
        choices = [(0,) if size == 1 else (1,) if size == 2 else (1, 2) for size in sizes]
        per = nz // LANES
        for cx, cy, cz in itertools.product(*choices):
            total, more_units = 0, more
            for round_ in rounds:
                total += per * (cx * ny + cy * nx + (1 if round_ == 0 else 3) * cx * cy)
                if round_ == 0:
                    total += (cx + cy + cx * cy) * (nx * ny * nz // (cols * LANES))
                    more_units += cz * (1 + cx) * (1 + cy) * TILE_UNITS // cols // 2
            total = total * TILE_UNITS // cols + more_units
            if total:
                tests = [numbers[i] == c for i, c in enumerate((cx, cy, cz)) if len(choices[i]) > 1]
                take = functools.partial(wait_units, total, sem)
                if tests:
                    pl.when(functools.reduce(jnp.logical_and, tests))(take)
                else:
                    take()

    def each(count, body):
        if count <= 8:
            for k in range(1, count):
                body(k, 0)
        else:
            lax.fori_loop(1, count, body, 0)

    def group_of(axes):
        count, index = 1, 0
        for axis in axes:
            i = AXES.index(axis)
            count *= sizes[i]
            index = index * sizes[i] + me[i]
        return count, index

    def peer_id(axes, peer):
        coords = {axis: me[i] for i, axis in enumerate(AXES)}
        for axis in reversed(axes):
            size = sizes[AXES.index(axis)]
            coords[axis] = lax.rem(peer, size)
            peer = lax.div(peer, size)
        return coords

    def offset_of(round_, number):
        return sum(group_of(axes)[0] for axes in plans[round_][:number])

    direct = (AXES,) in plans

    barrier = pltpu.get_barrier_semaphore()
    expected = 0
    if direct:
        flat = sizes[0] * sizes[1]
        spot = me[0] * sizes[1] + me[1]
        for dz in (-1, 0, 1):
            good = True if dz == 0 else exists((0, 0, dz))

            def greet(k, carry, dz=dz):
                there = lax.rem(spot + k, flat)
                pl.semaphore_signal(
                    barrier, inc=1, device_id_type=pl.DeviceIdType.MESH,
                    device_id={"gx": lax.div(there, sizes[1]), "gy": lax.rem(there, sizes[1]), "gz": me[2] + dz},
                )
                return carry

            if dz == 0:
                each(flat, greet)
                expected = expected + flat - 1
            elif sizes[2] > 1:
                @pl.when(good)
                def _():
                    greet(0, 0)
                    each(flat, greet)
                expected = expected + jnp.where(good, flat, 0)
    else:
        for axes in plans[0]:
            count, index = group_of(axes)

            def greet(k, carry, axes=axes, count=count, index=index):
                pl.semaphore_signal(barrier, inc=1, device_id=peer_id(axes, lax.rem(index + k, count)),
                                    device_id_type=pl.DeviceIdType.MESH)
                return carry

            each(count, greet)
            expected = expected + count - 1
        for direction in directions:
            good = exists(direction)

            @pl.when(good)
            def _():
                pl.semaphore_signal(barrier, inc=1, device_id=target(direction),
                                    device_id_type=pl.DeviceIdType.MESH)
            expected = expected + jnp.where(good, 1, 0)

    for x, y in own:
        pltpu.make_async_copy(loads_ref.at[:, x, y, :], stack.at[x, y, pl.ds(0, cols), :], local_sems.at[0]).start()
    mat_copy = pltpu.make_async_copy(mat_hbm, mat_ref, local_sems.at[1])
    mat_copy.start()
    moduli_copy = pltpu.make_async_copy(moduli_hbm, moduli_ref, local_sems.at[2])
    moduli_copy.start()

    for direction in itertools.product((-1, 0, 1), repeat=3):
        dx, dy, dz = direction
        if any(direction):
            bx, by = 1 + dx, 1 + dy
            clear = []
            if dz:
                clear.append(ends_rx.at[bx, by, 0 if dz < 0 else 1])
            else:
                x_part = {0: range(2, nx + 2), 1: (nx + 2, nx + 3), -1: (0, 1)}[dx]
                y_part = {0: range(2, ny + 2), 1: (ny + 2, ny + 3), -1: (0, 1)}[dy]
                for x, y in itertools.product(x_part, y_part):
                    clear.append(padded.at[x, y])
                clear.append(mats_rx.at[bx, by])

            def wipe():
                for ref in clear:
                    ref[...] = jnp.zeros(ref.shape, ref.dtype)

            if all(step == 0 or sizes[i] > 1 for i, step in enumerate(direction)):
                pl.when(jnp.logical_not(exists(direction)))(wipe)
            else:
                wipe()

    vouches = max(sizes[2] - 2, 0) if direct else 0

    def vouch(round_):
        for dz in (-1, 1):
            @pl.when(exists((0, 0, dz)))
            def _():
                pl.semaphore_signal(vouch_sem.at[round_, 0 if dz > 0 else 1], inc=1, device_id=target((0, 0, dz)),
                                    device_id_type=pl.DeviceIdType.MESH)

    def vouched(round_):
        for dz in (-1, 1):
            @pl.when(exists((0, 0, dz)))
            def _():
                pl.semaphore_wait(vouch_sem.at[round_, 1 if dz > 0 else 0], 1)

    lane = lax.broadcasted_iota(jnp.int32, (1, LANES), 1)

    def spread(firsts, lasts, row, first, last, at):
        spot = at + 4 * row
        ahead = jnp.logical_and(lane >= spot, lane < spot + 2)
        start = (spot - 2) % LANES
        behind = jnp.logical_and(lane >= start, lane < start + 2)
        return (jnp.where(ahead, pltpu.roll(first, spot, 1), firsts),
                jnp.where(behind, pltpu.roll(last, spot, 1), lasts))

    mat_copy.wait()
    ids = jnp.concatenate([mat_ref[x] for x in range(nx)], axis=0)
    ids = (ids + 1).astype(F32)
    mats_rx[1, 1] = ids.astype(BF16)
    firsts = lasts = jnp.zeros((cols, LANES), F32)
    for x, y in own:
        row = x * ny + y
        first = jnp.broadcast_to(ids[row : row + 1, 0:LANES], (cols, LANES))
        last = jnp.broadcast_to(ids[row : row + 1, nz - LANES : nz], (cols, LANES))
        firsts, lasts = spread(firsts, lasts, row, first, last, IDS)
    whole = stack.at[:, :, pl.ds(0, cols), :]
    pltpu.make_async_copy(whole, whole, local_sems.at[0]).wait()
    for x, y in own:
        values = stack[x, y, 0:cols, :]
        padded[x + 2, y + 2] = values.astype(BF16)
        firsts, lasts = spread(firsts, lasts, x * ny + y, values[:, 0:LANES], values[:, nz - LANES : nz], 0)
    upper = cols // 2
    for side, tile in enumerate((firsts, lasts)):
        lower_half = jnp.logical_and(lane >= 2 * LANES // 4 - 2, lane < LANES - 2)
        ends[side] = jnp.where(lower_half, pltpu.roll(tile[upper:], LANES // 2, 1), tile[0:upper]).astype(BF16)
    pl.semaphore_wait(barrier, expected)
    halo_start(0)
    if vouches:
        vouch(0)

    def gram(left, right):
        return tree_sum([split_dot(*left(x, y), *right(x, y), 1, 1) for x, y in own])

    def sum_copy(round_, number, peer):
        axes = plans[round_][number]
        count, index = group_of(axes)
        slot = offset_of(round_, number) + index
        return pltpu.make_async_remote_copy(
            src_ref=shares_of[round_].at[slot], dst_ref=shares_of[round_].at[slot],
            send_sem=sent, recv_sem=sum_recv.at[arrival(round_, number)],
            device_id=peer, device_id_type=pl.DeviceIdType.MESH,
        )

    def sum_start(round_, number, tile):
        axes = plans[round_][number]
        count, index = group_of(axes)
        shares_of[round_][offset_of(round_, number) + index] = tile
        if axes == AXES:
            plane = []
            for k in range(flat):
                there = lax.rem(spot + k, flat)
                plane.append((lax.div(there, sizes[1]), lax.rem(there, sizes[1])))
            low = 2 * me[2] < sizes[2]
            far, turn = jnp.where(low, sizes[2] - 1, 0), jnp.where(low, -1, 1)
            away = jnp.where(low, sizes[2] - 1 - me[2], me[2])
            for i in range(sizes[2] - 1):
                level = far + turn * (i + jnp.where(i < away, 0, 1))
                for gx, gy in plane[::-1]:
                    sum_copy(round_, number, {"gx": gx, "gy": gy, "gz": level}).start()
            for gx, gy in plane[:0:-1]:
                sum_copy(round_, number, {"gx": gx, "gy": gy, "gz": me[2]}).start()
        else:
            def send(k, carry):
                sum_copy(round_, number, peer_id(axes, lax.rem(index + k, count))).start()
                return carry

            each(count, send)

    def arrival(round_, number):
        return sum(len(phases) for phases in plans[:round_]) + number

    def sum_units(round_, number):
        return (group_of(plans[round_][number])[0] - 1) * (2 if round_ == 1 else 1)

    def sum_finish(round_, number):
        total = sum_units(round_, number)
        if total:
            wait_units(total, sum_recv.at[arrival(round_, number)])
        start = offset_of(round_, number)
        return tree_sum([shares_of[round_][start + peer] for peer in range(group_of(plans[round_][number])[0])])

    def sum_turn(round_):
        for number in range(1, len(plans[round_])):
            sum_start(round_, number, sum_finish(round_, number - 1))

    def sum_rest(round_):
        return sum_finish(round_, len(plans[round_]) - 1)

    def loads_at(x, y):
        return stack[x, y, 0:cols, :]

    def image_at(x, y):
        return stack[x, y, cols:, :]

    for x, y in own:
        low[x, y, 0:cols, :] = (loads_at(x, y) - padded[x + 2, y + 2].astype(F32)).astype(BF16)

    def loads_split(x, y):
        return padded[x + 2, y + 2], low[x, y, 0:cols, :]

    def image_split(x, y):
        return padded_im[x, y], low[x, y, cols:, :]

    square_part = gram(loads_split, loads_split)
    sum_start(0, 0, pack(square_part))
    for round_ in range(1, vouches):
        vouched(round_ - 1)
        vouch(round_)
    halo_wait((0,), sent_first)
    halo_start(1)
    moduli_copy.wait()

    def block_of(x, y):
        bx, lx = (0, nx - 2 + x) if x < 2 else (2, x - nx - 2) if x >= nx + 2 else (1, x - 2)
        by, ly = (0, ny - 2 + y) if y < 2 else (2, y - ny - 2) if y >= ny + 2 else (1, y - 2)
        return bx, by, lx * ny + ly

    odd = lax.rem(lane, 4) >= 2

    def merged(edge):
        return {
            (bx, by): jnp.where(odd, edge[bx, by, 0].astype(F32), edge[bx, by, 1].astype(F32))
            for bx, by in itertools.product(range(3), repeat=2)
        }

    def tail_of(tiles, x, y, at=0):
        bx, by, row = block_of(x, y)
        tile = tiles[bx, by]
        near, far = ((2 * LANES - spot - 4 * row) % LANES for spot in (at, at + LANES // 2))
        if at:
            return pltpu.roll(tile, near, 1)
        return jnp.concatenate([pltpu.roll(tile, near, 1), pltpu.roll(tile, far, 1)], axis=0)

    def modulus_of(ids):
        found = jnp.zeros(ids.shape, F32)
        for number in range(mats):
            found = jnp.where(ids == float(number + 1), moduli_ref[number], found)
        return found

    own_modulus = modulus_of(mats_rx[1, 1].astype(F32))
    halo_wait((0,), halo_recv.at[0])
    if vouches:
        vouched(vouches - 1)
    sum_turn(0)
    full = nz + LANES
    tails = merged(ends_rx)
    flats = {
        key: own_modulus if key == (1, 1) else modulus_of(mats_rx[key].astype(F32)) for key in tails
    }
    sides = {key: modulus_of(tile) for key, tile in tails.items()}
    moduli = {}

    def modulus_at(x, y):
        if (x, y) not in moduli:
            bx, by, row = block_of(x, y)
            moduli[x, y] = jnp.concatenate([
                jnp.broadcast_to(flats[bx, by][row : row + 1, :], (8, nz)), tail_of(sides, x, y, IDS)
            ], axis=1)
        return moduli[x, y]

    def weigh(x, y):
        total = (modulus_at(x, y) + modulus_at(x, y + 1)) + (modulus_at(x + 1, y) + modulus_at(x + 1, y + 1))
        total = (0.125 * k_far) * total
        after, before = total + pltpu.roll(total, full - 1, 1), total + pltpu.roll(total, 1, 1)
        wt[x, y], wtr[x, y], level[x, y] = after, before, before + after

    def around_of(weights, x, y):
        return (weights[x, y] + weights[x, y + 1]) + (weights[x + 1, y] + weights[x + 1, y + 1])

    def gather(x, y):
        above, below = around_of(wtr, x, y), around_of(wt, x, y)
        node[0, x, y], node[1, x, y], node[2, x, y] = above, below, (k_self / k_far) * (above + below)

    def unfold(x, y):
        field[x, y] = jnp.concatenate([padded[x, y].astype(F32), tail_of(tails, x, y)], axis=1)

    inner = list(itertools.product(range(1, nx + 1), range(1, ny + 1)))
    outer = [key for key in itertools.product(range(nx + 2), range(ny + 2)) if key not in inner]
    near = list(itertools.product(range(1, nx + 3), range(1, ny + 3)))
    near_elements = list(itertools.product(range(1, nx + 2), range(1, ny + 2)))
    for key in near:
        unfold(*key)
    for key in near_elements:
        weigh(*key)
    for key in inner:
        gather(*key)

    def double(tile):
        return jnp.concatenate([tile, tile], axis=0)

    def operate(source, shift, cells, direction_of, write, width):
        lines, ahead_of, behind_of = {}, {}, {}

        def line(x, y):
            if (x, y) not in lines:
                lines[x, y] = source[x - shift, y - shift] + source[x - shift, y + 1 - shift]
            return lines[x, y]

        for x, y in cells:
            here = source[x + 1 - shift, y + 1 - shift]
            corners = list(itertools.product((x, x + 1), (y, y + 1)))
            flats = []
            for ex, ey in corners:
                if (ex, ey) not in ahead_of:
                    corner_sum = line(ex, ey) + line(ex + 1, ey)
                    ahead_of[ex, ey] = double(wtr[ex, ey]) * corner_sum
                    behind_of[ex, ey] = double(wt[ex, ey]) * corner_sum
                opposite = source[2 * ex - x - shift, 2 * ey - y - shift][:, 0:width]
                flats.append(double(level[ex, ey, :, 0:width]) * opposite)
            ahead = tree_sum([ahead_of[key] for key in corners]) - double(node[0, x, y]) * here
            behind = tree_sum([behind_of[key] for key in corners]) - double(node[1, x, y]) * here
            around = pltpu.roll(ahead, full - 1, 1)[:, 0:width] + pltpu.roll(behind, 1, 1)[:, 0:width]
            centre = double(node[2, x, y, :, 0:width]) * here[:, 0:width]
            write(x, y, SIGMA * direction_of(x, y) + (around + tree_sum(flats) + centre))

    has_right = (me[2] < sizes[2] - 1).astype(jnp.int32)
    has_left = (me[2] > 0).astype(jnp.int32)
    beyond = jnp.logical_or(lane < has_right, lane >= LANES - has_left)

    def write_first(x, y, image):
        main = image[:, 0:nz]
        stack[x - 1, y - 1, cols:, :] = main
        padded_im[x - 1, y - 1], low[x - 1, y - 1, cols:, :] = halves(main)
        field_im[x, y] = jnp.concatenate([main, jnp.where(beyond, image[:, nz:], 0.0)], axis=1)

    def loads_wide(x, y):
        return jnp.concatenate([loads_at(x - 1, y - 1), field[x + 1, y + 1][:, nz:]], axis=1)

    operate(field, 0, inner, loads_wide, write_first, full)

    def pair_split(x, y):
        return jnp.concatenate([padded[x + 2, y + 2], padded_im[x, y]], axis=0), low[x, y]

    both_part = gram(image_split, pair_split)
    sum_start(1, 0, jnp.concatenate([pack(both_part[:, 0:cols]), pack(both_part[:, cols:])], axis=0))
    for key in itertools.product(range(nx + 3), range(ny + 3)):
        if key not in near_elements:
            weigh(*key)
    for key in outer:
        gather(*key)
    halo_wait((1,), halo_recv.at[1])
    for key in itertools.product(range(nx + 4), range(ny + 4)):
        if key not in near:
            unfold(*key)

    def write_ring(x, y, image):
        dx = -1 if x == 0 else 1 if x == nx + 1 else 0
        dy = -1 if y == 0 else 1 if y == ny + 1 else 0
        if any(step and sizes[i] == 1 for i, step in enumerate((dx, dy))):
            field_im[x, y] = jnp.zeros(image.shape, F32)
        else:
            image = jnp.where(exists((dx, dy, 0)), image, 0.0)
            field_im[x, y] = jnp.concatenate([image[:, 0:nz], jnp.where(beyond, image[:, nz:], 0.0)], axis=1)

    operate(field, 0, outer, lambda x, y: field[x + 1, y + 1], write_ring, full)
    last_parts = []

    def write_last(x, y, image):
        last_parts.append(split_dot(*image_split(x - 1, y - 1), *halves(image), 1, 1))

    operate(field_im, 1, inner, lambda x, y: image_at(x - 1, y - 1), write_last, nz)
    sum_start(2, 0, pack(tree_sum(last_parts)))

    square = unpack(sum_rest(0), cols)
    sum_turn(1)
    row_id = lax.broadcasted_iota(jnp.int32, (cols, LANES), 0)
    col_id = lax.broadcasted_iota(jnp.int32, (cols, LANES), 1)
    eye = jnp.where(row_id == col_id, 1.0, 0.0)
    inverse = solve(columns_of(square), rows_of(eye))
    table = sum_rest(1)
    half = table.shape[0] // 2
    cross, quad = unpack(table[0:half], cols), unpack(table[half:], cols)
    cross = 0.5 * (cross + turn(cross))
    cross_columns = columns_of(cross)
    alpha_rows = solve(cross_columns, rows_of(square))
    alpha_t = turn(jnp.concatenate(alpha_rows, axis=0))
    alpha_columns = columns_of(alpha_t)
    moved, stood = weave(columns_of(quad), alpha_rows), weave(cross_columns, alpha_rows)
    alpha_t = alpha_t[:, 0:cols]
    alpha_split = halves(alpha_t)
    alpha_both = jnp.concatenate(alpha_split, axis=0)
    cells = list(itertools.product(range(nx + 2), range(ny + 2)))

    def start_of(cell):
        return nz if cell in inner else 0

    for x, y in cells:
        start = start_of((x, y))
        twice = dot(alpha_both, field_im[x, y, :, start:].astype(BF16), 1, 0, None)
        field_im[x, y, :, start:] = field[x + 1, y + 1, :, start:] - (twice[0:cols] + twice[cols:])
        if (x, y) in inner:
            base_ref[x - 1, y - 1, cols:, :] = loads_at(x - 1, y - 1) - dot(alpha_t, image_at(x - 1, y - 1), 1, 0)
    updated = square + weave(alpha_columns, rows_of(moved)) - (stood + turn(stood))
    beta_t = weave(columns_of(updated), inverse)
    grown_t = eye + beta_t
    grown_columns = columns_of(grown_t)
    joint = weave(grown_columns, rows_of(moved))
    known = weave(columns_of(weave(grown_columns, rows_of(cross))), rows_of(turn(grown_t))) - (joint + turn(joint))
    beta_t = beta_t[:, 0:cols]
    beta_both = jnp.concatenate(halves(beta_t), axis=0)
    for x, y in cells:
        start = start_of((x, y))
        twice = dot(beta_both, field[x + 1, y + 1, :, start:].astype(BF16), 1, 0, None)
        mixed = field_im[x, y, :, start:] + (twice[0:cols] + twice[cols:])
        if (x, y) in inner:
            direction = base_ref[x - 1, y - 1, cols:, :] + dot(beta_t, loads_at(x - 1, y - 1), 1, 0)
            mixed = jnp.concatenate([direction, mixed], axis=1)
        rounded = mixed.astype(BF16)
        field_im[x, y] = rounded.astype(F32)
        if (x, y) in inner:
            stack[x - 1, y - 1, cols:, :] = direction
            pair_ref[x - 1, y - 1, 0, 0:cols, :] = rounded[:, 0:nz]
            pair_ref[x - 1, y - 1, 0, cols:, :] = (direction - rounded[:, 0:nz].astype(F32)).astype(BF16)

    halo_wait((1,), sent, sum(
        sum_units(round_, number) for round_ in range(3) for number in range(len(plans[round_]))
        if (round_, number) != (2, 1)
    ))
    sum_turn(2)
    last = unpack(sum_rest(2), cols)
    total = known + weave(alpha_columns, rows_of(weave(columns_of(last), alpha_rows)))
    last_rows = solve(columns_of(total), rows_of(updated))
    coef_t = jnp.concatenate(last_rows, axis=0)[:, 0:cols].T
    coef_ref[0:cols, :], coef_ref[cols:, :] = halves(coef_t)

    def write_second(x, y, image):
        pair_ref[x - 1, y - 1, 1, 0:cols, :], pair_ref[x - 1, y - 1, 1, cols:, :] = halves(image)

    operate(field_im, 1, inner, lambda x, y: image_at(x - 1, y - 1), write_second, nz)
    for x, y in own:
        base_ref[x, y, 0:cols, :] = split_dot(*alpha_split, *loads_split(x, y), 1, 0)
    if len(plans[2]) > 1:
        wait_units(sum_units(2, 1), sent)


def last_body(coef_ref, base_ref, pair_ref, sol_ref, res_ref, stage, sems):
    cols, nx, ny, nz = sol_ref.shape
    high, low = coef_ref[0:cols, :], coef_ref[cols:, :]
    for x in range(nx):
        for which, ref, sign in ((0, sol_ref, 1.0), (1, res_ref, -1.0)):
            rows = slice(which * cols, (which + 1) * cols)
            for y in range(ny):
                added = split_dot(high, low, pair_ref[x, y, which, 0:cols, :], pair_ref[x, y, which, cols:, :], 1, 0)
                stage[which, :, x, y, :] = base_ref[x, y, rows, :] + sign * added
            pltpu.make_async_copy(stage.at[which, :, x], ref.at[:, x], sems.at[which]).start()
    for which in range(2):
        pltpu.make_async_copy(stage.at[which], stage.at[which], sems.at[which]).wait()


def on_device(sizes, loads, moduli, material):
    cols, nx, ny, nz = loads.shape
    count = int(np.prod(sizes))
    split = (("gx", "gy"), ("gz",))
    quick = (AXES,) if count <= DIRECT_LIMIT else split
    plans = (split, quick, quick)

    def slots(phases):
        return sum(int(np.prod([sizes[AXES.index(a)] for a in axes])) for axes in phases)

    vmem = pl.BlockSpec(memory_space=pltpu.VMEM)
    anywhere = pl.BlockSpec(memory_space=pl.ANY)
    full = nz + LANES
    tiles = (nz // LANES) * 4 * (nx + ny + 4) + 18 + 8 * (nx * ny * nz // (cols * LANES))
    credits = tiles * TILE_UNITS // cols + 2 * sum(slots(phases) for phases in plans)
    base, pair, coef = pl.pallas_call(
        functools.partial(main_body, sizes, plans, stiffness_values()),
        out_shape=(
            pltpu.VMEM((nx, ny, 2 * cols, nz), F32),
            pltpu.VMEM((nx, ny, 2, 2 * cols, nz), BF16),
            pltpu.VMEM((2 * cols, cols), BF16),
        ),
        in_specs=[anywhere, anywhere, anywhere],
        out_specs=(vmem, vmem, vmem),
        scratch_shapes=[
            pltpu.VMEM((nx, ny, 2 * cols, nz), F32),
            pltpu.VMEM((nx, ny, 2 * cols, nz), BF16),
            pltpu.VMEM((nx + 4, ny + 4, cols, nz), BF16),
            pltpu.VMEM((nx, ny, cols, nz), BF16),
            pltpu.VMEM((3, 3, nx * ny, nz), BF16),
            pltpu.VMEM((2, cols // 2, LANES), BF16),
            pltpu.VMEM((3, 3, 2, cols // 2, LANES), BF16),
            pltpu.VMEM((nx + 4, ny + 4, cols, full), F32),
            pltpu.VMEM((nx + 2, ny + 2, cols, full), F32),
            pltpu.VMEM((nx + 3, ny + 3, 8, full), F32),
            pltpu.VMEM((nx + 3, ny + 3, 8, full), F32),
            pltpu.VMEM((nx + 3, ny + 3, 8, full), F32),
            pltpu.VMEM((3, nx + 2, ny + 2, 8, full), F32),
            pltpu.VMEM((slots(plans[0]), cols * cols // LANES, LANES), F32),
            pltpu.VMEM((slots(plans[1]), 2 * cols * cols // LANES, LANES), F32),
            pltpu.VMEM((slots(plans[2]), cols * cols // LANES, LANES), F32),
            pltpu.SMEM(moduli.shape, F32),
            pltpu.VMEM(material.shape, jnp.int32),
            pltpu.VMEM((credits, cols * cols // LANES, LANES), F32),
            pltpu.SemaphoreType.DMA,
            pltpu.SemaphoreType.DMA,
            pltpu.SemaphoreType.DMA((2,)),
            pltpu.SemaphoreType.DMA((sum(len(phases) for phases in plans),)),
            pltpu.SemaphoreType.DMA((3,)),
            pltpu.SemaphoreType.REGULAR((max(sizes[2] - 2, 1) if count <= DIRECT_LIMIT else 1, 2)),
        ],
        compiler_params=pltpu.CompilerParams(collective_id=0, has_side_effects=True),
    )(moduli, loads, material)
    out = jax.ShapeDtypeStruct(loads.shape, F32)
    return pl.pallas_call(
        last_body,
        out_shape=(out, out),
        in_specs=[vmem, vmem, vmem],
        out_specs=(anywhere, anywhere),
        scratch_shapes=[pltpu.VMEM((2, cols, nx, ny, nz), F32), pltpu.SemaphoreType.DMA((2,))],
        compiler_params=pltpu.CompilerParams(vmem_limit_bytes=4 * 2**20),
    )(coef, base, pair)


def solution(mesh):
    sizes = tuple(mesh.shape[axis] for axis in AXES)
    in_specs = (P(None, "gx", "gy", "gz"), P(), P("gx", "gy", "gz"))
    out_specs = (P(None, "gx", "gy", "gz"), P(None, "gx", "gy", "gz"))
    return jax.shard_map(
        functools.partial(on_device, sizes), mesh=mesh, in_specs=in_specs, out_specs=out_specs, check_vma=False
    )
```

```python
import functools
import itertools

import jax
import jax.numpy as jnp
import numpy as np
from jax import lax
from jax.experimental import pallas as pl
from jax.experimental.pallas import tpu as pltpu
from jax.sharding import PartitionSpec as P

SIGMA = 0.25
AXES = ("gx", "gy", "gz")
HIGH = lax.Precision.HIGHEST
F32 = jnp.float32
BF16 = jnp.bfloat16
LANES = 128
DIRECT_LIMIT = 32
IDS = 32
TILE_UNITS = 64


def stiffness_values():
    mass = (1.0 / 3.0, 1.0 / 6.0)
    stiff = (1.0, -1.0)
    values = []
    for differing in range(4):
        bits = [1 if dim < differing else 0 for dim in range(3)]
        total = 0.0
        for dim in range(3):
            factor = 1.0
            for other in range(3):
                factor *= stiff[bits[other]] if other == dim else mass[bits[other]]
            total += factor
        values.append(float(np.asarray(total, np.float32).astype(jnp.bfloat16).astype(np.float32)))
    return values


def dot(left, right, left_dim, right_dim, precision=HIGH):
    return lax.dot_general(
        left, right, (((left_dim,), (right_dim,)), ((), ())), precision=precision, preferred_element_type=F32
    )


def pack(matrix):
    rows, cols = matrix.shape
    wide = jnp.concatenate([matrix, jnp.zeros((rows, LANES - cols), F32)], axis=1)
    pieces = [
        jnp.sum(pltpu.roll(wide[start : start + 8], 0, 1, stride=cols, stride_axis=0), axis=0, keepdims=True)
        for start in range(0, rows, 8)
    ]
    return jnp.concatenate(pieces, axis=0)


def unpack(tile, cols):
    rows = tile.shape[0]
    tall = jnp.concatenate([tile, jnp.zeros((8 - rows, LANES), F32)], axis=0)
    turned = [tall] + [pltpu.roll(tall, LANES - cols * group, 1) for group in range(1, 8)]
    return jnp.concatenate(
        [turned[group][row : row + 1] for row in range(rows) for group in range(8)], axis=0
    )


def solve(columns, right):
    size = len(right)
    scales = [1.0 / columns[i][i : i + 1, :] for i in range(size)]
    left = [columns[i] * scales[i] for i in range(size)]
    right = [right[i] * scales[i] for i in range(size)]
    start = 0
    for step in range(0, size, 2):
        if step == size // 2 and step % 8 == 0:
            left = [row[step:, :] for row in left]
            start = step
        at = step - start
        top, low, top_right, low_right = left[step], left[step + 1], right[step], right[step + 1]
        first, mixed = top[at : at + 1, :], top[at + 1 : at + 2, :]
        cross, second = low[at : at + 1, :], low[at + 1 : at + 2, :]
        scale = 1.0 / (first * second - mixed * cross)
        aa, ab, ba, bb = second * scale, mixed * scale, cross * scale, first * scale
        one, two = aa * top - ab * low, bb * low - ba * top
        one_right, two_right = aa * top_right - ab * low_right, bb * low_right - ba * top_right
        for i in range(size):
            if i not in (step, step + 1):
                factor, other = left[i][at : at + 1, :], left[i][at + 1 : at + 2, :]
                left[i] = left[i] - (factor * one + other * two)
                right[i] = right[i] - (factor * one_right + other * two_right)
        left[step], left[step + 1], right[step], right[step + 1] = one, two, one_right, two_right
    return right


def columns_of(matrix):
    size = matrix.shape[0]
    return [jnp.broadcast_to(matrix[:, k : k + 1], (size, LANES)) for k in range(size)]


def rows_of(matrix):
    return [matrix[k : k + 1, :] for k in range(matrix.shape[0])]


def weave(columns, rows):
    return tree_sum([column * row for column, row in zip(columns, rows)])


def turn(matrix):
    size = matrix.shape[0]
    return jnp.concatenate([matrix[:, 0:size].T, jnp.zeros((size, LANES - size), F32)], axis=1)


def halves(value):
    high = value.astype(BF16)
    return high, (value - high.astype(F32)).astype(BF16)


def split_dot(left_high, left_low, right_high, right_low, left_dim, right_dim):
    rows = left_high.shape[0]
    both = dot(jnp.concatenate([left_high, left_low], axis=0), right_high, left_dim, right_dim, None)
    return both[0:rows] + both[rows:] + dot(left_high, right_low, left_dim, right_dim, None)


def thirds(value):
    high, low = halves(value)
    return high, low, ((value - high.astype(F32)) - low.astype(F32)).astype(BF16)


def tree_sum(terms):
    while len(terms) > 1:
        terms = [a + b for a, b in zip(terms[0::2], terms[1::2])] + terms[len(terms) & ~1 :]
    return terms[0]


def main_body(sizes, plans, stiff, moduli_hbm, loads_ref, mat_hbm, base_ref, pair_ref, coef_ref,
              stack, low, third, wide, padded, padded_im, mats_rx, ends, ends_rx, field, field_im, wt, wtr, level, node,
              shares_square, shares_cross, shares_quad, shares_last, moduli_ref, mat_ref, credit,
              sent, sent_first, halo_recv, sum_recv, local_sems, vouch_sem):
    cols, nx, ny, nz = loads_ref.shape
    mats = moduli_ref.shape[0]
    me = [lax.axis_index(axis) for axis in AXES]
    k_self, k_edge, k_far = stiff[0], stiff[1], stiff[2]
    assert k_edge == 0.0 and stiff[2] == stiff[3]
    assert 4 * nx * ny <= IDS and nx * ny <= 8 and (nx * ny * nz) % (cols * LANES) == 0 and nz % LANES == 0 and TILE_UNITS % cols == 0
    assert nx >= 2 and ny >= 2
    shares_of = (shares_square, shares_cross, shares_quad, shares_last)
    own = list(itertools.product(range(nx), range(ny)))

    directions = [
        d for d in itertools.product((-1, 0, 1), repeat=3)
        if any(d) and all(step == 0 or sizes[i] > 1 for i, step in enumerate(d))
    ]
    directions.sort(key=lambda d: (-sum(abs(step) for step in d), d[0] == 0))

    def exists(direction):
        good = None
        for i, step in enumerate(direction):
            if step:
                here = (me[i] > 0) if step < 0 else (me[i] < sizes[i] - 1)
                good = here if good is None else jnp.logical_and(good, here)
        return good

    def target(direction):
        return {axis: me[i] + direction[i] for i, axis in enumerate(AXES)}

    def place(direction):
        return 1 - direction[0], 1 - direction[1]

    def spans(step, size, ring):
        if step == 0:
            return pl.ds(2, size), pl.ds(2, size)
        if ring == 0:
            return (pl.ds(size, 2), pl.ds(0, 2)) if step > 0 else (pl.ds(2, 2), pl.ds(size + 2, 2))
        if step > 0:
            return pl.ds(size + 2 - ring, 1), pl.ds(2 - ring, 1)
        return pl.ds(1 + ring, 1), pl.ds(size + 1 + ring, 1)

    def slab(direction, ring_x, ring_y):
        src_x, dst_x = spans(direction[0], nx, ring_x)
        src_y, dst_y = spans(direction[1], ny, ring_y)
        return padded.at[src_x, src_y], padded.at[dst_x, dst_y]

    def halo_start(round_):
        for direction in directions:
            dx, dy, dz = direction
            pairs = []
            if dz == 0:
                if round_ == 0:
                    pairs.append(slab(direction, 1, 1))
                    pairs.append((mats_rx.at[1, 1], mats_rx.at[place(direction)]))
                elif dx and dy:
                    pairs.append(slab(direction, 2, 0))
                    pairs.append(slab(direction, 1, 2))
                else:
                    pairs.append(slab(direction, 2, 2))
            elif round_ == 0:
                pairs.append((ends.at[1 if dz > 0 else 0], ends_rx.at[(*place(direction), 0 if dz > 0 else 1)]))
            else:
                continue

            @pl.when(exists(direction))
            def _():
                for src, dst in pairs:
                    pltpu.make_async_remote_copy(
                        src_ref=src, dst_ref=dst, send_sem=sent if round_ else sent_first, recv_sem=halo_recv.at[round_],
                        device_id=target(direction), device_id_type=pl.DeviceIdType.MESH,
                    ).start()

    def wait_units(total, sem):
        part = credit.at[pl.ds(0, total)]
        pltpu.make_async_copy(part, part, sem).wait()

    def halo_wait(rounds, sem, more=0):
        numbers = [
            ((me[i] > 0).astype(jnp.int32) + (me[i] < sizes[i] - 1).astype(jnp.int32)) for i in range(3)
        ]
        choices = [(0,) if size == 1 else (1,) if size == 2 else (1, 2) for size in sizes]
        per = nz // LANES
        for cx, cy, cz in itertools.product(*choices):
            total, more_units = 0, more
            for round_ in rounds:
                total += per * (cx * ny + cy * nx + (1 if round_ == 0 else 3) * cx * cy)
                if round_ == 0:
                    total += (cx + cy + cx * cy) * (nx * ny * nz // (cols * LANES))
                    more_units += cz * (1 + cx) * (1 + cy) * TILE_UNITS // cols // 2
            total = total * TILE_UNITS // cols + more_units
            if total:
                tests = [numbers[i] == c for i, c in enumerate((cx, cy, cz)) if len(choices[i]) > 1]
                take = functools.partial(wait_units, total, sem)
                if tests:
                    pl.when(functools.reduce(jnp.logical_and, tests))(take)
                else:
                    take()

    def each(count, body):
        if count <= 8:
            for k in range(1, count):
                body(k, 0)
        else:
            lax.fori_loop(1, count, body, 0)

    def group_of(axes):
        count, index = 1, 0
        for axis in axes:
            i = AXES.index(axis)
            count *= sizes[i]
            index = index * sizes[i] + me[i]
        return count, index

    def peer_id(axes, peer):
        coords = {axis: me[i] for i, axis in enumerate(AXES)}
        for axis in reversed(axes):
            size = sizes[AXES.index(axis)]
            coords[axis] = lax.rem(peer, size)
            peer = lax.div(peer, size)
        return coords

    def offset_of(round_, number):
        return sum(group_of(axes)[0] for axes in plans[round_][:number])

    direct = (AXES,) in plans

    barrier = pltpu.get_barrier_semaphore()
    expected = 0
    if direct:
        flat = sizes[0] * sizes[1]
        spot = me[0] * sizes[1] + me[1]
        for dz in (-1, 0, 1):
            good = True if dz == 0 else exists((0, 0, dz))

            def greet(k, carry, dz=dz):
                there = lax.rem(spot + k, flat)
                pl.semaphore_signal(
                    barrier, inc=1, device_id_type=pl.DeviceIdType.MESH,
                    device_id={"gx": lax.div(there, sizes[1]), "gy": lax.rem(there, sizes[1]), "gz": me[2] + dz},
                )
                return carry

            if dz == 0:
                each(flat, greet)
                expected = expected + flat - 1
            elif sizes[2] > 1:
                @pl.when(good)
                def _():
                    greet(0, 0)
                    each(flat, greet)
                expected = expected + jnp.where(good, flat, 0)
    else:
        for axes in plans[0]:
            count, index = group_of(axes)

            def greet(k, carry, axes=axes, count=count, index=index):
                pl.semaphore_signal(barrier, inc=1, device_id=peer_id(axes, lax.rem(index + k, count)),
                                    device_id_type=pl.DeviceIdType.MESH)
                return carry

            each(count, greet)
            expected = expected + count - 1
        for direction in directions:
            good = exists(direction)

            @pl.when(good)
            def _():
                pl.semaphore_signal(barrier, inc=1, device_id=target(direction),
                                    device_id_type=pl.DeviceIdType.MESH)
            expected = expected + jnp.where(good, 1, 0)

    for x, y in own:
        pltpu.make_async_copy(loads_ref.at[:, x, y, :], stack.at[x, y, pl.ds(0, cols), :], local_sems.at[0]).start()
    mat_copy = pltpu.make_async_copy(mat_hbm, mat_ref, local_sems.at[1])
    mat_copy.start()
    moduli_copy = pltpu.make_async_copy(moduli_hbm, moduli_ref, local_sems.at[2])
    moduli_copy.start()

    for direction in itertools.product((-1, 0, 1), repeat=3):
        dx, dy, dz = direction
        if any(direction):
            bx, by = 1 + dx, 1 + dy
            clear = []
            if dz:
                clear.append(ends_rx.at[bx, by, 0 if dz < 0 else 1])
            else:
                x_part = {0: range(2, nx + 2), 1: (nx + 2, nx + 3), -1: (0, 1)}[dx]
                y_part = {0: range(2, ny + 2), 1: (ny + 2, ny + 3), -1: (0, 1)}[dy]
                for x, y in itertools.product(x_part, y_part):
                    clear.append(padded.at[x, y])
                clear.append(mats_rx.at[bx, by])

            def wipe():
                for ref in clear:
                    ref[...] = jnp.zeros(ref.shape, ref.dtype)

            if all(step == 0 or sizes[i] > 1 for i, step in enumerate(direction)):
                pl.when(jnp.logical_not(exists(direction)))(wipe)
            else:
                wipe()

    vouches = max(sizes[2] - 2, 0) if direct else 0

    def vouch(round_):
        for dz in (-1, 1):
            @pl.when(exists((0, 0, dz)))
            def _():
                pl.semaphore_signal(vouch_sem.at[round_, 0 if dz > 0 else 1], inc=1, device_id=target((0, 0, dz)),
                                    device_id_type=pl.DeviceIdType.MESH)

    def vouched(round_):
        for dz in (-1, 1):
            @pl.when(exists((0, 0, dz)))
            def _():
                pl.semaphore_wait(vouch_sem.at[round_, 1 if dz > 0 else 0], 1)

    lane = lax.broadcasted_iota(jnp.int32, (1, LANES), 1)
    id_spot = IDS + 4 * (nx * ny - 1)

    def spread(firsts, lasts, spot, first, last):
        ahead = jnp.logical_and(lane >= spot, lane < spot + 2)
        start = (spot - 2) % LANES
        behind = jnp.logical_and(lane >= start, lane < start + 2)
        return (jnp.where(ahead, pltpu.roll(first, spot, 1), firsts),
                jnp.where(behind, pltpu.roll(last, spot, 1), lasts))

    mat_copy.wait()
    ids = jnp.concatenate([mat_ref[x] for x in range(nx)], axis=0)
    ids = (ids + 1).astype(F32)
    mats_rx[1, 1] = ids.astype(BF16)
    firsts = lasts = jnp.zeros((cols, LANES), F32)
    for x, y in own:
        row = x * ny + y
        first = jnp.broadcast_to(ids[row : row + 1, 0:LANES], (cols, LANES))
        last = jnp.broadcast_to(ids[row : row + 1, nz - LANES : nz], (cols, LANES))
        firsts, lasts = spread(firsts, lasts, id_spot - 4 * row, first, last)
    whole = stack.at[:, :, pl.ds(0, cols), :]
    pltpu.make_async_copy(whole, whole, local_sems.at[0]).wait()
    for x, y in own:
        values = stack[x, y, 0:cols, :]
        padded[x + 2, y + 2] = values.astype(BF16)
        firsts, lasts = spread(firsts, lasts, 4 * (x * ny + y), values[:, 0:LANES], values[:, nz - LANES : nz])
    upper = cols // 2
    for side, tile in enumerate((firsts, lasts)):
        lower_half = jnp.logical_and(lane >= 2 * LANES // 4 - 2, lane < LANES - 2)
        ends[side] = jnp.where(lower_half, pltpu.roll(tile[upper:], LANES // 2, 1), tile[0:upper]).astype(BF16)
    pl.semaphore_wait(barrier, expected)
    halo_start(0)
    if vouches:
        vouch(0)

    def gram(left, right):
        return tree_sum([split_dot(*left(x, y), *right(x, y), 1, 1) for x, y in own])

    def sum_copy(round_, number, peer):
        axes = plans[round_][number]
        count, index = group_of(axes)
        slot = offset_of(round_, number) + index
        return pltpu.make_async_remote_copy(
            src_ref=shares_of[round_].at[slot], dst_ref=shares_of[round_].at[slot],
            send_sem=sent, recv_sem=sum_recv.at[arrival(round_, number)],
            device_id=peer, device_id_type=pl.DeviceIdType.MESH,
        )

    def sum_start(round_, number, tile):
        axes = plans[round_][number]
        count, index = group_of(axes)
        shares_of[round_][offset_of(round_, number) + index] = tile
        if axes == AXES:
            plane = []
            for k in range(flat):
                there = lax.rem(spot + k, flat)
                plane.append((lax.div(there, sizes[1]), lax.rem(there, sizes[1])))
            low = 2 * me[2] < sizes[2]
            far, turn = jnp.where(low, sizes[2] - 1, 0), jnp.where(low, -1, 1)
            away = jnp.where(low, sizes[2] - 1 - me[2], me[2])
            for i in range(sizes[2] - 1):
                level = far + turn * (i + jnp.where(i < away, 0, 1))
                for gx, gy in plane[::-1]:
                    sum_copy(round_, number, {"gx": gx, "gy": gy, "gz": level}).start()
            for gx, gy in plane[:0:-1]:
                sum_copy(round_, number, {"gx": gx, "gy": gy, "gz": me[2]}).start()
        else:
            def send(k, carry):
                sum_copy(round_, number, peer_id(axes, lax.rem(index + k, count))).start()
                return carry

            each(count, send)

    def arrival(round_, number):
        return sum(len(phases) for phases in plans[:round_]) + number

    def sum_units(round_, number):
        return (group_of(plans[round_][number])[0] - 1)

    def sum_finish(round_, number):
        total = sum_units(round_, number)
        if total:
            wait_units(total, sum_recv.at[arrival(round_, number)])
        start = offset_of(round_, number)
        return tree_sum([shares_of[round_][start + peer] for peer in range(group_of(plans[round_][number])[0])])

    def sum_turn(round_):
        for number in range(1, len(plans[round_])):
            sum_start(round_, number, sum_finish(round_, number - 1))

    def sum_rest(round_):
        return sum_finish(round_, len(plans[round_]) - 1)

    def loads_at(x, y):
        return stack[x, y, 0:cols, :]

    def image_at(x, y):
        return stack[x, y, cols:, :]

    for x, y in own:
        low[x, y, 0:cols, :] = (loads_at(x, y) - padded[x + 2, y + 2].astype(F32)).astype(BF16)

    def loads_split(x, y):
        return padded[x + 2, y + 2], low[x, y, 0:cols, :]

    def image_split(x, y):
        return padded_im[x, y], low[x, y, cols:, :]

    square_part = gram(loads_split, loads_split)
    sum_start(0, 0, pack(square_part))
    for round_ in range(1, vouches):
        vouched(round_ - 1)
        vouch(round_)
    halo_wait((0,), sent_first)
    halo_start(1)
    moduli_copy.wait()

    def block_of(x, y):
        bx, lx = (0, nx - 2 + x) if x < 2 else (2, x - nx - 2) if x >= nx + 2 else (1, x - 2)
        by, ly = (0, ny - 2 + y) if y < 2 else (2, y - ny - 2) if y >= ny + 2 else (1, y - 2)
        return bx, by, lx * ny + ly

    odd = lax.rem(lane, 4) >= 2

    def merged(edge):
        return {
            (bx, by): jnp.where(odd, edge[bx, by, 0].astype(F32), edge[bx, by, 1].astype(F32))
            for bx, by in itertools.product(range(3), repeat=2)
        }

    def tail_of(tiles, x, y):
        bx, by, row = block_of(x, y)
        tile = tiles[bx, by]
        near, far = ((2 * LANES - spot - 4 * row) % LANES for spot in (0, LANES // 2))
        return jnp.concatenate([pltpu.roll(tile, near, 1), pltpu.roll(tile, far, 1)], axis=0)

    def modulus_of(ids):
        found = jnp.zeros(ids.shape, F32)
        for number in range(mats):
            found = jnp.where(ids == float(number + 1), moduli_ref[number], found)
        return found

    own_modulus = modulus_of(mats_rx[1, 1].astype(F32))
    halo_wait((0,), halo_recv.at[0])
    if vouches:
        vouched(vouches - 1)
    sum_turn(0)
    full = nz + LANES
    tails = merged(ends_rx)
    dense = {}
    for key in tails:
        flat_ids = own_modulus if key == (1, 1) else modulus_of(mats_rx[key].astype(F32))
        side = pltpu.roll(modulus_of(tails[key]), LANES - id_spot, 1, stride=4, stride_axis=0)
        both = jnp.concatenate([flat_ids, side], axis=1)
        dense[key] = ((0.125 * k_far) * (both + pltpu.roll(both, full - 1, 1)),
                      (0.125 * k_far) * (both + pltpu.roll(both, 1, 1)))
    sums = {}

    def sum_at(x, y):
        if (x, y) not in sums:
            bx, by, row = block_of(x, y)
            sums[x, y] = [jnp.broadcast_to(part[row : row + 1, :], (8, full)) for part in dense[bx, by]]
        return sums[x, y]

    def weigh(x, y):
        around = [sum_at(x, y), sum_at(x, y + 1), sum_at(x + 1, y), sum_at(x + 1, y + 1)]
        after, before = (tree_sum([pair[side] for pair in around]) for side in range(2))
        wt[x, y], wtr[x, y], level[x, y] = after, before, before + after

    def around_of(weights, x, y):
        return (weights[x, y] + weights[x, y + 1]) + (weights[x + 1, y] + weights[x + 1, y + 1])

    def gather(x, y):
        above, below = around_of(wtr, x, y), around_of(wt, x, y)
        node[0, x, y], node[1, x, y], node[2, x, y] = above, below, (k_self / k_far) * (above + below)

    def unfold(x, y):
        field[x, y] = jnp.concatenate([padded[x, y].astype(F32), tail_of(tails, x, y)], axis=1)

    inner = list(itertools.product(range(1, nx + 1), range(1, ny + 1)))
    outer = [key for key in itertools.product(range(nx + 2), range(ny + 2)) if key not in inner]
    near = list(itertools.product(range(1, nx + 3), range(1, ny + 3)))
    near_elements = list(itertools.product(range(1, nx + 2), range(1, ny + 2)))
    for key in near:
        unfold(*key)
    for key in near_elements:
        weigh(*key)
    for key in inner:
        gather(*key)

    def double(tile):
        return jnp.concatenate([tile, tile], axis=0)

    def operate(source, shift, cells, direction_of, write, width):
        lines, ahead_of, behind_of = {}, {}, {}

        def line(x, y):
            if (x, y) not in lines:
                lines[x, y] = source[x - shift, y - shift] + source[x - shift, y + 1 - shift]
            return lines[x, y]

        for x, y in cells:
            here = source[x + 1 - shift, y + 1 - shift]
            corners = list(itertools.product((x, x + 1), (y, y + 1)))
            flats = []
            for ex, ey in corners:
                if (ex, ey) not in ahead_of:
                    corner_sum = line(ex, ey) + line(ex + 1, ey)
                    ahead_of[ex, ey] = double(wtr[ex, ey]) * corner_sum
                    behind_of[ex, ey] = double(wt[ex, ey]) * corner_sum
                opposite = source[2 * ex - x - shift, 2 * ey - y - shift][:, 0:width]
                flats.append(double(level[ex, ey, :, 0:width]) * opposite)
            ahead = tree_sum([ahead_of[key] for key in corners]) - double(node[0, x, y]) * here
            behind = tree_sum([behind_of[key] for key in corners]) - double(node[1, x, y]) * here
            around = pltpu.roll(ahead, full - 1, 1)[:, 0:width] + pltpu.roll(behind, 1, 1)[:, 0:width]
            centre = double(node[2, x, y, :, 0:width]) * here[:, 0:width]
            write(x, y, SIGMA * direction_of(x, y) + (around + tree_sum(flats) + centre))

    has_right = (me[2] < sizes[2] - 1).astype(jnp.int32)
    has_left = (me[2] > 0).astype(jnp.int32)
    beyond = jnp.logical_or(lane < has_right, lane >= LANES - has_left)

    def write_first(x, y, image):
        main = image[:, 0:nz]
        stack[x - 1, y - 1, cols:, :] = main
        padded_im[x - 1, y - 1], low[x - 1, y - 1, cols:, :] = halves(main)
        field_im[x, y] = jnp.concatenate([main, jnp.where(beyond, image[:, nz:], 0.0)], axis=1)

    def loads_wide(x, y):
        return jnp.concatenate([loads_at(x - 1, y - 1), field[x + 1, y + 1][:, nz:]], axis=1)

    operate(field, 0, inner, loads_wide, write_first, full)

    def pair_split(x, y):
        return jnp.concatenate([padded[x + 2, y + 2], padded_im[x, y]], axis=0), low[x, y]

    both_part = gram(image_split, pair_split)
    sum_start(1, 0, pack(both_part[:, 0:cols]))
    sum_start(2, 0, pack(both_part[:, cols:]))
    for key in itertools.product(range(nx + 3), range(ny + 3)):
        if key not in near_elements:
            weigh(*key)
    for key in outer:
        gather(*key)
    halo_wait((1,), halo_recv.at[1])
    for key in itertools.product(range(nx + 4), range(ny + 4)):
        if key not in near:
            unfold(*key)

    def write_ring(x, y, image):
        dx = -1 if x == 0 else 1 if x == nx + 1 else 0
        dy = -1 if y == 0 else 1 if y == ny + 1 else 0
        if any(step and sizes[i] == 1 for i, step in enumerate((dx, dy))):
            field_im[x, y] = jnp.zeros(image.shape, F32)
        else:
            image = jnp.where(exists((dx, dy, 0)), image, 0.0)
            field_im[x, y] = jnp.concatenate([image[:, 0:nz], jnp.where(beyond, image[:, nz:], 0.0)], axis=1)

    operate(field, 0, outer, lambda x, y: field[x + 1, y + 1], write_ring, full)
    last_parts = []

    def write_last(x, y, image):
        last_parts.append(split_dot(*image_split(x - 1, y - 1), *halves(image), 1, 1))

    operate(field_im, 1, inner, lambda x, y: image_at(x - 1, y - 1), write_last, nz)
    sum_start(3, 0, pack(tree_sum(last_parts)))

    square = unpack(sum_rest(0), cols)
    sum_turn(1)
    sum_turn(2)
    row_id = lax.broadcasted_iota(jnp.int32, (cols, LANES), 0)
    col_id = lax.broadcasted_iota(jnp.int32, (cols, LANES), 1)
    eye = jnp.where(row_id == col_id, 1.0, 0.0)
    inverse = solve(columns_of(square), rows_of(eye))
    cells = list(itertools.product(range(nx + 2), range(ny + 2)))
    for x, y in cells:
        wide[x, y, 0:cols, :] = field[x + 1, y + 1].astype(BF16)
        wide[x, y, cols:, :] = field_im[x, y].astype(BF16)
    for x, y in own:
        high = jnp.concatenate([padded[x + 2, y + 2], padded_im[x, y]], axis=0).astype(F32)
        third[x, y] = ((stack[x, y] - high) - low[x, y].astype(F32)).astype(BF16)

    def mixture(parts, cell, rows):
        x, y = cell
        if cell not in inner:
            product = dot(jnp.concatenate(parts[0:2], axis=0), wide[x, y, rows, :], 1, 0, None)
            return product[0:cols] + product[cols:]
        one = dot(jnp.concatenate(parts, axis=0), wide[x, y, rows, :], 1, 0, None)
        two = dot(jnp.concatenate(parts[0:2], axis=0), low[x - 1, y - 1, rows, :], 1, 0, None)
        three = dot(parts[0], third[x - 1, y - 1, rows, :], 1, 0, None)
        small = (one[cols : 2 * cols, 0:nz] + two[0:cols]) + ((one[2 * cols :, 0:nz] + two[cols:]) + three)
        return jnp.concatenate([one[0:cols, 0:nz] + small, one[0:cols, nz:] + one[cols : 2 * cols, nz:]], axis=1)

    cross = unpack(sum_rest(1), cols)
    cross = 0.5 * (cross + turn(cross))
    cross_columns = columns_of(cross)
    alpha_rows = solve(cross_columns, rows_of(square))
    alpha_t = turn(jnp.concatenate(alpha_rows, axis=0))
    alpha_columns = columns_of(alpha_t)
    quad = unpack(sum_rest(2), cols)
    moved, stood = weave(columns_of(quad), alpha_rows), weave(cross_columns, alpha_rows)
    alpha_t = alpha_t[:, 0:cols]
    alpha_split = halves(alpha_t)
    alpha_parts = thirds(alpha_t)
    for cell in cells:
        x, y = cell
        base = field[x + 1, y + 1]
        if cell in inner:
            base = jnp.concatenate([loads_at(x - 1, y - 1), base[:, nz:]], axis=1)
        field_im[x, y] = base - mixture(alpha_parts, cell, slice(cols, 2 * cols))
    updated = square + weave(alpha_columns, rows_of(moved)) - (stood + turn(stood))
    beta_t = weave(columns_of(updated), inverse)
    grown_t = eye + beta_t
    grown_columns = columns_of(grown_t)
    joint = weave(grown_columns, rows_of(moved))
    known = weave(columns_of(weave(grown_columns, rows_of(cross))), rows_of(turn(grown_t))) - (joint + turn(joint))
    beta_t = beta_t[:, 0:cols]
    beta_parts = thirds(beta_t)
    for cell in cells:
        x, y = cell
        rest = field_im[x, y]
        direction = rest + mixture(beta_parts, cell, slice(0, cols))
        rounded = direction.astype(BF16)
        field_im[x, y] = rounded.astype(F32)
        if cell in inner:
            base_ref[x - 1, y - 1, cols:, :] = rest[:, 0:nz]
            direction, rounded = direction[:, 0:nz], rounded[:, 0:nz]
            stack[x - 1, y - 1, cols:, :] = direction
            pair_ref[x - 1, y - 1, 0, 0:cols, :] = rounded
            pair_ref[x - 1, y - 1, 0, cols:, :] = (direction - rounded.astype(F32)).astype(BF16)

    halo_wait((1,), sent, sum(
        sum_units(round_, number) for round_ in range(4) for number in range(len(plans[round_]))
        if (round_, number) != (3, 1)
    ))
    sum_turn(3)
    last = unpack(sum_rest(3), cols)
    total = known + weave(alpha_columns, rows_of(weave(columns_of(last), alpha_rows)))
    last_rows = solve(columns_of(total), rows_of(updated))
    coef_t = jnp.concatenate(last_rows, axis=0)[:, 0:cols].T
    coef_ref[0:cols, :], coef_ref[cols:, :] = halves(coef_t)

    def write_second(x, y, image):
        pair_ref[x - 1, y - 1, 1, 0:cols, :], pair_ref[x - 1, y - 1, 1, cols:, :] = halves(image)

    operate(field_im, 1, inner, lambda x, y: image_at(x - 1, y - 1), write_second, nz)
    for x, y in own:
        base_ref[x, y, 0:cols, :] = split_dot(*alpha_split, *loads_split(x, y), 1, 0)
    if len(plans[3]) > 1:
        wait_units(sum_units(3, 1), sent)


def last_body(coef_ref, base_ref, pair_ref, sol_ref, res_ref, stage, sems):
    cols, nx, ny, nz = sol_ref.shape
    high, low = coef_ref[0:cols, :], coef_ref[cols:, :]
    for x in range(nx):
        for which, ref, sign in ((0, sol_ref, 1.0), (1, res_ref, -1.0)):
            rows = slice(which * cols, (which + 1) * cols)
            for y in range(ny):
                added = split_dot(high, low, pair_ref[x, y, which, 0:cols, :], pair_ref[x, y, which, cols:, :], 1, 0)
                stage[which, :, x, y, :] = base_ref[x, y, rows, :] + sign * added
            pltpu.make_async_copy(stage.at[which, :, x], ref.at[:, x], sems.at[which]).start()
    for which in range(2):
        pltpu.make_async_copy(stage.at[which], stage.at[which], sems.at[which]).wait()


def on_device(sizes, loads, moduli, material):
    cols, nx, ny, nz = loads.shape
    count = int(np.prod(sizes))
    split = (("gx", "gy"), ("gz",))
    quick = (AXES,) if count <= DIRECT_LIMIT else split
    plans = (split, quick, quick, quick)

    def slots(phases):
        return sum(int(np.prod([sizes[AXES.index(a)] for a in axes])) for axes in phases)

    vmem = pl.BlockSpec(memory_space=pltpu.VMEM)
    anywhere = pl.BlockSpec(memory_space=pl.ANY)
    full = nz + LANES
    tiles = (nz // LANES) * 4 * (nx + ny + 4) + 18 + 8 * (nx * ny * nz // (cols * LANES))
    credits = tiles * TILE_UNITS // cols + 2 * sum(slots(phases) for phases in plans)
    base, pair, coef = pl.pallas_call(
        functools.partial(main_body, sizes, plans, stiffness_values()),
        out_shape=(
            pltpu.VMEM((nx, ny, 2 * cols, nz), F32),
            pltpu.VMEM((nx, ny, 2, 2 * cols, nz), BF16),
            pltpu.VMEM((2 * cols, cols), BF16),
        ),
        in_specs=[anywhere, anywhere, anywhere],
        out_specs=(vmem, vmem, vmem),
        scratch_shapes=[
            pltpu.VMEM((nx, ny, 2 * cols, nz), F32),
            pltpu.VMEM((nx, ny, 2 * cols, nz), BF16),
            pltpu.VMEM((nx, ny, 2 * cols, nz), BF16),
            pltpu.VMEM((nx + 2, ny + 2, 2 * cols, full), BF16),
            pltpu.VMEM((nx + 4, ny + 4, cols, nz), BF16),
            pltpu.VMEM((nx, ny, cols, nz), BF16),
            pltpu.VMEM((3, 3, nx * ny, nz), BF16),
            pltpu.VMEM((2, cols // 2, LANES), BF16),
            pltpu.VMEM((3, 3, 2, cols // 2, LANES), BF16),
            pltpu.VMEM((nx + 4, ny + 4, cols, full), F32),
            pltpu.VMEM((nx + 2, ny + 2, cols, full), F32),
            pltpu.VMEM((nx + 3, ny + 3, 8, full), F32),
            pltpu.VMEM((nx + 3, ny + 3, 8, full), F32),
            pltpu.VMEM((nx + 3, ny + 3, 8, full), F32),
            pltpu.VMEM((3, nx + 2, ny + 2, 8, full), F32),
            pltpu.VMEM((slots(plans[0]), cols * cols // LANES, LANES), F32),
            pltpu.VMEM((slots(plans[1]), cols * cols // LANES, LANES), F32),
            pltpu.VMEM((slots(plans[2]), cols * cols // LANES, LANES), F32),
            pltpu.VMEM((slots(plans[3]), cols * cols // LANES, LANES), F32),
            pltpu.SMEM(moduli.shape, F32),
            pltpu.VMEM(material.shape, jnp.int32),
            pltpu.VMEM((credits, cols * cols // LANES, LANES), F32),
            pltpu.SemaphoreType.DMA,
            pltpu.SemaphoreType.DMA,
            pltpu.SemaphoreType.DMA((2,)),
            pltpu.SemaphoreType.DMA((sum(len(phases) for phases in plans),)),
            pltpu.SemaphoreType.DMA((3,)),
            pltpu.SemaphoreType.REGULAR((max(sizes[2] - 2, 1) if count <= DIRECT_LIMIT else 1, 2)),
        ],
        compiler_params=pltpu.CompilerParams(collective_id=0, has_side_effects=True),
    )(moduli, loads, material)
    out = jax.ShapeDtypeStruct(loads.shape, F32)
    return pl.pallas_call(
        last_body,
        out_shape=(out, out),
        in_specs=[vmem, vmem, vmem],
        out_specs=(anywhere, anywhere),
        scratch_shapes=[pltpu.VMEM((2, cols, nx, ny, nz), F32), pltpu.SemaphoreType.DMA((2,))],
        compiler_params=pltpu.CompilerParams(vmem_limit_bytes=4 * 2**20),
    )(coef, base, pair)


def solution(mesh):
    sizes = tuple(mesh.shape[axis] for axis in AXES)
    in_specs = (P(None, "gx", "gy", "gz"), P(), P("gx", "gy", "gz"))
    out_specs = (P(None, "gx", "gy", "gz"), P(None, "gx", "gy", "gz"))
    return jax.shard_map(
        functools.partial(on_device, sizes), mesh=mesh, in_specs=in_specs, out_specs=out_specs, check_vma=False
    )
```

```python
import functools
import itertools

import jax
import jax.numpy as jnp
import numpy as np
from jax import lax
from jax.experimental import pallas as pl
from jax.experimental.pallas import tpu as pltpu
from jax.sharding import PartitionSpec as P

SIGMA = 0.25
AXES = ("gx", "gy", "gz")
HIGH = lax.Precision.HIGHEST
F32 = jnp.float32
BF16 = jnp.bfloat16
LANES = 128
DIRECT_LIMIT = 32
IDS = 32
TILE_UNITS = 64


def stiffness_values():
    mass = (1.0 / 3.0, 1.0 / 6.0)
    stiff = (1.0, -1.0)
    values = []
    for differing in range(4):
        bits = [1 if dim < differing else 0 for dim in range(3)]
        total = 0.0
        for dim in range(3):
            factor = 1.0
            for other in range(3):
                factor *= stiff[bits[other]] if other == dim else mass[bits[other]]
            total += factor
        values.append(float(np.asarray(total, np.float32).astype(jnp.bfloat16).astype(np.float32)))
    return values


def dot(left, right, left_dim, right_dim, precision=HIGH):
    return lax.dot_general(
        left, right, (((left_dim,), (right_dim,)), ((), ())), precision=precision, preferred_element_type=F32
    )


def pack(matrix):
    rows, cols = matrix.shape
    wide = jnp.concatenate([matrix, jnp.zeros((rows, LANES - cols), F32)], axis=1)
    pieces = [
        jnp.sum(pltpu.roll(wide[start : start + 8], 0, 1, stride=cols, stride_axis=0), axis=0, keepdims=True)
        for start in range(0, rows, 8)
    ]
    return jnp.concatenate(pieces, axis=0)


def unpack(tile, cols):
    rows = tile.shape[0]
    tall = jnp.concatenate([tile, jnp.zeros((8 - rows, LANES), F32)], axis=0)
    turned = [tall] + [pltpu.roll(tall, LANES - cols * group, 1) for group in range(1, 8)]
    return jnp.concatenate(
        [turned[group][row : row + 1] for row in range(rows) for group in range(8)], axis=0
    )


def solve(columns, right):
    size = len(right)
    scales = [1.0 / columns[i][i : i + 1, :] for i in range(size)]
    left = [columns[i] * scales[i] for i in range(size)]
    right = [right[i] * scales[i] for i in range(size)]
    start = 0
    for step in range(0, size, 2):
        if step == size // 2 and step % 8 == 0:
            left = [row[step:, :] for row in left]
            start = step
        at = step - start
        top, low, top_right, low_right = left[step], left[step + 1], right[step], right[step + 1]
        first, mixed = top[at : at + 1, :], top[at + 1 : at + 2, :]
        cross, second = low[at : at + 1, :], low[at + 1 : at + 2, :]
        scale = 1.0 / (first * second - mixed * cross)
        aa, ab, ba, bb = second * scale, mixed * scale, cross * scale, first * scale
        one, two = aa * top - ab * low, bb * low - ba * top
        one_right, two_right = aa * top_right - ab * low_right, bb * low_right - ba * top_right
        for i in range(size):
            if i not in (step, step + 1):
                factor, other = left[i][at : at + 1, :], left[i][at + 1 : at + 2, :]
                left[i] = left[i] - (factor * one + other * two)
                right[i] = right[i] - (factor * one_right + other * two_right)
        left[step], left[step + 1], right[step], right[step + 1] = one, two, one_right, two_right
    return right


def columns_of(matrix):
    size = matrix.shape[0]
    return [jnp.broadcast_to(matrix[:, k : k + 1], (size, LANES)) for k in range(size)]


def rows_of(matrix):
    return [matrix[k : k + 1, :] for k in range(matrix.shape[0])]


def weave(columns, rows):
    return tree_sum([column * row for column, row in zip(columns, rows)])


def turn(matrix):
    size = matrix.shape[0]
    return jnp.concatenate([matrix[:, 0:size].T, jnp.zeros((size, LANES - size), F32)], axis=1)


def halves(value):
    high = value.astype(BF16)
    return high, (value - high.astype(F32)).astype(BF16)


def split_dot(left_high, left_low, right_high, right_low, left_dim, right_dim):
    rows = left_high.shape[0]
    both = dot(jnp.concatenate([left_high, left_low], axis=0), right_high, left_dim, right_dim, None)
    return both[0:rows] + both[rows:] + dot(left_high, right_low, left_dim, right_dim, None)


def thirds(value):
    high, low = halves(value)
    return high, low, ((value - high.astype(F32)) - low.astype(F32)).astype(BF16)


def tree_sum(terms):
    while len(terms) > 1:
        terms = [a + b for a, b in zip(terms[0::2], terms[1::2])] + terms[len(terms) & ~1 :]
    return terms[0]


def main_body(sizes, plans, stiff, moduli_hbm, loads_ref, mat_hbm, base_ref, pair_ref, coef_ref,
              stack, low, third, wide, padded, padded_im, mats_rx, ends, ends_rx, field, field_im, wt, wtr, level, node,
              shares_square, shares_cross, shares_quad, shares_last, moduli_ref, mat_ref, credit,
              sent, sent_first, halo_recv, sum_recv, local_sems, vouch_sem):
    cols, nx, ny, nz = loads_ref.shape
    mats = moduli_ref.shape[0]
    me = [lax.axis_index(axis) for axis in AXES]
    k_self, k_edge, k_far = stiff[0], stiff[1], stiff[2]
    assert k_edge == 0.0 and stiff[2] == stiff[3]
    assert 4 * nx * ny <= IDS and nx * ny <= 8 and (nx * ny * nz) % (cols * LANES) == 0 and nz % LANES == 0 and TILE_UNITS % cols == 0
    assert nx >= 2 and ny >= 2
    shares_of = (shares_square, shares_cross, shares_quad, shares_last)
    own = list(itertools.product(range(nx), range(ny)))

    directions = [
        d for d in itertools.product((-1, 0, 1), repeat=3)
        if any(d) and all(step == 0 or sizes[i] > 1 for i, step in enumerate(d))
    ]
    directions.sort(key=lambda d: (-sum(abs(step) for step in d), d[0] == 0))

    def exists(direction):
        good = None
        for i, step in enumerate(direction):
            if step:
                here = (me[i] > 0) if step < 0 else (me[i] < sizes[i] - 1)
                good = here if good is None else jnp.logical_and(good, here)
        return good

    def target(direction):
        return {axis: me[i] + direction[i] for i, axis in enumerate(AXES)}

    def place(direction):
        return 1 - direction[0], 1 - direction[1]

    def spans(step, size, ring):
        if step == 0:
            return pl.ds(2, size), pl.ds(2, size)
        if ring == 0:
            return (pl.ds(size, 2), pl.ds(0, 2)) if step > 0 else (pl.ds(2, 2), pl.ds(size + 2, 2))
        if step > 0:
            return pl.ds(size + 2 - ring, 1), pl.ds(2 - ring, 1)
        return pl.ds(1 + ring, 1), pl.ds(size + 1 + ring, 1)

    def slab(direction, ring_x, ring_y):
        src_x, dst_x = spans(direction[0], nx, ring_x)
        src_y, dst_y = spans(direction[1], ny, ring_y)
        return padded.at[src_x, src_y], padded.at[dst_x, dst_y]

    def halo_start(round_):
        for direction in directions:
            dx, dy, dz = direction
            pairs = []
            if dz == 0:
                if round_ == 0:
                    pairs.append(slab(direction, 1, 1))
                    pairs.append((mats_rx.at[1, 1], mats_rx.at[place(direction)]))
                elif dx and dy:
                    pairs.append(slab(direction, 2, 0))
                    pairs.append(slab(direction, 1, 2))
                else:
                    pairs.append(slab(direction, 2, 2))
            elif round_ == 0:
                pairs.append((ends.at[1 if dz > 0 else 0], ends_rx.at[(*place(direction), 0 if dz > 0 else 1)]))
            else:
                continue

            @pl.when(exists(direction))
            def _():
                for src, dst in pairs:
                    pltpu.make_async_remote_copy(
                        src_ref=src, dst_ref=dst, send_sem=sent if round_ else sent_first, recv_sem=halo_recv.at[round_],
                        device_id=target(direction), device_id_type=pl.DeviceIdType.MESH,
                    ).start()

    def wait_units(total, sem):
        part = credit.at[pl.ds(0, total)]
        pltpu.make_async_copy(part, part, sem).wait()

    def halo_wait(rounds, sem, more=0):
        numbers = [
            ((me[i] > 0).astype(jnp.int32) + (me[i] < sizes[i] - 1).astype(jnp.int32)) for i in range(3)
        ]
        choices = [(0,) if size == 1 else (1,) if size == 2 else (1, 2) for size in sizes]
        per = nz // LANES
        for cx, cy, cz in itertools.product(*choices):
            total, more_units = 0, more
            for round_ in rounds:
                total += per * (cx * ny + cy * nx + (1 if round_ == 0 else 3) * cx * cy)
                if round_ == 0:
                    total += (cx + cy + cx * cy) * (nx * ny * nz // (cols * LANES))
                    more_units += cz * (1 + cx) * (1 + cy) * TILE_UNITS // cols // 2
            total = total * TILE_UNITS // cols + more_units
            if total:
                tests = [numbers[i] == c for i, c in enumerate((cx, cy, cz)) if len(choices[i]) > 1]
                take = functools.partial(wait_units, total, sem)
                if tests:
                    pl.when(functools.reduce(jnp.logical_and, tests))(take)
                else:
                    take()

    def each(count, body):
        if count <= 8:
            for k in range(1, count):
                body(k, 0)
        else:
            lax.fori_loop(1, count, body, 0)

    def group_of(axes):
        count, index = 1, 0
        for axis in axes:
            i = AXES.index(axis)
            count *= sizes[i]
            index = index * sizes[i] + me[i]
        return count, index

    def peer_id(axes, peer):
        coords = {axis: me[i] for i, axis in enumerate(AXES)}
        for axis in reversed(axes):
            size = sizes[AXES.index(axis)]
            coords[axis] = lax.rem(peer, size)
            peer = lax.div(peer, size)
        return coords

    def offset_of(round_, number):
        return sum(group_of(axes)[0] for axes in plans[round_][:number])

    direct = (AXES,) in plans

    barrier = pltpu.get_barrier_semaphore()
    expected = 0
    if direct:
        flat = sizes[0] * sizes[1]
        spot = me[0] * sizes[1] + me[1]
        for dz in (-1, 0, 1):
            good = True if dz == 0 else exists((0, 0, dz))

            def greet(k, carry, dz=dz):
                there = lax.rem(spot + k, flat)
                pl.semaphore_signal(
                    barrier, inc=1, device_id_type=pl.DeviceIdType.MESH,
                    device_id={"gx": lax.div(there, sizes[1]), "gy": lax.rem(there, sizes[1]), "gz": me[2] + dz},
                )
                return carry

            if dz == 0:
                each(flat, greet)
                expected = expected + flat - 1
            elif sizes[2] > 1:
                @pl.when(good)
                def _():
                    greet(0, 0)
                    each(flat, greet)
                expected = expected + jnp.where(good, flat, 0)
    else:
        for axes in plans[0]:
            count, index = group_of(axes)

            def greet(k, carry, axes=axes, count=count, index=index):
                pl.semaphore_signal(barrier, inc=1, device_id=peer_id(axes, lax.rem(index + k, count)),
                                    device_id_type=pl.DeviceIdType.MESH)
                return carry

            each(count, greet)
            expected = expected + count - 1
        for direction in directions:
            good = exists(direction)

            @pl.when(good)
            def _():
                pl.semaphore_signal(barrier, inc=1, device_id=target(direction),
                                    device_id_type=pl.DeviceIdType.MESH)
            expected = expected + jnp.where(good, 1, 0)

    for x, y in own:
        pltpu.make_async_copy(loads_ref.at[:, x, y, :], stack.at[x, y, pl.ds(0, cols), :], local_sems.at[0]).start()
    mat_copy = pltpu.make_async_copy(mat_hbm, mat_ref, local_sems.at[1])
    mat_copy.start()
    moduli_copy = pltpu.make_async_copy(moduli_hbm, moduli_ref, local_sems.at[2])
    moduli_copy.start()

    for direction in itertools.product((-1, 0, 1), repeat=3):
        dx, dy, dz = direction
        if any(direction):
            bx, by = 1 + dx, 1 + dy
            clear = []
            if dz:
                clear.append(ends_rx.at[bx, by, 0 if dz < 0 else 1])
            else:
                x_part = {0: range(2, nx + 2), 1: (nx + 2, nx + 3), -1: (0, 1)}[dx]
                y_part = {0: range(2, ny + 2), 1: (ny + 2, ny + 3), -1: (0, 1)}[dy]
                for x, y in itertools.product(x_part, y_part):
                    clear.append(padded.at[x, y])
                clear.append(mats_rx.at[bx, by])

            def wipe():
                for ref in clear:
                    ref[...] = jnp.zeros(ref.shape, ref.dtype)

            if all(step == 0 or sizes[i] > 1 for i, step in enumerate(direction)):
                pl.when(jnp.logical_not(exists(direction)))(wipe)
            else:
                wipe()

    vouches = max(sizes[2] - 2, 0) if direct else 0

    def vouch(round_):
        for dz in (-1, 1):
            @pl.when(exists((0, 0, dz)))
            def _():
                pl.semaphore_signal(vouch_sem.at[round_, 0 if dz > 0 else 1], inc=1, device_id=target((0, 0, dz)),
                                    device_id_type=pl.DeviceIdType.MESH)

    def vouched(round_):
        for dz in (-1, 1):
            @pl.when(exists((0, 0, dz)))
            def _():
                pl.semaphore_wait(vouch_sem.at[round_, 1 if dz > 0 else 0], 1)

    lane = lax.broadcasted_iota(jnp.int32, (1, LANES), 1)
    id_spot = IDS + 4 * (nx * ny - 1)

    def spread(firsts, lasts, spot, first, last):
        ahead = jnp.logical_and(lane >= spot, lane < spot + 2)
        start = (spot - 2) % LANES
        behind = jnp.logical_and(lane >= start, lane < start + 2)
        return (jnp.where(ahead, pltpu.roll(first, spot, 1), firsts),
                jnp.where(behind, pltpu.roll(last, spot, 1), lasts))

    mat_copy.wait()
    ids = jnp.concatenate([mat_ref[x] for x in range(nx)], axis=0)
    ids = (ids + 1).astype(F32)
    mats_rx[1, 1] = ids.astype(BF16)
    firsts = lasts = jnp.zeros((cols, LANES), F32)
    for x, y in own:
        row = x * ny + y
        first = jnp.broadcast_to(ids[row : row + 1, 0:LANES], (cols, LANES))
        last = jnp.broadcast_to(ids[row : row + 1, nz - LANES : nz], (cols, LANES))
        firsts, lasts = spread(firsts, lasts, id_spot - 4 * row, first, last)
    whole = stack.at[:, :, pl.ds(0, cols), :]
    pltpu.make_async_copy(whole, whole, local_sems.at[0]).wait()
    for x, y in own:
        values = stack[x, y, 0:cols, :]
        padded[x + 2, y + 2] = values.astype(BF16)
        firsts, lasts = spread(firsts, lasts, 4 * (x * ny + y), values[:, 0:LANES], values[:, nz - LANES : nz])
    upper = cols // 2
    for side, tile in enumerate((firsts, lasts)):
        lower_half = jnp.logical_and(lane >= 2 * LANES // 4 - 2, lane < LANES - 2)
        ends[side] = jnp.where(lower_half, pltpu.roll(tile[upper:], LANES // 2, 1), tile[0:upper]).astype(BF16)
    pl.semaphore_wait(barrier, expected)
    halo_start(0)
    if vouches:
        vouch(0)

    def gram(left, right):
        return tree_sum([split_dot(*left(x, y), *right(x, y), 1, 1) for x, y in own])

    def sum_copy(round_, number, peer):
        axes = plans[round_][number]
        count, index = group_of(axes)
        slot = offset_of(round_, number) + index
        return pltpu.make_async_remote_copy(
            src_ref=shares_of[round_].at[slot], dst_ref=shares_of[round_].at[slot],
            send_sem=sent, recv_sem=sum_recv.at[arrival(round_, number)],
            device_id=peer, device_id_type=pl.DeviceIdType.MESH,
        )

    def sum_start(round_, number, tile):
        axes = plans[round_][number]
        count, index = group_of(axes)
        shares_of[round_][offset_of(round_, number) + index] = tile
        if axes == AXES:
            plane = []
            for k in range(flat):
                there = lax.rem(spot + k, flat)
                plane.append((lax.div(there, sizes[1]), lax.rem(there, sizes[1])))
            low = 2 * me[2] < sizes[2]
            far, turn = jnp.where(low, sizes[2] - 1, 0), jnp.where(low, -1, 1)
            away = jnp.where(low, sizes[2] - 1 - me[2], me[2])
            for i in range(sizes[2] - 1):
                level = far + turn * (i + jnp.where(i < away, 0, 1))
                for gx, gy in plane[::-1]:
                    sum_copy(round_, number, {"gx": gx, "gy": gy, "gz": level}).start()
            for gx, gy in plane[:0:-1]:
                sum_copy(round_, number, {"gx": gx, "gy": gy, "gz": me[2]}).start()
        else:
            def send(k, carry):
                sum_copy(round_, number, peer_id(axes, lax.rem(index + k, count))).start()
                return carry

            each(count, send)

    def arrival(round_, number):
        return sum(len(phases) for phases in plans[:round_]) + number

    def sum_units(round_, number):
        return (group_of(plans[round_][number])[0] - 1)

    def sum_finish(round_, number):
        total = sum_units(round_, number)
        if total:
            wait_units(total, sum_recv.at[arrival(round_, number)])
        start = offset_of(round_, number)
        return tree_sum([shares_of[round_][start + peer] for peer in range(group_of(plans[round_][number])[0])])

    def sum_turn(round_):
        for number in range(1, len(plans[round_])):
            sum_start(round_, number, sum_finish(round_, number - 1))

    def sum_rest(round_):
        return sum_finish(round_, len(plans[round_]) - 1)

    def loads_at(x, y):
        return stack[x, y, 0:cols, :]

    def image_at(x, y):
        return stack[x, y, cols:, :]

    for x, y in own:
        low[x, y, 0:cols, :] = (loads_at(x, y) - padded[x + 2, y + 2].astype(F32)).astype(BF16)

    def loads_split(x, y):
        return padded[x + 2, y + 2], low[x, y, 0:cols, :]

    def image_split(x, y):
        return padded_im[x, y], low[x, y, cols:, :]

    square_part = gram(loads_split, loads_split)
    sum_start(0, 0, pack(square_part))
    halo_wait((0,), sent_first)
    halo_start(1)
    for round_ in range(1, vouches):
        vouched(round_ - 1)
        vouch(round_)
    moduli_copy.wait()

    def block_of(x, y):
        bx, lx = (0, nx - 2 + x) if x < 2 else (2, x - nx - 2) if x >= nx + 2 else (1, x - 2)
        by, ly = (0, ny - 2 + y) if y < 2 else (2, y - ny - 2) if y >= ny + 2 else (1, y - 2)
        return bx, by, lx * ny + ly

    odd = lax.rem(lane, 4) >= 2

    def merged(edge):
        return {
            (bx, by): jnp.where(odd, edge[bx, by, 0].astype(F32), edge[bx, by, 1].astype(F32))
            for bx, by in itertools.product(range(3), repeat=2)
        }

    def tail_of(tiles, x, y):
        bx, by, row = block_of(x, y)
        tile = tiles[bx, by]
        near, far = ((2 * LANES - spot - 4 * row) % LANES for spot in (0, LANES // 2))
        return jnp.concatenate([pltpu.roll(tile, near, 1), pltpu.roll(tile, far, 1)], axis=0)

    def modulus_of(ids):
        found = jnp.zeros(ids.shape, F32)
        for number in range(mats):
            found = jnp.where(ids == float(number + 1), moduli_ref[number], found)
        return found

    own_modulus = modulus_of(mats_rx[1, 1].astype(F32))
    halo_wait((0,), halo_recv.at[0])
    if vouches:
        vouched(vouches - 1)
    sum_turn(0)
    full = nz + LANES
    tails = merged(ends_rx)
    dense = {}
    for key in tails:
        flat_ids = own_modulus if key == (1, 1) else modulus_of(mats_rx[key].astype(F32))
        side = pltpu.roll(modulus_of(tails[key]), LANES - id_spot, 1, stride=4, stride_axis=0)
        both = jnp.concatenate([flat_ids, side], axis=1)
        dense[key] = ((0.125 * k_far) * (both + pltpu.roll(both, full - 1, 1)),
                      (0.125 * k_far) * (both + pltpu.roll(both, 1, 1)))
    sums = {}

    def sum_at(x, y):
        if (x, y) not in sums:
            bx, by, row = block_of(x, y)
            sums[x, y] = [jnp.broadcast_to(part[row : row + 1, :], (8, full)) for part in dense[bx, by]]
        return sums[x, y]

    def weigh(x, y):
        around = [sum_at(x, y), sum_at(x, y + 1), sum_at(x + 1, y), sum_at(x + 1, y + 1)]
        after, before = (tree_sum([pair[side] for pair in around]) for side in range(2))
        wt[x, y], wtr[x, y], level[x, y] = after, before, before + after

    def around_of(weights, x, y):
        return (weights[x, y] + weights[x, y + 1]) + (weights[x + 1, y] + weights[x + 1, y + 1])

    def gather(x, y):
        above, below = around_of(wtr, x, y), around_of(wt, x, y)
        node[0, x, y], node[1, x, y], node[2, x, y] = above, below, (k_self / k_far) * (above + below)

    def unfold(x, y):
        field[x, y] = jnp.concatenate([padded[x, y].astype(F32), tail_of(tails, x, y)], axis=1)

    inner = list(itertools.product(range(1, nx + 1), range(1, ny + 1)))
    outer = [key for key in itertools.product(range(nx + 2), range(ny + 2)) if key not in inner]
    near = list(itertools.product(range(1, nx + 3), range(1, ny + 3)))
    near_elements = list(itertools.product(range(1, nx + 2), range(1, ny + 2)))
    for key in near:
        unfold(*key)
    for key in near_elements:
        weigh(*key)
    for key in inner:
        gather(*key)

    def double(tile):
        return jnp.concatenate([tile, tile], axis=0)

    def operate(source, shift, cells, direction_of, write, width):
        lines, ahead_of, behind_of = {}, {}, {}

        def line(x, y):
            if (x, y) not in lines:
                lines[x, y] = source[x - shift, y - shift] + source[x - shift, y + 1 - shift]
            return lines[x, y]

        for x, y in cells:
            here = source[x + 1 - shift, y + 1 - shift]
            corners = list(itertools.product((x, x + 1), (y, y + 1)))
            flats = []
            for ex, ey in corners:
                if (ex, ey) not in ahead_of:
                    corner_sum = line(ex, ey) + line(ex + 1, ey)
                    ahead_of[ex, ey] = double(wtr[ex, ey]) * corner_sum
                    behind_of[ex, ey] = double(wt[ex, ey]) * corner_sum
                opposite = source[2 * ex - x - shift, 2 * ey - y - shift][:, 0:width]
                flats.append(double(level[ex, ey, :, 0:width]) * opposite)
            ahead = tree_sum([ahead_of[key] for key in corners]) - double(node[0, x, y]) * here
            behind = tree_sum([behind_of[key] for key in corners]) - double(node[1, x, y]) * here
            around = pltpu.roll(ahead, full - 1, 1)[:, 0:width] + pltpu.roll(behind, 1, 1)[:, 0:width]
            centre = double(node[2, x, y, :, 0:width]) * here[:, 0:width]
            write(x, y, SIGMA * direction_of(x, y) + (around + tree_sum(flats) + centre))

    has_right = (me[2] < sizes[2] - 1).astype(jnp.int32)
    has_left = (me[2] > 0).astype(jnp.int32)
    beyond = jnp.logical_or(lane < has_right, lane >= LANES - has_left)

    def write_first(x, y, image):
        main = image[:, 0:nz]
        stack[x - 1, y - 1, cols:, :] = main
        padded_im[x - 1, y - 1], low[x - 1, y - 1, cols:, :] = halves(main)
        field_im[x, y] = jnp.concatenate([main, jnp.where(beyond, image[:, nz:], 0.0)], axis=1)

    def loads_wide(x, y):
        return jnp.concatenate([loads_at(x - 1, y - 1), field[x + 1, y + 1][:, nz:]], axis=1)

    operate(field, 0, inner, loads_wide, write_first, full)

    def pair_split(x, y):
        return jnp.concatenate([padded[x + 2, y + 2], padded_im[x, y]], axis=0), low[x, y]

    both_part = gram(image_split, pair_split)
    sum_start(1, 0, pack(both_part[:, 0:cols]))
    sum_start(2, 0, pack(both_part[:, cols:]))
    for key in itertools.product(range(nx + 3), range(ny + 3)):
        if key not in near_elements:
            weigh(*key)
    for key in outer:
        gather(*key)
    halo_wait((1,), halo_recv.at[1])
    for key in itertools.product(range(nx + 4), range(ny + 4)):
        if key not in near:
            unfold(*key)

    def write_ring(x, y, image):
        dx = -1 if x == 0 else 1 if x == nx + 1 else 0
        dy = -1 if y == 0 else 1 if y == ny + 1 else 0
        if any(step and sizes[i] == 1 for i, step in enumerate((dx, dy))):
            field_im[x, y] = jnp.zeros(image.shape, F32)
        else:
            image = jnp.where(exists((dx, dy, 0)), image, 0.0)
            field_im[x, y] = jnp.concatenate([image[:, 0:nz], jnp.where(beyond, image[:, nz:], 0.0)], axis=1)

    operate(field, 0, outer, lambda x, y: field[x + 1, y + 1], write_ring, full)
    last_parts = []

    def write_last(x, y, image):
        last_parts.append(split_dot(*image_split(x - 1, y - 1), *halves(image), 1, 1))

    operate(field_im, 1, inner, lambda x, y: image_at(x - 1, y - 1), write_last, nz)
    sum_start(3, 0, pack(tree_sum(last_parts)))

    square = unpack(sum_rest(0), cols)
    sum_turn(1)
    sum_turn(2)
    row_id = lax.broadcasted_iota(jnp.int32, (cols, LANES), 0)
    col_id = lax.broadcasted_iota(jnp.int32, (cols, LANES), 1)
    eye = jnp.where(row_id == col_id, 1.0, 0.0)
    inverse = solve(columns_of(square), rows_of(eye))
    cells = list(itertools.product(range(nx + 2), range(ny + 2)))
    for x, y in cells:
        wide[x, y, 0:cols, :] = field[x + 1, y + 1].astype(BF16)
        wide[x, y, cols:, :] = field_im[x, y].astype(BF16)
    for x, y in own:
        high = jnp.concatenate([padded[x + 2, y + 2], padded_im[x, y]], axis=0).astype(F32)
        third[x, y] = ((stack[x, y] - high) - low[x, y].astype(F32)).astype(BF16)

    def mixture(parts, cell, rows):
        x, y = cell
        if cell not in inner:
            product = dot(jnp.concatenate(parts[0:2], axis=0), wide[x, y, rows, :], 1, 0, None)
            return product[0:cols] + product[cols:]
        one = dot(jnp.concatenate(parts, axis=0), wide[x, y, rows, :], 1, 0, None)
        two = dot(jnp.concatenate(parts[0:2], axis=0), low[x - 1, y - 1, rows, :], 1, 0, None)
        three = dot(parts[0], third[x - 1, y - 1, rows, :], 1, 0, None)
        small = (one[cols : 2 * cols, 0:nz] + two[0:cols]) + ((one[2 * cols :, 0:nz] + two[cols:]) + three)
        return jnp.concatenate([one[0:cols, 0:nz] + small, one[0:cols, nz:] + one[cols : 2 * cols, nz:]], axis=1)

    cross = unpack(sum_rest(1), cols)
    cross = 0.5 * (cross + turn(cross))
    cross_columns = columns_of(cross)
    alpha_rows = solve(cross_columns, rows_of(square))
    alpha_t = turn(jnp.concatenate(alpha_rows, axis=0))
    alpha_columns = columns_of(alpha_t)
    quad = unpack(sum_rest(2), cols)
    moved, stood = weave(columns_of(quad), alpha_rows), weave(cross_columns, alpha_rows)
    alpha_t = alpha_t[:, 0:cols]
    alpha_split = halves(alpha_t)
    alpha_parts = thirds(alpha_t)
    for cell in cells:
        x, y = cell
        base = field[x + 1, y + 1]
        if cell in inner:
            base = jnp.concatenate([loads_at(x - 1, y - 1), base[:, nz:]], axis=1)
        field_im[x, y] = base - mixture(alpha_parts, cell, slice(cols, 2 * cols))
    updated = square + weave(alpha_columns, rows_of(moved)) - (stood + turn(stood))
    beta_t = weave(columns_of(updated), inverse)
    grown_t = eye + beta_t
    grown_columns = columns_of(grown_t)
    joint = weave(grown_columns, rows_of(moved))
    known = weave(columns_of(weave(grown_columns, rows_of(cross))), rows_of(turn(grown_t))) - (joint + turn(joint))
    beta_t = beta_t[:, 0:cols]
    beta_parts = thirds(beta_t)
    for cell in cells:
        x, y = cell
        rest = field_im[x, y]
        direction = rest + mixture(beta_parts, cell, slice(0, cols))
        rounded = direction.astype(BF16)
        field_im[x, y] = rounded.astype(F32)
        if cell in inner:
            base_ref[x - 1, y - 1, cols:, :] = rest[:, 0:nz]
            direction, rounded = direction[:, 0:nz], rounded[:, 0:nz]
            stack[x - 1, y - 1, cols:, :] = direction
            pair_ref[x - 1, y - 1, 0, 0:cols, :] = rounded
            pair_ref[x - 1, y - 1, 0, cols:, :] = (direction - rounded.astype(F32)).astype(BF16)

    halo_wait((1,), sent, sum(
        sum_units(round_, number) for round_ in range(4) for number in range(len(plans[round_]))
        if (round_, number) != (3, 1)
    ))
    sum_turn(3)
    last = unpack(sum_rest(3), cols)
    total = known + weave(alpha_columns, rows_of(weave(columns_of(last), alpha_rows)))
    last_rows = solve(columns_of(total), rows_of(updated))
    coef_t = jnp.concatenate(last_rows, axis=0)[:, 0:cols].T
    coef_ref[0:cols, :], coef_ref[cols:, :] = halves(coef_t)

    def write_second(x, y, image):
        pair_ref[x - 1, y - 1, 1, 0:cols, :], pair_ref[x - 1, y - 1, 1, cols:, :] = halves(image)

    operate(field_im, 1, inner, lambda x, y: image_at(x - 1, y - 1), write_second, nz)
    for x, y in own:
        base_ref[x, y, 0:cols, :] = split_dot(*alpha_split, *loads_split(x, y), 1, 0)
    if len(plans[3]) > 1:
        wait_units(sum_units(3, 1), sent)


def last_body(coef_ref, base_ref, pair_ref, sol_ref, res_ref, stage, sems):
    cols, nx, ny, nz = sol_ref.shape
    high, low = coef_ref[0:cols, :], coef_ref[cols:, :]
    for x in range(nx):
        for which, ref, sign in ((0, sol_ref, 1.0), (1, res_ref, -1.0)):
            rows = slice(which * cols, (which + 1) * cols)
            for y in range(ny):
                added = split_dot(high, low, pair_ref[x, y, which, 0:cols, :], pair_ref[x, y, which, cols:, :], 1, 0)
                stage[which, :, x, y, :] = base_ref[x, y, rows, :] + sign * added
            pltpu.make_async_copy(stage.at[which, :, x], ref.at[:, x], sems.at[which]).start()
    for which in range(2):
        pltpu.make_async_copy(stage.at[which], stage.at[which], sems.at[which]).wait()


def on_device(sizes, loads, moduli, material):
    cols, nx, ny, nz = loads.shape
    count = int(np.prod(sizes))
    split = (("gx", "gy"), ("gz",))
    quick = (AXES,) if count <= DIRECT_LIMIT else split
    plans = (split, quick, quick, quick)

    def slots(phases):
        return sum(int(np.prod([sizes[AXES.index(a)] for a in axes])) for axes in phases)

    vmem = pl.BlockSpec(memory_space=pltpu.VMEM)
    anywhere = pl.BlockSpec(memory_space=pl.ANY)
    full = nz + LANES
    tiles = (nz // LANES) * 4 * (nx + ny + 4) + 18 + 8 * (nx * ny * nz // (cols * LANES))
    credits = tiles * TILE_UNITS // cols + 2 * sum(slots(phases) for phases in plans)
    base, pair, coef = pl.pallas_call(
        functools.partial(main_body, sizes, plans, stiffness_values()),
        out_shape=(
            pltpu.VMEM((nx, ny, 2 * cols, nz), F32),
            pltpu.VMEM((nx, ny, 2, 2 * cols, nz), BF16),
            pltpu.VMEM((2 * cols, cols), BF16),
        ),
        in_specs=[anywhere, anywhere, anywhere],
        out_specs=(vmem, vmem, vmem),
        scratch_shapes=[
            pltpu.VMEM((nx, ny, 2 * cols, nz), F32),
            pltpu.VMEM((nx, ny, 2 * cols, nz), BF16),
            pltpu.VMEM((nx, ny, 2 * cols, nz), BF16),
            pltpu.VMEM((nx + 2, ny + 2, 2 * cols, full), BF16),
            pltpu.VMEM((nx + 4, ny + 4, cols, nz), BF16),
            pltpu.VMEM((nx, ny, cols, nz), BF16),
            pltpu.VMEM((3, 3, nx * ny, nz), BF16),
            pltpu.VMEM((2, cols // 2, LANES), BF16),
            pltpu.VMEM((3, 3, 2, cols // 2, LANES), BF16),
            pltpu.VMEM((nx + 4, ny + 4, cols, full), F32),
            pltpu.VMEM((nx + 2, ny + 2, cols, full), F32),
            pltpu.VMEM((nx + 3, ny + 3, 8, full), F32),
            pltpu.VMEM((nx + 3, ny + 3, 8, full), F32),
            pltpu.VMEM((nx + 3, ny + 3, 8, full), F32),
            pltpu.VMEM((3, nx + 2, ny + 2, 8, full), F32),
            pltpu.VMEM((slots(plans[0]), cols * cols // LANES, LANES), F32),
            pltpu.VMEM((slots(plans[1]), cols * cols // LANES, LANES), F32),
            pltpu.VMEM((slots(plans[2]), cols * cols // LANES, LANES), F32),
            pltpu.VMEM((slots(plans[3]), cols * cols // LANES, LANES), F32),
            pltpu.SMEM(moduli.shape, F32),
            pltpu.VMEM(material.shape, jnp.int32),
            pltpu.VMEM((credits, cols * cols // LANES, LANES), F32),
            pltpu.SemaphoreType.DMA,
            pltpu.SemaphoreType.DMA,
            pltpu.SemaphoreType.DMA((2,)),
            pltpu.SemaphoreType.DMA((sum(len(phases) for phases in plans),)),
            pltpu.SemaphoreType.DMA((3,)),
            pltpu.SemaphoreType.REGULAR((max(sizes[2] - 2, 1) if count <= DIRECT_LIMIT else 1, 2)),
        ],
        compiler_params=pltpu.CompilerParams(collective_id=0, has_side_effects=True),
    )(moduli, loads, material)
    out = jax.ShapeDtypeStruct(loads.shape, F32)
    return pl.pallas_call(
        last_body,
        out_shape=(out, out),
        in_specs=[vmem, vmem, vmem],
        out_specs=(anywhere, anywhere),
        scratch_shapes=[pltpu.VMEM((2, cols, nx, ny, nz), F32), pltpu.SemaphoreType.DMA((2,))],
        compiler_params=pltpu.CompilerParams(vmem_limit_bytes=4 * 2**20),
    )(coef, base, pair)


def solution(mesh):
    sizes = tuple(mesh.shape[axis] for axis in AXES)
    in_specs = (P(None, "gx", "gy", "gz"), P(), P("gx", "gy", "gz"))
    out_specs = (P(None, "gx", "gy", "gz"), P(None, "gx", "gy", "gz"))
    return jax.shard_map(
        functools.partial(on_device, sizes), mesh=mesh, in_specs=in_specs, out_specs=out_specs, check_vma=False
    )
```
